8 devices in a mesh: rep: 1 (over z), dp: 8 (over x, y, core).
Axes of the slice: x: 2, y: 2, z: 1, core: 2. Of those that a mesh axis runs over, the one named last changes fastest.
Arguments:
- x: bfloat16 [8, 2048, 896], P(('rep', 'dp'))
- dy: bfloat16 [8, 2048, 896], P(('rep', 'dp'))
- wq: bfloat16 [2, 896, 896], P(None, 'dp')
- wk: bfloat16 [2, 896, 128], P(None, 'dp')
- wv: bfloat16 [2, 896, 128], P(None, 'dp')
- wo: bfloat16 [2, 896, 896], P(None, 'dp')
- w_gate: bfloat16 [2, 896, 2560], P(None, 'dp')
- w_up: bfloat16 [2, 896, 2560], P(None, 'dp')
- w_down: bfloat16 [2, 2560, 896], P(None, 'dp')
- m_wq: float32 [2, 896, 896], P(None, 'dp')
- m_wk: float32 [2, 896, 128], P(None, 'dp')
- m_wv: float32 [2, 896, 128], P(None, 'dp')
- m_wo: float32 [2, 896, 896], P(None, 'dp')
- m_w_gate: float32 [2, 896, 2560], P(None, 'dp')
- m_w_up: float32 [2, 896, 2560], P(None, 'dp')
- m_w_down: float32 [2, 2560, 896], P(None, 'dp')
- v_wq: float32 [2, 896, 896], P(None, 'dp')
- v_wk: float32 [2, 896, 128], P(None, 'dp')
- v_wv: float32 [2, 896, 128], P(None, 'dp')
- v_wo: float32 [2, 896, 896], P(None, 'dp')
- v_w_gate: float32 [2, 896, 2560], P(None, 'dp')
- v_w_up: float32 [2, 896, 2560], P(None, 'dp')
- v_w_down: float32 [2, 2560, 896], P(None, 'dp')
Outputs:
- output 1: bfloat16 [2, 896, 896], P('rep', 'dp')
- output 2: bfloat16 [2, 896, 128], P('rep', 'dp')
- output 3: bfloat16 [2, 896, 128], P('rep', 'dp')
- output 4: bfloat16 [2, 896, 896], P('rep', 'dp')
- output 5: bfloat16 [2, 896, 2560], P('rep', 'dp')
- output 6: bfloat16 [2, 896, 2560], P('rep', 'dp')
- output 7: bfloat16 [2, 2560, 896], P('rep', 'dp')
- output 8: float32 [2, 896, 896], P('rep', 'dp')
- output 9: float32 [2, 896, 128], P('rep', 'dp')
- output 10: float32 [2, 896, 128], P('rep', 'dp')
- output 11: float32 [2, 896, 896], P('rep', 'dp')
- output 12: float32 [2, 896, 2560], P('rep', 'dp')
- output 13: float32 [2, 896, 2560], P('rep', 'dp')
- output 14: float32 [2, 2560, 896], P('rep', 'dp')
- output 15: float32 [2, 896, 896], P('rep', 'dp')
- output 16: float32 [2, 896, 128], P('rep', 'dp')
- output 17: float32 [2, 896, 128], P('rep', 'dp')
- output 18: float32 [2, 896, 896], P('rep', 'dp')
- output 19: float32 [2, 896, 2560], P('rep', 'dp')
- output 20: float32 [2, 896, 2560], P('rep', 'dp')
- output 21: float32 [2, 2560, 896], P('rep', 'dp')
All inputs are finite; a program needn't handle non-finite values.
Results may differ from the reference program's by a relative error of at most 0.0291.
Values are sent between devices in bfloat16 or wider.
A program may use at most 2 GiB of HBM per device.

```python
import jax
import jax.numpy as jnp
from jax import lax

SEQUENCES = 8
TOKENS = 2048
D = 896
HEADS = 7
KV_HEADS = 1
HEAD = 128
FF = 2560
LAYERS = 2
THETA = 10000
NAMES = ("wq", "wk", "wv", "wo", "w_gate", "w_up", "w_down")
SHAPES = {
    "wq": (LAYERS, D, HEADS * HEAD),
    "wk": (LAYERS, D, KV_HEADS * HEAD),
    "wv": (LAYERS, D, KV_HEADS * HEAD),
    "wo": (LAYERS, HEADS * HEAD, D),
    "w_gate": (LAYERS, D, FF),
    "w_up": (LAYERS, D, FF),
    "w_down": (LAYERS, FF, D),
}


def bump(key, n, height):
    away = (jnp.arange(n, dtype=jnp.int32) - jax.random.randint(key, (), 0, n, jnp.int32)) % n
    return jnp.where(away < n // 8, height, 1.0)


def together(key, own, strength):
    shared = jax.random.normal(key, own.shape[1:], jnp.float32)
    return (own + strength * shared) * lax.rsqrt(1 + strength * strength)


def setup_inputs(seed: int = 0, part: int = 0) -> dict:
    kx, kdy, ka, kb, kz, kf, kh, kl, *keys = jax.random.split(jax.random.key(seed), 8 + 3 * len(NAMES))
    kx, kdy, ka, kb = (jax.random.fold_in(k, part) for k in (kx, kdy, ka, kb))
    kw, km, kv = (keys[i::3] for i in range(3))
    shape = (SEQUENCES, TOKENS, D)
    much_x, much_dy = jax.random.uniform(kz, (2,), jnp.float32, 0.0, 1.0)
    loud = 2.0 ** jax.random.uniform(jax.random.fold_in(kz, 1), (), jnp.float32, -1.0, 2.0)
    layers = 2.0 ** jax.random.uniform(kl, (LAYERS, 1, 1), jnp.float32, -1.0, 1.0)
    times = {"wq": 1.0, "wk": 1.0, "wv": 2.0, "wo": layers, "w_gate": 1.0, "w_up": bump(kh, FF, 4.0), "w_down": layers}
    x = together(ka, jax.random.normal(kx, shape, jnp.float32), much_x) * bump(kf, D, 4.0)
    dy = together(kb, jax.random.normal(kdy, shape, jnp.float32), much_dy)
    drawn = {"x": x.astype(jnp.bfloat16), "dy": (loud * dy * (SEQUENCES * TOKENS) ** -0.5).astype(jnp.bfloat16)}
    for key, name in zip(kw, NAMES, strict=True):
        drawn[name] = (jax.random.normal(key, SHAPES[name], jnp.float32) * SHAPES[name][1] ** -0.5 * times[name]).astype(jnp.bfloat16)
    for key, name in zip(km, NAMES, strict=True):
        drawn[f"m_{name}"] = 0.1 * jax.random.normal(key, SHAPES[name], jnp.float32)
    for key, name in zip(kv, NAMES, strict=True):
        drawn[f"v_{name}"] = jax.random.uniform(key, SHAPES[name], jnp.float32, 0.02, 0.06)
    return drawn


def matmul(a, w):
    return jnp.dot(a, w, preferred_element_type=jnp.float32).astype(jnp.bfloat16)


def normed(h):
    wide = h.astype(jnp.float32)
    scale = lax.rsqrt(jnp.mean(wide**2, -1, keepdims=True) + 1e-6)
    return (wide * scale).astype(jnp.bfloat16)


def turned(t, theta):
    half = t.shape[-1] // 2
    angle = jnp.arange(t.shape[0], dtype=jnp.float32)[:, None] * theta ** (-jnp.arange(half, dtype=jnp.float32) / half)
    cos, sin = jnp.cos(angle)[:, None], jnp.sin(angle)[:, None]
    a, b = t[..., :half].astype(jnp.float32), t[..., half:].astype(jnp.float32)
    return jnp.concatenate([a * cos - b * sin, b * cos + a * sin], -1).astype(jnp.bfloat16)


def seen_by(q, k, v):
    tokens, kv = q.shape[0], k.shape[1]
    q = q.reshape(tokens, kv, -1, q.shape[-1])
    scores = jnp.einsum("tgsd,ugd->gstu", q.astype(jnp.float32), k.astype(jnp.float32)) * q.shape[-1] ** -0.5
    place = jnp.arange(tokens)
    weights = jax.nn.softmax(jnp.where(place[:, None] >= place, scores, -jnp.inf), -1).astype(jnp.bfloat16)
    return jnp.einsum("gstu,ugd->tgsd", weights.astype(jnp.float32), v.astype(jnp.float32)).astype(jnp.bfloat16).reshape(tokens, -1)


def layer(h, w):
    a = normed(h)
    q, k = (turned(matmul(a, w[name]).reshape(h.shape[0], -1, HEAD), THETA) for name in ("wq", "wk"))
    h = h + matmul(seen_by(q, k, matmul(a, w["wv"]).reshape(h.shape[0], -1, HEAD)), w["wo"])
    b = normed(h)
    gate = jnp.dot(b, w["w_gate"], preferred_element_type=jnp.float32)
    up = jnp.dot(b, w["w_up"], preferred_element_type=jnp.float32)
    return h + matmul((jax.nn.silu(gate) * up).astype(jnp.bfloat16), w["w_down"])


def adamw(w, m, v, g):
    m = 0.9 * m + 0.1 * g
    v = 0.95 * v + 0.05 * g * g
    step = m * lax.rsqrt(v + 1e-8) + 0.1 * w
    return (w - 0.02 * step).astype(jnp.bfloat16), m, v


def clipped(gradients, sum_of_squares, count):
    factor = jnp.minimum(1.0, 0.5 * lax.rsqrt(sum_of_squares / count + 1e-30))
    return [g * factor for g in gradients]


def stack(weights, h):
    return lax.scan(lambda h, w: (layer(h, w), None), h, weights)[0]


def reference(x, dy, wq, wk, wv, wo, w_gate, w_up, w_down, m_wq, m_wk, m_wv, m_wo, m_w_gate, m_w_up, m_w_down, v_wq, v_wk, v_wv, v_wo, v_w_gate, v_w_up, v_w_down):
    weights = dict(zip(NAMES, (wq, wk, wv, wo, w_gate, w_up, w_down), strict=True))

    def take(so_far, sequence):
        h, by_y = sequence
        _, back = jax.vjp(stack, weights, h)
        by_weights, by_h = back(by_y)
        return jax.tree.map(lambda total, term: total + term.astype(jnp.float32), so_far, by_weights), by_h

    none_yet = {name: jnp.zeros(w.shape, jnp.float32) for name, w in weights.items()}
    by_weights, by_x = lax.scan(take, none_yet, (x, dy))
    gradients = [by_weights[name].astype(jnp.bfloat16).astype(jnp.float32) for name in NAMES]
    gradients = clipped(gradients, sum(jnp.sum(g * g) for g in gradients), sum(g.size for g in gradients))
    first = (m_wq, m_wk, m_wv, m_wo, m_w_gate, m_w_up, m_w_down)
    second = (v_wq, v_wk, v_wv, v_wo, v_w_gate, v_w_up, v_w_down)
    new = [adamw(weights[name].astype(jnp.float32), m, v, g) for name, m, v, g in zip(NAMES, first, second, gradients, strict=True)]
    return tuple(one[which] for which in range(3) for one in new)
```

```python
import functools

import jax
import jax.numpy as jnp
import numpy as np
from jax import lax
from jax.experimental import pallas as pl
from jax.experimental.pallas import tpu as pltpu
from jax.sharding import PartitionSpec as P

NEG = -1e30
HIDDEN = 2 * NEG
LOG2E = 1.4426950408889634
VMEM = 62 * 2**20
STRIP = 512
HEAD = 128
HALF = HEAD // 2
THETA = 10000
F32, BF16 = jnp.float32, jnp.bfloat16


def dot(a, b, ca=1, cb=0):
    return lax.dot_general(a, b, (((ca,), (cb,)), ((), ())), preferred_element_type=F32)


def dot_t(a, b):
    return dot(a, b, 1, 1)


def loop(stop, body, start=0):
    lax.fori_loop(start, stop, body, None)


def rounded(a):
    return a.astype(BF16).astype(F32)


def norm_scale(wide):
    return lax.rsqrt(jnp.mean(wide * wide, -1, keepdims=True) + 1e-6)


def norm_back(wide, by):
    scale = norm_scale(wide)
    return scale * (by - wide * (scale * scale * jnp.mean(by * wide, -1, keepdims=True)))


def params(**more):
    return pltpu.CompilerParams(vmem_limit_bytes=VMEM, **more)


def whole(*shape):
    return pl.BlockSpec(shape, lambda *_: (0,) * len(shape))


def cost(flops, nbytes=0, exps=0):
    return pl.CostEstimate(flops=int(flops), bytes_accessed=int(nbytes), transcendentals=int(exps))


def tables(tokens):
    angle = np.arange(tokens, dtype=np.float64)[:, None] * THETA ** (-np.arange(HALF, dtype=np.float64) / HALF)
    cos, sin = np.cos(angle), np.sin(angle)
    return jnp.asarray(np.concatenate([cos, cos], 1), F32), jnp.asarray(np.concatenate([-sin, sin], 1), F32)


def gap(bk, cols, bq):
    return lax.broadcasted_iota(jnp.int32, (bk, cols), 1) - lax.broadcasted_iota(jnp.int32, (bk, cols), 0)


def side_by_side(ref):
    return jnp.concatenate([ref[n] for n in range(ref.shape[0])], axis=1)


X, Y, CORE, HERE = 4, 2, 1, 0
NEAR = (HERE, X, Y, X + Y)


def flip(me, bits):
    for bit in (X, Y, CORE):
        if bits & bit:
            me = me + bit - 2 * bit * lax.rem(lax.div(me, bit), 2)
    return me


def greet(me):
    barrier = pltpu.get_barrier_semaphore()
    for bit in (X, Y, CORE):
        pl.semaphore_signal(barrier, inc=1, device_id=(0, flip(me, bit)), device_id_type=pl.DeviceIdType.MESH)
    pl.semaphore_wait(barrier, 3)


def remote(me, bit, src, dst, send, recv):
    return pltpu.make_async_remote_copy(src_ref=src, dst_ref=dst, send_sem=send, recv_sem=recv, device_id=(0, flip(me, bit)),
                                        device_id_type=pl.DeviceIdType.MESH)


def halves(r):
    a = (r // 2 + 15) // 16 * 16
    return (0, a), (a, r - a)


def upper(r):
    return halves(r)[0]


def lower(r):
    return halves(r)[1]


ALL = None
ROUTES = {"x": (X, HERE, ALL), "y": (Y, HERE, ALL), "core": (CORE, HERE, ALL), "xy": (Y, X, upper), "x core": (CORE, X, ALL),
          "yx": (X, Y, lower), "y core": (CORE, Y, ALL), "xy core": (CORE, X + Y, upper), "yx core": (CORE, X + Y, lower)}


class Gather:
    def __init__(self, me, block, full, send, recv, cols=None):
        r, n = block.shape
        self.me, self.r = me, r
        self.cols = cols or (0, n)
        self.full, self.send, self.recv = full, send, recv
        self.own = block.at[:, pl.ds(*self.cols)]

    def rows(self, bits, part=None):
        first, count = part or (0, self.r)
        at = pl.multiple_of(flip(self.me, bits) * self.r + first, 16)
        return self.full.at[pl.ds(at, count), pl.ds(*self.cols)]

    def copy(self, which, got=False):
        bit, bits, part = ROUTES[which]
        there = self.rows(bits + bit if got else bits, part and part(self.r))
        n = tuple(ROUTES).index(which)
        return remote(self.me, bit, self.own if bits == HERE and not got else there, there, self.send.at[n], self.recv.at[n])

    def got(self, which):
        self.copy(which, got=True).wait_recv()

    def begin(self):
        for n in ("x", "y", "core"):
            self.copy(n).start()

    def hand_on(self):
        self.got("x")
        self.copy("xy").start()
        self.copy("x core").start()
        self.got("y")
        self.copy("yx").start()
        self.copy("y core").start()

    def finish(self):
        self.got("xy")
        self.copy("xy core").start()
        self.got("yx")
        self.copy("yx core").start()

    def arrived(self):
        for n in ("core", "x core", "y core", "xy core", "yx core"):
            self.got(n)

    def sent(self):
        for n in ROUTES:
            self.copy(n).wait_send()


class Scatter:
    def __init__(self, me, src, mine, theirs, across, from_x, from_y, out, send, recv, local):
        self.me, self.src, self.out = me, src, out
        self.r, self.n = theirs.shape[1:]
        self.own, self.theirs, self.across, self.from_x, self.from_y = mine, theirs, across, from_x, from_y
        self.send, self.recv, self.local = send, recv, local
        self.a, self.b = halves(self.r)
        self.all = (0, self.r)

    def block(self, bits, part=None):
        first, count = part or self.all
        return self.src.at[pl.ds(pl.multiple_of(flip(self.me, bits) * self.r + first, 16), count)]

    def mine(self, j, part):
        return self.block(NEAR[j], part) if self.own is None else self.own.at[j, pl.ds(*part)]

    def load(self, j):
        return pltpu.make_async_copy(self.block(NEAR[j]), self.own.at[j], self.local.at[j])

    def copy(self, n):
        if n < 4:
            bit, src, dst = CORE, self.block(CORE + NEAR[n]), self.theirs.at[n]
        else:
            bit, j, part, to = ((X, 3, self.a, self.across), (Y, 3, self.b, self.across), (X, 1, self.a, self.from_x),
                                (Y, 2, self.b, self.from_y), (Y, 2, self.a, self.from_y), (X, 1, self.b, self.from_x))[n - 4]
            src, dst = self.mine(j, part), to.at[pl.ds(*part)]
        return remote(self.me, bit, src, dst, self.send.at[n], self.recv.at[n])

    def add(self, j, part, *more):
        step = 16
        ref = self.mine(j, part)

        def one(i, _):
            rows = pl.ds(pl.multiple_of(i * step, step), step)
            full = pl.ds(pl.multiple_of(part[0] + i * step, step), step)
            total = ref[rows, :].astype(F32) + self.theirs[j, full, :].astype(F32)
            for other in more:
                total += other[full, :].astype(F32)
            ref[rows, :] = total.astype(BF16)

        loop(part[1] // step, one)

    def exchange(self):
        for j in range(4):
            self.copy(j).start()
            if self.own is not None:
                self.load(j).start()

    def first(self):
        for j in range(4):
            if self.own is not None:
                self.load(j).wait()
            self.copy(j).wait_recv()
        self.add(3, self.all)
        self.copy(4).start()
        self.copy(5).start()
        self.add(1, self.a)
        self.copy(6).start()
        self.add(2, self.b)
        self.copy(7).start()

    def second(self):
        self.copy(4).wait_recv()
        self.add(2, self.a, self.across)
        self.copy(8).start()
        self.copy(5).wait_recv()
        self.add(1, self.b, self.across)
        self.copy(9).start()

    def result(self):
        return pltpu.make_async_copy(self.mine(0, self.all), self.out, self.local.at[4])

    def last(self, squares):
        for n in range(6, 10):
            self.copy(n).wait_recv()
        self.add(0, self.all, self.from_x, self.from_y)
        ref = self.mine(0, self.all)
        self.result().start()
        squares[:] += sum_of_squares(ref)

    def done(self):
        for n in range(10):
            self.copy(n).wait_send()
        self.result().wait()


def sum_of_squares(ref):
    rows, cols = ref.shape

    def one(i, total):
        g = ref[pl.ds(pl.multiple_of(i * 16, 16), 16), :].astype(F32)
        g = g * g
        for c in range(0, cols, 128):
            total += g[:8, c : c + 128] + g[8:, c : c + 128]
        return total

    return lax.fori_loop(0, rows // 16, one, jnp.zeros((8, 128), F32))


def scatter_scratch(r, n, in_vmem=False):
    dma = pltpu.SemaphoreType.DMA
    block = pltpu.VMEM((r, n), BF16)
    return [*([] if in_vmem else [pltpu.VMEM((4, r, n), BF16)]), pltpu.VMEM((4, r, n), BF16), block, block, block,
            dma((10,)), dma((10,)), dma((5,))]


BQ = BK = 512
BT = 512
BF = 512
CUT = 1024
TENSORS = ("qkv", "o", "ga", "ua", "gb", "ub", "d")
PLAN = {}


def _forward(x_ref, sqkv, so, sg, su, sd, cos_ref, sin_ref, fqkv, fo, fg, fu, fd, q_o, k_o, v_o, o_o, lse_o, mid_o, gate_o, up_o, h_o,
             h_s, b_s, q_s, k_s, v_s, o_s, lse_s, act_s, wqkv_s, wo_s, wg_s, wu_s, wd_s, stage_s, top_s, mix_s, gap_s,
             send, recv, load, keep, out, wsem):
    layer, layers = pl.program_id(0), pl.num_programs(0)
    me = lax.axis_index("dp")
    tokens, d = h_s.shape
    heads = q_s.shape[0]
    ff = act_s.shape[1]

    def gathers(n):
        sems = lambda i: (send.at[n, i], recv.at[n, i])
        return {"qkv": Gather(me, sqkv.at[n], fqkv.at[n], *sems(0)), "o": Gather(me, so.at[n], fo.at[n], *sems(1)),
                "ga": Gather(me, sg.at[n], fg.at[n], *sems(2), (0, CUT)), "ua": Gather(me, su.at[n], fu.at[n], *sems(3), (0, CUT)),
                "gb": Gather(me, sg.at[n], fg.at[n], *sems(4), (CUT, ff - CUT)),
                "ub": Gather(me, su.at[n], fu.at[n], *sems(5), (CUT, ff - CUT)), "d": Gather(me, sd.at[n], fd.at[n], *sems(6))}

    def own_blocks():
        at = 0
        for s, f in ((sqkv, fqkv), (so, fo), (sg, fg), (su, fu), (sd, fd)):
            r, n = s.shape[1:]
            for i in range(s.shape[0]):
                yield s.at[i], act_s.at[pl.ds(at, r), pl.ds(0, n)], f.at[i, pl.ds(pl.multiple_of(me * r, 16), r)]
                at += r

    copies_in = lambda: [pltpu.make_async_copy(a, b, load.at[i]) for i, (a, b, _) in enumerate(own_blocks())]
    copies_out = lambda: [pltpu.make_async_copy(b, c, load.at[i]) for i, (_, b, c) in enumerate(own_blocks())]
    here = lambda i, n: pl.ds(pl.multiple_of(i * n, n), n)
    start_x = lambda: pltpu.make_async_copy(x_ref, h_s, keep.at[0])
    kept_qkv = lambda: [pltpu.make_async_copy(q_s, q_o.at[layer], keep.at[1]), pltpu.make_async_copy(k_s, k_o.at[layer], keep.at[2]),
                        pltpu.make_async_copy(v_s, v_o.at[layer], keep.at[3])]
    kept_o = lambda: [pltpu.make_async_copy(o_s, o_o.at[layer], keep.at[4]), pltpu.make_async_copy(lse_s, lse_o.at[layer], keep.at[5])]
    kept_mid = lambda: pltpu.make_async_copy(h_s, mid_o.at[layer], keep.at[6])
    kept_h = lambda: pltpu.make_async_copy(h_s, h_o, keep.at[7])
    weight = lambda n: pltpu.make_async_copy(*{"qkv": (fqkv.at[layer], wqkv_s, wsem.at[0]), "o": (fo.at[layer], wo_s, wsem.at[1]),
                                               "d": (fd.at[layer], wd_s, wsem.at[2])}[n])

    def column(c):
        cols = here(c, BF)
        slot = lax.rem(c, 2)
        return (pltpu.make_async_copy(fg.at[layer, :, cols], wg_s.at[slot], wsem.at[3 + slot]),
                pltpu.make_async_copy(fu.at[layer, :, cols], wu_s.at[slot], wsem.at[5 + slot]))

    def tick(phase, i):
        for (n, p, k), actions in PLAN.items():
            if p == phase:
                @pl.when((layer == n) & (i == k))
                def _():
                    for do, which, names in actions:
                        for name in names:
                            getattr(gathers(which)[name], do)()

    @pl.when(layer == 0)
    def _():
        start_x().start()
        for c in copies_in():
            c.start()
        greet(me)
        g = gathers(0)
        g["qkv"].begin()
        gap_s[:] = gap(BK, BQ, BQ)
        for c in copies_in():
            c.wait()
        for c in copies_out():
            c.start()
        start_x().wait()
        g["qkv"].hand_on()
        g["o"].begin()
        g["ga"].begin()
        g["ua"].begin()
        for c in copies_out():
            c.wait()
        g["qkv"].finish()
        g["qkv"].arrived()

    @pl.when(layer > 0)
    def _():
        kept_h().start()
        gathers(1)["qkv"].arrived()

    weight("qkv").start()
    weight("qkv").wait()

    def qkv_step(i, _):
        tick("qkv", i)
        rows = here(i, BT)
        wide = h_s[rows, :].astype(F32)
        a = (wide * norm_scale(wide)).astype(BF16)
        z = dot(a, wqkv_s[:])
        cos, sin = cos_ref[rows, :], sin_ref[rows, :]
        for n in range(heads + 1):
            t = rounded(z[:, n * HEAD : (n + 1) * HEAD])
            t = (t * cos + pltpu.roll(t, HALF, 1) * sin).astype(BF16)
            if n < heads:
                q_s[n, rows, :] = t
            else:
                k_s[rows, :] = t
        v_s[rows, :] = z[:, (heads + 1) * HEAD :].astype(BF16)

    loop(tokens // BT, qkv_step)
    for c in kept_qkv():
        c.start()

    scale = HEAD**-0.5
    e = scale * LOG2E
    ones = jnp.ones((8, BK), BF16)

    def attend_step(i, _):
        tick("attend", i)
        rows = here(i, BQ)
        top_s[:] = jnp.full(top_s.shape, NEG, F32)
        mix_s[:] = jnp.zeros(mix_s.shape, F32)

        def block(j, masked=False):
            keys = here(j, BK)
            scores = [dot_t(k_s[keys, :], q_s[n, rows, :]) for n in range(heads)]
            weights, rests = [], []
            for n, s in enumerate(scores):
                if masked:
                    s = jnp.where(gap_s[:] >= 0, s, HIDDEN)
                old = top_s[n : n + 1, :]
                top = jnp.maximum(old, s.max(axis=0, keepdims=True))
                top_s[n : n + 1, :] = top
                weights.append(jnp.exp2((s - top) * e).astype(BF16))
                rests.append(jnp.exp2((old - top) * e))
            values = jnp.concatenate([v_s[keys, :].T, ones], axis=0)
            for n, (p, rest) in enumerate(zip(weights, rests)):
                mix_s[n] = mix_s[n] * rest + dot(values, p)

        loop(i, lambda j, _: block(j))
        block(i, masked=True)
        for n in range(heads):
            total = mix_s[n, HEAD : HEAD + 1, :]
            o_s[n, rows, :] = (mix_s[n, :HEAD, :] * (1 / total)).T.astype(BF16)
            lse_s[n : n + 1, rows] = top_s[n : n + 1, :] * scale + jnp.log(total)

    loop(tokens // BQ, attend_step)
    for c in kept_o():
        c.start()

    for n in range(2):
        @pl.when(layer == n)
        def _():
            gathers(n)["o"].arrived()

    weight("o").start()

    @pl.when(layer > 0)
    def _():
        kept_h().wait()

    weight("o").wait()

    def out_step(i, _):
        tick("out", i)
        rows = here(i, BT)
        o = jnp.concatenate([o_s[n, rows, :] for n in range(heads)], axis=1)
        mid = (h_s[rows, :].astype(F32) + rounded(dot(o, wo_s[:]))).astype(BF16)
        h_s[rows, :] = mid
        wide = mid.astype(F32)
        b_s[rows, :] = (wide * norm_scale(wide)).astype(BF16)

    loop(tokens // BT, out_step)
    kept_mid().start()

    def staged(n, i, c):
        slot = lax.rem(n, 2)
        rows, cols = here(i, BT), here(c, BF)
        return [pltpu.make_async_copy(stage_s.at[slot, w], ref.at[layer, rows, cols], out.at[slot, w])
                for w, ref in enumerate((gate_o, up_o))]

    blocks = tokens // BT
    for n in range(2):
        @pl.when(layer == n)
        def _():
            gathers(n)["ga"].arrived()
            gathers(n)["ua"].arrived()

    for copy in column(0):
        copy.start()

    def gate_column(c, _):
        for n in range(2):
            @pl.when((layer == n) & (c + 1 == CUT // BF))
            def _():
                gathers(n)["gb"].arrived()
                gathers(n)["ub"].arrived()

        @pl.when(c + 1 < ff // BF)
        def _():
            for copy in column(c + 1):
                copy.start()

        for copy in column(c):
            copy.wait()

        def gate_step(i, _):
            tick("gate", c * blocks + i)
            n = c * blocks + i
            rows, slot = here(i, BT), lax.rem(n, 2)
            b = b_s[rows, :]
            gate, up = dot(b, wg_s[lax.rem(c, 2)]), dot(b, wu_s[lax.rem(c, 2)])

            @pl.when(n >= 2)
            def _():
                for copy in staged(n, i, c):
                    copy.wait()

            stage_s[slot, 0] = gate
            stage_s[slot, 1] = up
            for copy in staged(n, i, c):
                copy.start()
            act_s[rows, here(c, BF)] = (gate * jax.nn.sigmoid(gate) * up).astype(BF16)

        loop(blocks, gate_step)

    loop(ff // BF, gate_column)
    for slot in range(2):
        for copy in staged(slot, 0, 0):
            copy.wait()
    for c in (*kept_qkv(), *kept_o(), kept_mid()):
        c.wait()

    @pl.when(layer < layers - 1)
    def _():
        for n in range(1):
            gathers(n)["d"].arrived()
        weight("d").start()
        weight("d").wait()

        def down_step(i, _):
            tick("down", i)
            rows = here(i, BT)
            h_s[rows, :] = (h_s[rows, :].astype(F32) + rounded(dot(act_s[rows, :], wd_s[:]))).astype(BF16)

        loop(blocks, down_step)

    @pl.when(layer == layers - 1)
    def _():
        gathers(1)["d"].finish()
        gathers(1)["d"].arrived()
        for n in range(2):
            for g in gathers(n).values():
                g.sent()


PLAN = {
    (0, "qkv", 1): [("hand_on", 0, ["o"]), ("begin", 0, ["gb", "ub"])],
    (0, "attend", 0): [("hand_on", 0, ["ga", "ua"]), ("finish", 0, ["o"]), ("begin", 0, ["d"])],
    (0, "attend", 2): [("hand_on", 0, ["gb", "ub"]), ("finish", 0, ["ga", "ua"]), ("begin", 1, ["qkv", "o"])],
    (0, "attend", 3): [("hand_on", 0, ["d"])],
    (0, "out", 0): [("finish", 0, ["gb", "ub"]), ("begin", 1, ["ga", "ua"])],
    (0, "gate", 0): [("finish", 0, ["d"]), ("hand_on", 1, ["qkv", "o"])],
    (0, "gate", 4): [("begin", 1, ["gb", "ub"])],
    (0, "gate", 8): [("finish", 1, ["qkv", "o"]), ("hand_on", 1, ["ga", "ua"])],
    (0, "gate", 12): [("begin", 1, ["d"])],
    (0, "down", 0): [("finish", 1, ["ga", "ua"])],
    (1, "qkv", 0): [("hand_on", 1, ["gb", "ub"])],
    (1, "attend", 0): [("finish", 1, ["gb", "ub"])],
    (1, "attend", 2): [("hand_on", 1, ["d"])],
}


def forward(x, shards, cos, sin):
    tokens, d = x.shape
    layers = shards[0].shape[0]
    heads, ff = shards[0].shape[2] // HEAD - 2, shards[2].shape[2]
    full = [jax.ShapeDtypeStruct((layers, 8 * s.shape[1], s.shape[2]), BF16) for s in shards]
    shape = lambda *s: jax.ShapeDtypeStruct((layers, *s), BF16)
    wide = jax.ShapeDtypeStruct((layers, tokens, ff), F32)
    once = lambda a: pl.BlockSpec(a.shape, lambda i: (0,) * len(a.shape), pipeline_mode=pl.Buffered(1))
    anywhere = pl.BlockSpec(memory_space=pl.ANY)
    dma = pltpu.SemaphoreType.DMA
    outs = [*full, shape(heads, tokens, HEAD), shape(tokens, HEAD), shape(tokens, HEAD), shape(heads, tokens, HEAD),
            jax.ShapeDtypeStruct((layers, heads, tokens), F32), shape(tokens, d), wide, wide, jax.ShapeDtypeStruct((tokens, d), BF16)]
    return pl.pallas_call(
        _forward,
        grid=(layers,),
        in_specs=[anywhere] * 6 + [once(cos), once(sin)],
        out_specs=[anywhere] * len(outs),
        out_shape=outs,
        scratch_shapes=[pltpu.VMEM((tokens, d), BF16), pltpu.VMEM((tokens, d), BF16), pltpu.VMEM((heads, tokens, HEAD), BF16),
                        pltpu.VMEM((tokens, HEAD), BF16), pltpu.VMEM((tokens, HEAD), BF16), pltpu.VMEM((heads, tokens, HEAD), BF16),
                        pltpu.VMEM((heads, tokens), F32), pltpu.VMEM((tokens, ff), BF16),
                        pltpu.VMEM(full[0].shape[1:], BF16), pltpu.VMEM(full[1].shape[1:], BF16), pltpu.VMEM((2, d, BF), BF16),
                        pltpu.VMEM((2, d, BF), BF16), pltpu.VMEM(full[4].shape[1:], BF16), pltpu.VMEM((2, 2, BT, BF), F32),
                        pltpu.VMEM((heads, BQ), F32), pltpu.VMEM((heads, HEAD + 8, BQ), F32), pltpu.VMEM((BK, BQ), jnp.int32),
                        dma((layers, len(TENSORS), 9)), dma((layers, len(TENSORS), 9)), dma((5 * layers,)), dma((8,)), dma((2, 2)),
                        dma((7,))],
        compiler_params=params(collective_id=0, has_side_effects=True),
        cost_estimate=cost(4 * tokens * (7 * HEAD * 1200 + 3 * d * ff)),
        name="forward",
    )(x, *shards, cos, sin)


def act_on(plan, step, scatters, squares):
    for at, actions in plan.items():
        @pl.when(step == at)
        def _():
            for what, names in actions:
                for name in names:
                    getattr(scatters[name], what)(*([squares] if what == "last" else []))


def _mlp_back(dy_ref, mid_ref, gate_ref, up_ref, wg_ref, wu_ref, wd_ref, *rest, bt, plan):
    if plan:
        dwqkv_ref, dmid_ref, dwg_ref, dwu_ref, dwd_ref, g_ref, squares_ref, *rest = rest
    else:
        dmid_ref, dwg_ref, dwu_ref, dwd_ref, *rest = rest
    bt_s, dyt_s, db_s, dwg_s, dwu_s, dwd_s, *rest = rest
    f, t = pl.program_id(0), pl.program_id(1)
    if plan:
        me = lax.axis_index("dp")
        own, theirs, across, from_x, from_y, *sems = rest
        scatters = {"qkv": Scatter(me, dwqkv_ref, own, theirs, across, from_x, from_y, g_ref, *sems)}

        @pl.when((f == 0) & (t == 0))
        def _():
            greet(me)
            squares_ref[:] = jnp.zeros_like(squares_ref)

        act_on(plan, f * pl.num_programs(1) + t, scatters, squares_ref)
    here = pl.ds(pl.multiple_of(t * bt, bt), bt)
    dy = dy_ref[here, :]

    @pl.when(f == 0)
    def _():
        wide = mid_ref[here, :].astype(F32)
        bt_s[:, here] = (wide * norm_scale(wide)).T.astype(BF16)
        dyt_s[:, here] = dy.T

    gate, up = gate_ref[:], up_ref[:]
    dact = rounded(dot_t(dy, wd_ref[:]))
    sig = jax.nn.sigmoid(gate)
    silu = gate * sig
    act = (silu * up).astype(BF16)
    du = (dact * silu).astype(BF16)
    dg = (dact * up * (sig * (1 + gate * (1 - sig)))).astype(BF16)
    parts = ((dwd_s, dot(dyt_s[:, here], act)), (dwg_s, dot(bt_s[:, here], dg)), (dwu_s, dot(bt_s[:, here], du)))

    @pl.when(t == 0)
    def _():
        for s, part in parts:
            s[:] = part

    @pl.when(t > 0)
    def _():
        for s, part in parts:
            s[:] += part

    db = dot_t(dg, wg_ref[:]) + dot_t(du, wu_ref[:])

    @pl.when(f == 0)
    def _():
        db_s[here, :] = db

    @pl.when(f > 0)
    def _():
        db_s[here, :] += db

    @pl.when(t == pl.num_programs(1) - 1)
    def _():
        dwg_ref[:] = dwg_s[:].astype(BF16)
        dwu_ref[:] = dwu_s[:].astype(BF16)
        dwd_ref[:] = dwd_s[:].T.astype(BF16)

    @pl.when(f == pl.num_programs(0) - 1)
    def _():
        wide = mid_ref[here, :].astype(F32)
        dmid_ref[here, :] = (dy.astype(F32) + norm_back(wide, rounded(db_s[here, :]))).astype(BF16)


def mlp_back(layer, dy, mid, gate, up, wg, wu, wd, dwqkv=None, bt=512, bf=512):
    tokens, d = dy.shape
    ff = wg.shape[2]
    one = pl.Buffered(1)
    pair = pl.BlockSpec((None, bt, bf), lambda f, t: (layer, t, f))
    column, row = pl.BlockSpec((None, d, bf), lambda f, t: (layer, 0, f)), pl.BlockSpec((None, bf, d), lambda f, t: (layer, f, 0))
    states = pl.BlockSpec((tokens, d), lambda f, t: (0, 0), pipeline_mode=one)
    column_out, row_out = pl.BlockSpec((d, bf), lambda f, t: (0, f)), pl.BlockSpec((bf, d), lambda f, t: (f, 0))
    out = lambda *s: jax.ShapeDtypeStruct(s, BF16)
    more_in, more_out, more_shapes, more_scratch, more_args, plan = [], [], [], [], [], {}
    if dwqkv is not None:
        r, n = dwqkv.shape[0] // 8, dwqkv.shape[1]
        plan = {0: [("exchange", ["qkv"])], 2: [("first", ["qkv"])], 5: [("second", ["qkv"])], 8: [("last", ["qkv"])],
                12: [("done", ["qkv"])]}
        more_in, more_args = [pl.BlockSpec(memory_space=pl.ANY)], [dwqkv]
        more_out, more_shapes = [pl.BlockSpec(memory_space=pl.ANY), whole(8, 128)], [out(r, n), jax.ShapeDtypeStruct((8, 128), F32)]
        more_scratch = scatter_scratch(r, n)
    return pl.pallas_call(
        functools.partial(_mlp_back, bt=bt, plan=plan),
        grid=(ff // bf, tokens // bt),
        in_specs=[states, pl.BlockSpec((None, tokens, d), lambda f, t: (layer, 0, 0), pipeline_mode=one), pair, pair, column, column, row,
                  *more_in],
        out_specs=[whole(tokens, d), column_out, column_out, row_out, *more_out],
        out_shape=[out(tokens, d), out(d, ff), out(d, ff), out(ff, d), *more_shapes],
        scratch_shapes=[pltpu.VMEM((d, tokens), BF16), pltpu.VMEM((d, tokens), BF16), pltpu.VMEM((tokens, d), F32),
                        *[pltpu.VMEM((d, bf), F32)] * 3, *more_scratch],
        compiler_params=params(collective_id=1, has_side_effects=True) if plan else params(),
        cost_estimate=cost(12 * tokens * d * ff, exps=tokens * ff),
        name="mlp_back",
    )(dy, mid, gate, up, wg, wu, wd, *more_args)


BACK_PLAN = {
    0: [("exchange", ["g", "u", "d"])],
    4: [("first", ["g"])],
    6: [("first", ["u"])],
    8: [("first", ["d"]), ("exchange", ["o"])],
    10: [("second", ["g"]), ("first", ["o"])],
    11: [("second", ["u"])],
    12: [("second", ["d"])],
    13: [("last", ["g"])],
    14: [("second", ["o"])],
    15: [("last", ["u"])],
    16: [("last", ["d"])],
    20: [("last", ["o"])],
    23: [("done", ["g", "u", "d", "o"])],
}


def _attention_back(dmid_ref, o_ref, q_ref, k_ref, v_ref, lse_ref, h_ref, wo_ref, wqkv_ref, cos_ref, sin_ref, dwg_ref, dwu_ref, dwd_ref,
                    dh_ref, dwqkv_ref, gg_ref, gu_ref, gd_ref, go_ref, squares_ref,
                    do_s, dq_s, delta_s, dwo_s, dwob_s, dwqkv_s, dqt_s, dk_s, dv_s, gap_s, *rest, bq, bk):
    me = lax.axis_index("dp")
    step = pl.program_id(0)
    heads = q_ref.shape[0]
    n = pl.num_programs(0) // 3
    sized = {"g": rest[:8], "u": rest[8:16], "d": rest[16:24]}
    scatters = {name: Scatter(me, src, *sized[name][:5], out, *sized[name][5:])
                for name, src, out in (("g", dwg_ref, gg_ref), ("u", dwu_ref, gu_ref), ("d", dwd_ref, gd_ref))}
    scatters["o"] = Scatter(me, dwob_s, None, *rest[24:28], go_ref, *rest[28:])

    @pl.when(step == 0)
    def _():
        greet(me)
        squares_ref[:] = jnp.zeros_like(squares_ref)
        dwo_s[:] = jnp.zeros_like(dwo_s)
        dwqkv_s[:] = jnp.zeros_like(dwqkv_s)
        dk_s[:] = jnp.zeros_like(dk_s)
        dv_s[:] = jnp.zeros_like(dv_s)
        gap_s[:] = gap(bk, bq, bq)

    act_on(BACK_PLAN, step, scatters, squares_ref)

    @pl.when(step < n)
    def _():
        rows = pl.ds(pl.multiple_of(step * bq, bq), bq)
        dmid = dmid_ref[:]
        do = dot_t(dmid, wo_ref[:]).astype(BF16)
        for i in range(heads):
            mine = do[:, i * HEAD : (i + 1) * HEAD]
            do_s[i, rows, :] = mine
            delta_s[i : i + 1, rows] = jnp.sum((mine.astype(F32) * o_ref[i].astype(F32)).T, axis=0, keepdims=True)
        dwo_s[:] += dot(side_by_side(o_ref).T, dmid)

        @pl.when(step == n - 1)
        def _():
            dwob_s[:] = dwo_s[:].astype(BF16)

    @pl.when((step >= n) & (step < 2 * n))
    def _():
        iq = step - n
        rows = pl.ds(pl.multiple_of(iq * bq, bq), bq)
        scale = HEAD**-0.5
        e = scale * LOG2E
        dqt_s[:] = jnp.zeros_like(dqt_s)

        def block(j, masked=False):
            keys = pl.ds(pl.multiple_of(j * bk, bk), bk)
            qs, dos = [q_ref[i] for i in range(heads)], [do_s[i, rows, :] for i in range(heads)]
            scores = [dot_t(k_ref[keys, :], x) for x in qs]
            dps = [dot_t(v_ref[keys, :], x) for x in dos]
            for i in range(heads):
                p = jnp.exp2(scores[i] * e - lse_ref[i : i + 1, :] * LOG2E)
                if masked:
                    p = jnp.where(gap_s[:] >= j * bk - iq * bq, p, 0.0)
                ds = (p * (dps[i] - delta_s[i : i + 1, rows])).astype(BF16)
                dv_s[keys, :] += dot(p.astype(BF16), dos[i])
                dk_s[keys, :] += dot(ds, qs[i])
                dqt_s[i] += dot(k_ref[keys, :].T, ds)

        seen_whole = lax.div(iq * bq + 1, bk)
        seen = lax.div(iq * bq + bq - 1 + bk, bk)
        loop(seen_whole, lambda j, _: block(j))
        loop(seen, lambda j, _: block(j, masked=True), seen_whole)
        for i in range(heads):
            dq_s[i, rows, :] = (dqt_s[i] * scale).T.astype(BF16)

    @pl.when(step >= 2 * n)
    def _():
        rows = pl.ds(pl.multiple_of((step - 2 * n) * bq, bq), bq)
        cos, sin = cos_ref[:], sin_ref[:]
        parts = []
        for t in [*(dq_s[i, rows, :] for i in range(heads)), (dk_s[rows, :] * HEAD**-0.5).astype(BF16)]:
            t = t.astype(F32)
            parts.append((t * cos - pltpu.roll(t, HALF, 1) * sin).astype(BF16))
        dz = jnp.concatenate([*parts, dv_s[rows, :].astype(BF16)], axis=1)
        wide = h_ref[:].astype(F32)
        a = (wide * norm_scale(wide)).T.astype(BF16)
        dwqkv_s[:] += dot(a, dz)
        da = rounded(dot_t(dz, wqkv_ref[:]))
        dh_ref[:] = (dmid_ref[:].astype(F32) + norm_back(wide, da)).astype(BF16)

        @pl.when(step == 3 * n - 1)
        def _():
            dwqkv_ref[:] = dwqkv_s[:].astype(BF16)


def attention_back(layer, dmid, o, q, k, v, lse, h, wo, wqkv, cos, sin, dwg, dwu, dwd, bq=256, bk=512):
    tokens, d = dmid.shape
    heads = o.shape[1]
    n = tokens // bq
    one = pl.Buffered(1)
    early = lambda s: jnp.minimum(s, n - 1)
    middle = lambda s: jnp.clip(s - n, 0, n - 1)
    late = lambda s: jnp.maximum(s - 2 * n, 0)
    twice = lambda s: jnp.where(s < n, s, jnp.maximum(s - 2 * n, 0))
    rows = lambda w, which: pl.BlockSpec((bq, w), lambda s: (which(s), 0))
    by_head = lambda which: pl.BlockSpec((None, heads, bq, HEAD), lambda s: (layer, 0, which(s), 0))
    all_of = lambda a: pl.BlockSpec((None, *a.shape[1:]), lambda s: (layer, 0, 0), pipeline_mode=one)
    anywhere = pl.BlockSpec(memory_space=pl.ANY)
    cuts = [(a.shape[0] // 8, a.shape[1]) for a in (dwg, dwu, dwd)]
    cut_o = (wo.shape[1] // 8, wo.shape[2])
    out = lambda s: jax.ShapeDtypeStruct(s, BF16)
    flops = 4 * tokens * d * (d + wqkv.shape[2]) + 5 * heads * tokens * tokens * HEAD
    return pl.pallas_call(
        functools.partial(_attention_back, bq=bq, bk=bk),
        grid=(3 * n,),
        in_specs=[rows(d, twice), by_head(early), by_head(middle), all_of(k), all_of(v),
                  pl.BlockSpec((None, heads, bq), lambda s: (layer, 0, middle(s))), rows(d, late), all_of(wo), all_of(wqkv),
                  rows(HEAD, late), rows(HEAD, late), anywhere, anywhere, anywhere],
        out_specs=[rows(d, late), whole(*wqkv.shape[1:]), *[anywhere] * 4, whole(8, 128)],
        out_shape=[out((tokens, d)), out(wqkv.shape[1:]), *(out(c) for c in cuts), out(cut_o), jax.ShapeDtypeStruct((8, 128), F32)],
        scratch_shapes=[pltpu.VMEM((heads, tokens, HEAD), BF16), pltpu.VMEM((heads, tokens, HEAD), BF16), pltpu.VMEM((heads, tokens), F32),
                        pltpu.VMEM(wo.shape[1:], F32), pltpu.VMEM(wo.shape[1:], BF16), pltpu.VMEM(wqkv.shape[1:], F32),
                        pltpu.VMEM((heads, HEAD, bq), F32), pltpu.VMEM((tokens, HEAD), F32), pltpu.VMEM((tokens, HEAD), F32),
                        pltpu.VMEM((bk, bq), jnp.int32), *(s for c in cuts for s in scatter_scratch(*c)),
                        *scatter_scratch(*cut_o, in_vmem=True)],
        compiler_params=params(collective_id=2 + layer, has_side_effects=True),
        cost_estimate=cost(flops, exps=heads * tokens * tokens // 2),
        name="attention_back",
    )(dmid, o, q, k, v, lse, h, wo, wqkv, cos, sin, dwg, dwu, dwd)


def _finish(dwqkv_ref, *rest, known, count):
    squares_refs, (g_ref, factor_ref, own, theirs, across, from_x, from_y, send, recv, local, all_s, total_s, send_all, recv_all) = \
        rest[:known], rest[known:]
    me = lax.axis_index("dp")
    barrier = pltpu.get_barrier_semaphore()
    for bits in range(1, 8):
        pl.semaphore_signal(barrier, inc=1, device_id=(0, flip(me, bits)), device_id_type=pl.DeviceIdType.MESH)
    pl.semaphore_wait(barrier, 7)
    total_s[:] = jnp.zeros_like(total_s)
    for ref in squares_refs:
        total_s[:] += ref[:]
    scatter = Scatter(me, dwqkv_ref, own, theirs, across, from_x, from_y, g_ref, send, recv, local)
    scatter.exchange()
    scatter.first()
    scatter.second()
    scatter.last(total_s)
    copies = [pltpu.make_async_remote_copy(src_ref=total_s, dst_ref=all_s.at[bits], send_sem=send_all.at[bits], recv_sem=recv_all.at[bits],
                                           device_id=(0, flip(me, bits)), device_id_type=pl.DeviceIdType.MESH) for bits in range(1, 8)]
    for c in copies:
        c.start()
    for c in copies:
        c.wait_recv()
    tiles = [total_s[:], *(all_s[bits] for bits in range(1, 8))]
    tiles = [jnp.sum(t) for t in tiles]
    while len(tiles) > 1:
        tiles = [a + b for a, b in zip(tiles[::2], tiles[1::2])]
    factor_ref[:] = jnp.full((8, 128), jnp.minimum(1.0, 0.5 * lax.rsqrt(jnp.full((8, 128), tiles[0] / count) + 1e-30)), F32)
    for c in copies:
        c.wait_send()
    scatter.done()


def finish(dwqkv, squares, count):
    r, n = dwqkv.shape[0] // 8, dwqkv.shape[1]
    dma = pltpu.SemaphoreType.DMA
    anywhere = pl.BlockSpec(memory_space=pl.ANY)
    return pl.pallas_call(
        functools.partial(_finish, known=len(squares), count=count),
        in_specs=[anywhere] + [pl.BlockSpec(memory_space=pltpu.VMEM)] * len(squares),
        out_specs=[anywhere, pl.BlockSpec(memory_space=pltpu.VMEM)],
        out_shape=[jax.ShapeDtypeStruct((r, n), BF16), jax.ShapeDtypeStruct((8, 128), F32)],
        scratch_shapes=[*scatter_scratch(r, n), pltpu.VMEM((8, 8, 128), F32), pltpu.VMEM((8, 128), F32), dma((8,)), dma((8,))],
        compiler_params=pltpu.CompilerParams(collective_id=4, has_side_effects=True, vmem_limit_bytes=8 * 2**20),
        name="finish",
    )(dwqkv, *squares)


def adamw(w, m, v, g):
    m = 0.9 * m + 0.1 * g
    v = 0.95 * v + 0.05 * g * g
    step = m * lax.rsqrt(v + 1e-8) + 0.1 * w
    return (w - 0.02 * step).astype(BF16), m, v


def solution(mesh):
    def step(x, dy, *arrays):
        weights, m, v = (arrays[i : i + 7] for i in (0, 7, 14))
        tokens, d = x.shape[1:]
        cos, sin = tables(tokens)
        shards = [jnp.concatenate(weights[:3], axis=2), *weights[3:]]
        fqkv, fo, fg, fu, fd, q, k, v_, o, lse, mid, gate, up, h1 = forward(x[0], shards, cos, sin)
        dmid, dwg, dwu, dwd = mlp_back(1, dy[0], mid, gate, up, fg, fu, fd)
        dh, dwqkv, g1, u1, d1, o1, s1 = attention_back(1, dmid, o, q, k, v_, lse, h1, fo, fqkv, cos, sin, dwg, dwu, dwd)
        dmid, dwg, dwu, dwd, qkv1, s2 = mlp_back(0, dh, mid, gate, up, fg, fu, fd, dwqkv)
        _, dwqkv, g0, u0, d0, o0, s3 = attention_back(0, dmid, o, q, k, v_, lse, x[0], fo, fqkv, cos, sin, dwg, dwu, dwd)
        qkv0, factor = finish(dwqkv, [s1, s2, s3], 8 * sum(w.size for w in weights))
        factor = factor[0, 0]
        split = lambda a: [a[:, :d], a[:, d : d + HEAD], a[:, d + HEAD :]]
        mine = [[*split(qkv0), o0, g0, u0, d0], [*split(qkv1), o1, g1, u1, d1]]
        gradients = [jnp.stack([one[i] for one in mine]).astype(F32) for i in range(7)]
        new = [adamw(w.astype(F32), m, v, g * factor) for w, m, v, g in zip(weights, m, v, gradients, strict=True)]
        return tuple(one[which] for which in range(3) for one in new)

    states, cut = P(("rep", "dp"), None, None), P(None, "dp", None)
    return jax.shard_map(
        step,
        mesh=mesh,
        in_specs=(states, states) + (cut,) * 21,
        out_specs=(P("rep", "dp", None),) * 21,
        check_vma=False,
    )
```

```python
import functools

import jax
import jax.numpy as jnp
import numpy as np
from jax import lax
from jax.experimental import pallas as pl
from jax.experimental.pallas import tpu as pltpu
from jax.sharding import PartitionSpec as P

NEG = -1e30
HIDDEN = 2 * NEG
LOG2E = 1.4426950408889634
VMEM = 127 * 2**19
STRIP = 512
HEAD = 128
HALF = HEAD // 2
THETA = 10000
F32, BF16 = jnp.float32, jnp.bfloat16


def dot(a, b, ca=1, cb=0):
    return lax.dot_general(a, b, (((ca,), (cb,)), ((), ())), preferred_element_type=F32)


def dot_t(a, b):
    return dot(a, b, 1, 1)


def loop(stop, body, start=0):
    lax.fori_loop(start, stop, body, None)


def rounded(a):
    return a.astype(BF16).astype(F32)


def norm_scale(wide):
    return lax.rsqrt(jnp.mean(wide * wide, -1, keepdims=True) + 1e-6)


def norm_back(wide, by):
    scale = norm_scale(wide)
    return scale * (by - wide * (scale * scale * jnp.mean(by * wide, -1, keepdims=True)))


def params(**more):
    return pltpu.CompilerParams(vmem_limit_bytes=VMEM, **more)


def whole(*shape):
    return pl.BlockSpec(shape, lambda *_: (0,) * len(shape))


def cost(flops, nbytes=0, exps=0):
    return pl.CostEstimate(flops=int(flops), bytes_accessed=int(nbytes), transcendentals=int(exps))


def tables(tokens):
    angle = np.arange(tokens, dtype=np.float64)[:, None] * THETA ** (-np.arange(HALF, dtype=np.float64) / HALF)
    cos, sin = np.cos(angle), np.sin(angle)
    return jnp.asarray(np.concatenate([cos, cos], 1), F32), jnp.asarray(np.concatenate([-sin, sin], 1), F32)


def hidden(keys, queries, later=0):
    gap = lax.broadcasted_iota(jnp.int32, (keys, queries), 1) - lax.broadcasted_iota(jnp.int32, (keys, queries), 0)
    return jnp.where(gap + later >= 0, 0.0, HIDDEN)


def side_by_side(ref):
    return jnp.concatenate([ref[n] for n in range(ref.shape[0])], axis=1)


X, Y, CORE, HERE = 4, 2, 1, 0
NEAR = (HERE, X, Y, X + Y)


def places():
    at = [lax.axis_index("dp")]
    for bit in (CORE, Y, X):
        at += [n + bit - 2 * bit * lax.rem(lax.div(n, bit), 2) for n in at]
    return at


def greet(me, all_of=(X, Y, CORE)):
    barrier = pltpu.get_barrier_semaphore()
    for bits in all_of:
        pl.semaphore_signal(barrier, inc=1, device_id=(0, me[bits]), device_id_type=pl.DeviceIdType.MESH)
    return lambda: pl.semaphore_wait(barrier, len(all_of))


def remote(me, bit, src, dst, send, recv):
    return pltpu.make_async_remote_copy(src_ref=src, dst_ref=dst, send_sem=send, recv_sem=recv, device_id=(0, me[bit]),
                                        device_id_type=pl.DeviceIdType.MESH)


def halves(r):
    a = (r // 2 + 15) // 16 * 16
    return (0, a), (a, r - a)


def upper(r):
    return halves(r)[0]


def lower(r):
    return halves(r)[1]


ALL = None
ROUTES = {"x": (X, HERE, ALL), "y": (Y, HERE, ALL), "core": (CORE, HERE, ALL), "xy": (Y, X, upper), "x core": (CORE, X, ALL),
          "yx": (X, Y, lower), "y core": (CORE, Y, ALL), "xy core": (CORE, X + Y, upper), "yx core": (CORE, X + Y, lower)}


class Gather:
    def __init__(self, me, block, full, send, recv, cols, at):
        first, count = cols
        self.me, self.r = me, block.shape[0]
        self.full, self.send, self.recv = full, send, recv
        self.own, self.cols = block.at[:, pl.ds(first, count)], pl.ds(at + first, count)

    def rows(self, bits, part=None):
        first, count = part or (0, self.r)
        at = pl.multiple_of(self.me[bits] * self.r + first, 16)
        return self.full.at[pl.ds(at, count), self.cols]

    def copy(self, which, got=False):
        bit, bits, part = ROUTES[which]
        there = self.rows(bits + bit if got else bits, part and part(self.r))
        n = tuple(ROUTES).index(which)
        return remote(self.me, bit, self.own if bits == HERE and not got else there, there, self.send.at[n], self.recv.at[n])

    def got(self, which):
        self.copy(which, got=True).wait_recv()

    def begin(self):
        for n in ("x", "y", "core"):
            self.copy(n).start()

    def hand_on(self):
        self.got("x")
        self.copy("xy").start()
        self.copy("x core").start()
        self.got("y")
        self.copy("yx").start()
        self.copy("y core").start()

    def finish(self):
        self.got("xy")
        self.copy("xy core").start()
        self.got("yx")
        self.copy("yx core").start()

    def arrived(self):
        for n in ("core", "x core", "y core", "xy core", "yx core"):
            self.got(n)

    def sent(self):
        for n in ROUTES:
            self.copy(n).wait_send()


class Scatter:
    def __init__(self, me, src, mine, theirs, across, from_x, from_y, out, send, recv, local):
        self.me, self.src, self.out = me, src, out
        self.r, self.n = theirs.shape[1:]
        self.own, self.theirs, self.across, self.from_x, self.from_y = mine, theirs, across, from_x, from_y
        self.send, self.recv, self.local = send, recv, local
        self.a, self.b = halves(self.r)
        self.all = (0, self.r)

    def block(self, bits, part=None):
        first, count = part or self.all
        return self.src.at[pl.ds(pl.multiple_of(self.me[bits] * self.r + first, 16), count)]

    def mine(self, j, part):
        return self.block(NEAR[j], part) if self.own is None else self.own.at[j, pl.ds(*part)]

    def load(self, j):
        return pltpu.make_async_copy(self.block(NEAR[j]), self.own.at[j], self.local.at[j])

    def copy(self, n):
        if n < 4:
            bit, src, dst = CORE, self.block(CORE + NEAR[n]), self.theirs.at[n]
        else:
            bit, j, part, to = ((X, 3, self.a, self.across), (Y, 3, self.b, self.across), (X, 1, self.a, self.from_x),
                                (Y, 2, self.b, self.from_y), (Y, 2, self.a, self.from_y), (X, 1, self.b, self.from_x))[n - 4]
            src, dst = self.mine(j, part), to.at[pl.ds(*part)]
        return remote(self.me, bit, src, dst, self.send.at[n], self.recv.at[n])

    def add(self, j, part, *more):
        step = 16
        ref = self.mine(j, part)

        def one(i, _):
            rows = pl.ds(pl.multiple_of(i * step, step), step)
            full = pl.ds(pl.multiple_of(part[0] + i * step, step), step)
            total = ref[rows, :].astype(F32) + self.theirs[j, full, :].astype(F32)
            for other in more:
                total += other[full, :].astype(F32)
            ref[rows, :] = total.astype(BF16)

        loop(part[1] // step, one)

    def exchange(self):
        for j in range(4):
            self.copy(j).start()
            if self.own is not None:
                self.load(j).start()

    def first(self):
        for j in range(4):
            if self.own is not None:
                self.load(j).wait()
            self.copy(j).wait_recv()
        self.add(3, self.all)
        self.copy(4).start()
        self.copy(5).start()
        self.add(1, self.a)
        self.add(2, self.b)

    def second(self):
        self.copy(6).start()
        self.copy(7).start()
        self.copy(4).wait_recv()
        self.add(2, self.a, self.across)
        self.copy(8).start()
        self.copy(5).wait_recv()
        self.add(1, self.b, self.across)
        self.copy(9).start()

    def result(self):
        return pltpu.make_async_copy(self.mine(0, self.all), self.out, self.local.at[4])

    def last(self, squares):
        for n in range(6, 10):
            self.copy(n).wait_recv()
        self.add(0, self.all, self.from_x, self.from_y)
        ref = self.mine(0, self.all)
        self.result().start()
        squares[:] += sum_of_squares(ref)

    def done(self):
        for n in range(10):
            self.copy(n).wait_send()
        self.result().wait()


def sum_of_squares(ref):
    rows, cols = ref.shape

    def one(i, total):
        g = ref[pl.ds(pl.multiple_of(i * 16, 16), 16), :].astype(F32)
        g = g * g
        for c in range(0, cols, 128):
            total += g[:8, c : c + 128] + g[8:, c : c + 128]
        return total

    return lax.fori_loop(0, rows // 16, one, jnp.zeros((8, 128), F32))


def scatter_scratch(r, n, in_vmem=False):
    dma = pltpu.SemaphoreType.DMA
    block = pltpu.VMEM((r, n), BF16)
    return [*([] if in_vmem else [pltpu.VMEM((4, r, n), BF16)]), pltpu.VMEM((4, r, n), BF16), block, block, block,
            dma((10,)), dma((10,)), dma((5,))]


BQ = BK = BT = BF = 512
CUT, CUT_Q = 2 * BF, 4 * HEAD
TENSORS = ("qa", "qb", "k", "v", "o", "ga", "ua", "gb", "ub", "d")
QKV, GU_A, GU_B = ["qa", "k", "v", "qb"], ["ga", "ua"], ["gb", "ub"]


def _forward(x_ref, sq, sk, sv, so, sg, su, sd, cos_ref, sin_ref, fqkv, fo, fg, fu, fd, q_o, k_o, v_o, o_o, lse_o, mid_o, gate_o, up_o, h_o,
             h_s, b_s, q_s, k_s, v_s, o_s, lse_s, act_s, wqkv_s, wo_s, wg_s, wu_s, wd_s, stage_s, top_s, mix_s, hide_s,
             send, recv, load, keep, out, wsem):
    layer, layers = pl.program_id(0), pl.num_programs(0)
    me = places()
    tokens, d = h_s.shape
    heads = q_s.shape[0]
    ff = act_s.shape[1]
    blocks = tokens // BT

    def gather(n, name):
        i = TENSORS.index(name)
        shard, full, cols, at = {
            "qa": (sq, fqkv, (0, CUT_Q), 0), "qb": (sq, fqkv, (CUT_Q, d - CUT_Q), 0), "k": (sk, fqkv, (0, HEAD), d),
            "v": (sv, fqkv, (0, HEAD), d + HEAD), "o": (so, fo, (0, d), 0), "d": (sd, fd, (0, d), 0),
            "ga": (sg, fg, (0, CUT), 0), "gb": (sg, fg, (CUT, ff - CUT), 0),
            "ua": (su, fu, (0, CUT), 0), "ub": (su, fu, (CUT, ff - CUT), 0)}[name]
        full = wqkv_s if name in QKV and n == 0 else full.at[n]
        return Gather(me, shard.at[n], full, send.at[n, i], recv.at[n, i], cols, at)

    def own_blocks():
        at = 0
        for s, f, column in ((sq, fqkv, 0), (sk, fqkv, d), (sv, fqkv, d + HEAD), (so, fo, 0), (sg, fg, 0), (su, fu, 0), (sd, fd, 0)):
            r, n = s.shape[1:]
            for i in range(s.shape[0]):
                where = pl.ds(pl.multiple_of(me[HERE] * r, 16), r), pl.ds(column, n)
                if f is fqkv and i == 0:
                    yield s.at[i], wqkv_s.at[where], None
                else:
                    yield s.at[i], act_s.at[pl.ds(at, r), pl.ds(0, n)], f.at[i, *where]
                    at += r

    copies_in = lambda: [pltpu.make_async_copy(a, b, load.at[i]) for i, (a, b, _) in enumerate(own_blocks())]
    copies_out = lambda: [pltpu.make_async_copy(b, c, load.at[i]) for i, (_, b, c) in enumerate(own_blocks()) if c is not None]
    here = lambda i, n: pl.ds(pl.multiple_of(i * n, n), n)

    def kept(*names):
        pairs = {"x": (x_ref, h_s), "q": (q_s, q_o.at[layer]), "k": (k_s, k_o.at[layer]), "v": (v_s, v_o.at[layer]), "o": (o_s, o_o.at[layer]),
                 "lse": (lse_s, lse_o.at[layer]), "mid": (h_s, mid_o.at[layer]), "h": (h_s, h_o), "qkv": (wqkv_s, fqkv.at[layer])}
        return [pltpu.make_async_copy(*pairs[n], keep.at[list(pairs).index(n)]) for n in names]

    def start(*copies):
        for c in copies:
            c.start()

    def wait(*copies):
        for c in copies:
            c.wait()

    def weight(n, name):
        return pltpu.make_async_copy(*{"qb": (fqkv.at[n], wqkv_s, wsem.at[0]), "o": (fo.at[n], wo_s, wsem.at[1]),
                                       "d": (fd.at[n], wd_s, wsem.at[2])}[name])

    def column(c, n=layer):
        cols, slot = here(c, BF), lax.rem(c, 2)
        return (pltpu.make_async_copy(fg.at[n, :, cols], wg_s.at[slot], wsem.at[3 + slot]),
                pltpu.make_async_copy(fu.at[n, :, cols], wu_s.at[slot], wsem.at[5 + slot]))

    def fetch(n, name):
        gather(n, name).arrived()
        if name in QKV:
            gather(0, name).sent()
        if name == "ua":
            start(*column(0, n))
        elif name in ("qb", "o", "d"):
            start(weight(n, name))

    def tick(phase, i):
        for n, plan in enumerate(PLAN):
            for p, k, *actions in plan:
                if p == phase:
                    @pl.when((layer == n) & (i == k))
                    def _():
                        for do, later, names in actions:
                            for name in names:
                                if do == "fetch":
                                    fetch(n + later, name)
                                else:
                                    getattr(gather(n + later, name), do)()

    @pl.when(layer == 0)
    def _():
        greeted = greet(me)
        start(*kept("x"), *copies_in())
        hide_s[:] = hidden(BK, BQ)
        greeted()
        for name in QKV:
            gather(0, name).begin()
        wait(*copies_in())
        start(*copies_out())
        wait(*kept("x"))
        for name in QKV:
            gather(0, name).hand_on()
        for name in ("o", *GU_A):
            gather(0, name).begin()
        wait(*copies_out())
        for do in (Gather.finish, Gather.arrived):
            for name in QKV:
                do(gather(0, name))

    @pl.when(layer > 0)
    def _():
        start(*kept("h"))
        wait(weight(1, "qb"))

    def qkv_step(i):
        tick("qkv", i)
        rows = here(i, BT)
        wide = h_s[rows, :].astype(F32)
        a = (wide * norm_scale(wide)).astype(BF16)
        z = dot(a, wqkv_s[:])
        cos, sin = cos_ref[rows, :], sin_ref[rows, :]
        for n in range(heads + 1):
            t = rounded(z[:, n * HEAD : (n + 1) * HEAD])
            t = (t * cos + pltpu.roll(t, HALF, 1) * sin).astype(BF16)
            if n < heads:
                q_s[n, rows, :] = t
            else:
                k_s[rows, :] = t
        v_s[rows, :] = z[:, (heads + 1) * HEAD :].astype(BF16)

    pairwise(blocks, qkv_step)
    start(*kept("q", "k", "v"))

    @pl.when(layer == 0)
    def _():
        start(*kept("qkv"))

    scale = HEAD**-0.5
    e = scale * LOG2E

    def attend_step(i, _):
        top_s[:] = jnp.full(top_s.shape, NEG, F32)
        mix_s[:] = jnp.zeros(mix_s.shape, F32)

        def block(first, count, at=0, hidden=None):
            keys, cols = pl.ds(pl.multiple_of(first, BK // 2), count), pl.ds(at, BQ - at)
            rows = pl.ds(pl.multiple_of(i * BQ + at, BQ // 2), BQ - at)
            values = jnp.concatenate([v_s[keys, :].T, jnp.ones((8, count), BF16)], axis=0)
            scores = [dot_t(k_s[keys, :], q_s[n, rows, :]) for n in range(heads)]
            weights = []
            for n, s in enumerate(scores):
                s = s if hidden is None else s + hidden
                old = top_s[n : n + 1, cols]
                top = jnp.maximum(old, s.max(axis=0, keepdims=True))
                top_s[n : n + 1, cols] = top
                weights.append((jnp.exp2((s - top) * e).astype(BF16), jnp.exp2((old - top) * e)))
            for n, (p, rest) in enumerate(weights):
                mix_s[n, :, cols] = mix_s[n, :, cols] * rest + dot(values, p)

        def before(j, _):
            tick("attend", lax.div(i * (i + 1), 2) + j)
            block(j * BK, BK)

        loop(i, before)
        tick("attend", lax.div(i * (i + 3), 2))
        half = BK // 2
        block(i * BK, half, hidden=hide_s[:half, :])
        block(i * BK + half, half, half, hide_s[half:, half:])
        rows = here(i, BQ)
        for n in range(heads):
            total = mix_s[n, HEAD : HEAD + 1, :]
            o_s[n, rows, :] = (mix_s[n, :HEAD, :] * (1 / total)).T.astype(BF16)
            lse_s[n : n + 1, rows] = top_s[n : n + 1, :] * scale + jnp.log(total)

    loop(tokens // BQ, attend_step)
    start(*kept("o", "lse"))

    @pl.when(layer == 0)
    def _():
        wait(*kept("qkv"))

    @pl.when(layer > 0)
    def _():
        wait(*kept("h"))

    wait(weight(layer, "o"))

    def out_step(i):
        tick("out", i)
        rows = here(i, BT)
        o = jnp.concatenate([o_s[n, rows, :] for n in range(heads)], axis=1)
        mid = (h_s[rows, :].astype(F32) + rounded(dot(o, wo_s[:]))).astype(BF16)
        h_s[rows, :] = mid
        wide = mid.astype(F32)
        b_s[rows, :] = (wide * norm_scale(wide)).astype(BF16)

    pairwise(blocks, out_step)
    start(*kept("mid"))

    def staged(slot, i, c):
        rows, cols = here(i, BT), here(c, BF)
        return [pltpu.make_async_copy(stage_s.at[slot, w], ref.at[layer, rows, cols], out.at[slot, w])
                for w, ref in enumerate((gate_o, up_o))]

    def gate_column(c, _):
        wait(*column(c))

        def gate_step(i):
            tick("gate", c * blocks + i)
            rows, slot = here(i, BT), i % 2

            @pl.when((i == blocks // 2) & (c + 1 < ff // BF))
            def _():
                start(*column(c + 1))

            @pl.when((layer > 0) | (c > 0) | (i >= 2))
            def _():
                wait(*staged(slot, i, c))

            b = b_s[rows, :]
            gate, up = dot(b, wg_s[lax.rem(c, 2)]), dot(b, wu_s[lax.rem(c, 2)])
            stage_s[slot, 0] = gate
            stage_s[slot, 1] = up
            act_s[rows, here(c, BF)] = (gate * jax.nn.sigmoid(gate) * up).astype(BF16)
            start(*staged(slot, i, c))

        for i in range(blocks):
            gate_step(i)

    loop(ff // BF, gate_column)
    wait(*kept("q", "k", "v", "o", "lse", "mid"))

    @pl.when(layer < layers - 1)
    def _():
        wait(weight(0, "d"))

        def down_step(i):
            tick("down", i)
            rows = here(i, BT)
            h_s[rows, :] = (h_s[rows, :].astype(F32) + rounded(dot(act_s[rows, :], wd_s[:]))).astype(BF16)

        pairwise(blocks, down_step)

    @pl.when(layer == layers - 1)
    def _():
        gather(1, "d").arrived()
        for slot in range(2):
            wait(*staged(slot, 0, 0))
        for n in range(2):
            for name in TENSORS:
                if name not in QKV or n > 0:
                    gather(n, name).sent()


def pairwise(count, body):
    def two(i, _):
        body(2 * i)
        body(2 * i + 1)

    loop(count // 2, two)


THIS, NEXT = range(2)
PLAN = ([
    ("qkv", 2, ("hand_on", THIS, ["o"]), ("begin", THIS, GU_B)),
    ("attend", 3, ("hand_on", THIS, GU_A), ("finish", THIS, ["o"])),
    ("attend", 8, ("fetch", THIS, ["o"])),
    ("attend", 9, ("hand_on", THIS, GU_B), ("begin", THIS, ["d"])),
    ("out", 2, ("finish", THIS, GU_A)),
    ("out", 3, ("fetch", THIS, GU_A)),
    ("gate", 3, ("finish", THIS, GU_B)),
    ("gate", 6, ("fetch", THIS, GU_B)),
    ("gate", 10, ("hand_on", THIS, ["d"]), ("begin", NEXT, QKV)),
    ("gate", 16, ("finish", THIS, ["d"])),
    ("gate", 17, ("fetch", THIS, ["d"])),
    ("gate", 18, ("hand_on", NEXT, QKV), ("begin", NEXT, ["o", *GU_A])),
    ("down", 2, ("finish", NEXT, QKV), ("hand_on", NEXT, ["o"]), ("begin", NEXT, GU_B)),
    ("down", 3, ("fetch", NEXT, QKV)),
], [
    ("qkv", 1, ("finish", THIS, ["o"]), ("hand_on", THIS, GU_A), ("begin", THIS, ["d"])),
    ("attend", 4, ("hand_on", THIS, GU_B)),
    ("attend", 6, ("finish", THIS, GU_A)),
    ("attend", 7, ("fetch", THIS, ["o"])),
    ("out", 2, ("fetch", THIS, GU_A)),
    ("out", 3, ("hand_on", THIS, ["d"])),
    ("gate", 2, ("finish", THIS, GU_B)),
    ("gate", 5, ("fetch", THIS, GU_B)),
    ("gate", 10, ("finish", THIS, ["d"])),
])


def forward(x, shards, cos, sin):
    tokens, d = x.shape
    layers = shards[0].shape[0]
    heads, ff = d // HEAD, shards[4].shape[2]
    full = [jax.ShapeDtypeStruct((layers, *s), BF16) for s in ((d, d + 2 * HEAD), (d, d), (d, ff), (d, ff), (ff, d))]
    shape = lambda *s: jax.ShapeDtypeStruct((layers, *s), BF16)
    wide = jax.ShapeDtypeStruct((layers, tokens, ff), F32)
    once = lambda a: pl.BlockSpec(a.shape, lambda i: (0,) * len(a.shape), pipeline_mode=pl.Buffered(1))
    anywhere = pl.BlockSpec(memory_space=pl.ANY)
    dma = pltpu.SemaphoreType.DMA
    outs = [*full, shape(heads, tokens, HEAD), shape(tokens, HEAD), shape(tokens, HEAD), shape(heads, tokens, HEAD),
            jax.ShapeDtypeStruct((layers, heads, tokens), F32), shape(tokens, d), wide, wide, jax.ShapeDtypeStruct((tokens, d), BF16)]
    states, by_head, one_head = pltpu.VMEM((tokens, d), BF16), pltpu.VMEM((heads, tokens, HEAD), BF16), pltpu.VMEM((tokens, HEAD), BF16)
    matrix, columns = lambda i: pltpu.VMEM(full[i].shape[1:], BF16), pltpu.VMEM((2, d, BF), BF16)
    routes = dma((layers, len(TENSORS), len(ROUTES)))
    return pl.pallas_call(
        _forward,
        grid=(layers,),
        in_specs=[anywhere] * 8 + [once(cos), once(sin)],
        out_specs=[anywhere] * len(outs),
        out_shape=outs,
        scratch_shapes=[states, states, by_head, one_head, one_head, by_head, pltpu.VMEM((heads, tokens), F32), pltpu.VMEM((tokens, ff), BF16),
                        matrix(0), matrix(1), columns, columns, matrix(4), pltpu.VMEM((2, 2, BT, BF), F32),
                        pltpu.VMEM((heads, BQ), F32), pltpu.VMEM((heads, HEAD + 8, BQ), F32), pltpu.VMEM((BK, BQ), F32),
                        routes, routes, dma((7 * layers,)), dma((9,)), dma((2, 2)), dma((7,))],
        compiler_params=params(collective_id=0, has_side_effects=True),
        cost_estimate=cost(4 * tokens * (7 * HEAD * 1200 + 3 * d * ff)),
        name="forward",
    )(x, *shards, cos, sin)


def act_on(plan, step, scatters, squares):
    for at, actions in plan.items():
        @pl.when(step == at)
        def _():
            for what, names in actions:
                for name in names:
                    getattr(scatters[name], what)(*([squares] if what == "last" else []))


MLP_PLAN = {
    1: [("exchange", ["qkv"])],
    2: [("first", ["qkv"])],
    3: [("second", ["qkv"])],
    4: [("last", ["qkv"])],
    6: [("exchange", ["g", "u"])],
    7: [("first", ["g", "u"])],
    8: [("second", ["g", "u"])],
}


def _mlp_back(*refs, bt, cut):
    dy_ref, mid_ref, gate_ref, up_ref, wg_ref, wu_ref, wd_ref, *refs = refs
    if cut:
        dlater_ref, dmid_ref, dwg_ref, dwu_ref, dwd_ref, gg_ref, gu_ref, gq_ref, squares_ref, *refs = refs
    else:
        dmid_ref, dwg_ref, dwu_ref, dwd_ref, *refs = refs
    bt_s, dyt_s, db_s, act_s, dgu_s, out_s, out_sem, *refs = refs
    f, steps = pl.program_id(0), pl.num_programs(0)
    tokens, bf = act_s.shape

    def results(f):
        cols, slot = pl.ds(pl.multiple_of(f * bf, bf), bf), lax.rem(f, 2)
        return [pltpu.make_async_copy(out_s.at[slot, w], ref.at[:, cols], out_sem.at[slot, w]) for w, ref in enumerate((dwg_ref, dwu_ref))]

    def finished(f):
        for c in results(f):
            c.wait()

    pl.when(f >= 2)(lambda: finished(f - 2))
    if cut:
        me = places()
        scatters = {}
        firsts = lambda ref: ref.at[:, pl.ds(0, cut)]
        for name, src, out in (("qkv", dlater_ref, gq_ref), ("g", firsts(dwg_ref), gg_ref), ("u", firsts(dwu_ref), gu_ref)):
            mine, theirs, across, from_x, from_y, send, recv, local, *refs = refs
            scatters[name] = Scatter(me, src, mine, theirs, across, from_x, from_y, out, send, recv, local)

        @pl.when(f == 0)
        def _():
            greet(me)
            squares_ref[:] = jnp.zeros_like(squares_ref)

        @pl.when(f == 1)
        def _():
            pl.semaphore_wait(pltpu.get_barrier_semaphore(), 3)

        act_on(MLP_PLAN, f, scatters, squares_ref)
    pieces = [pl.ds(at, bt) for at in range(0, tokens, bt)]

    @pl.when(f == 0)
    def _():
        db_s[:] = jnp.zeros_like(db_s)
        for here in pieces:
            wide = mid_ref[here, :].astype(F32)
            bt_s[:, here] = (wide * norm_scale(wide)).astype(BF16).T
            dyt_s[:, here] = dy_ref[here, :].T

    both = jnp.concatenate([wg_ref[:], wu_ref[:]], axis=1)
    for here in pieces:
        gate, up = gate_ref[here, :], up_ref[here, :]
        dact = rounded(dot_t(dy_ref[here, :], wd_ref[:]))
        sig = jax.nn.sigmoid(gate)
        silu = gate * sig
        act_s[here, :] = (silu * up).astype(BF16)
        dgu_s[here, bf:] = (dact * silu).astype(BF16)
        dgu_s[here, :bf] = (dact * up * (sig * (1 + gate * (1 - sig)))).astype(BF16)
        db_s[here, :] += dot_t(dgu_s[here, :], both)
    dgu = dot(bt_s[:], dgu_s[:])
    out_s[lax.rem(f, 2), 0] = dgu[:, :bf].astype(BF16)
    out_s[lax.rem(f, 2), 1] = dgu[:, bf:].astype(BF16)
    for c in results(f):
        c.start()
    dwd_ref[:] = dot(dyt_s[:], act_s[:]).astype(BF16).T

    @pl.when(f == steps - 1)
    def _():
        finished(f - 1)
        finished(f)
        if cut:
            for name in "gu":
                scatters[name].last(squares_ref)
            for scatter in scatters.values():
                scatter.done()
        for here in pieces:
            wide = mid_ref[here, :].astype(F32)
            dmid_ref[here, :] = (dy_ref[here, :].astype(F32) + norm_back(wide, rounded(db_s[here, :]))).astype(BF16)


def mlp_back(layer, dy, mid, gate, up, wg, wu, wd, dlater=None, cut=0, bt=512, bf=256):
    tokens, d = dy.shape
    ff = wg.shape[2]
    one = pl.Buffered(1)
    anywhere = pl.BlockSpec(memory_space=pl.ANY)
    pair = pl.BlockSpec((None, tokens, bf), lambda f: (layer, 0, f))
    column, row = pl.BlockSpec((None, d, bf), lambda f: (layer, 0, f)), pl.BlockSpec((None, bf, d), lambda f: (layer, f, 0))
    states = pl.BlockSpec((tokens, d), lambda f: (0, 0), pipeline_mode=one)
    out = lambda *s: jax.ShapeDtypeStruct(s, BF16)
    cuts = [(d // 8, n) for n in (dlater.shape[1], cut, cut)] if cut else []
    squares = [jax.ShapeDtypeStruct((8, 128), F32)] if cut else []
    return pl.pallas_call(
        functools.partial(_mlp_back, bt=bt, cut=cut),
        grid=(ff // bf,),
        in_specs=[states, pl.BlockSpec((None, tokens, d), lambda f: (layer, 0, 0), pipeline_mode=one), pair, pair, column, column, row,
                  *[anywhere for _ in squares]],
        out_specs=[whole(tokens, d), anywhere, anywhere, pl.BlockSpec((bf, d), lambda f: (f, 0)), *[anywhere for _ in cuts],
                   *[whole(*s.shape) for s in squares]],
        out_shape=[out(tokens, d), out(d, ff), out(d, ff), out(ff, d), *[out(*c) for c in cuts[1:] + cuts[:1]], *squares],
        scratch_shapes=[pltpu.VMEM((d, tokens), BF16), pltpu.VMEM((d, tokens), BF16), pltpu.VMEM((tokens, d), F32),
                        pltpu.VMEM((tokens, bf), BF16), pltpu.VMEM((tokens, 2 * bf), BF16), pltpu.VMEM((2, 2, d, bf), BF16),
                        pltpu.SemaphoreType.DMA((2, 2)), *(s for c in cuts for s in scatter_scratch(*c))],
        compiler_params=params(collective_id=1, has_side_effects=True) if cut else params(),
        cost_estimate=cost(12 * tokens * d * ff, exps=tokens * ff),
        name="mlp_back",
    )(dy, mid, gate, up, wg, wu, wd, *([dlater] if cut else []))


BACK_PLAN = {
    1: [("exchange", ["g", "u", "d"])],
    2: [("first", ["g"])],
    3: [("first", ["u"])],
    4: [("first", ["d"]), ("exchange", ["o"])],
    6: [("second", ["g"]), ("first", ["o"])],
    8: [("second", ["u"])],
    9: [("second", ["d"])],
    11: [("second", ["o"])],
    12: [("last", ["g"])],
    13: [("last", ["u"])],
    15: [("last", ["d", "o"]), ("done", ["g", "u", "d", "o"])],
}


def _attention_back(*refs, bq, bk, first, since):
    dmid_ref, o_ref, q_ref, k_ref, v_ref, lse_ref, h_ref, wo_ref, cos_ref, sin_ref, dwg_ref, dwu_ref, dwd_ref, *refs = refs
    if first:
        dwqkv_ref, gg_ref, gu_ref, gd_ref, go_ref, squares_ref, *refs = refs
    else:
        wqkv_ref, dwqkv_ref, gg_ref, gu_ref, gd_ref, go_ref, squares_ref, dh_ref, *refs = refs
    do_s, dq_s, delta_s, dwo_s, dwob_s, dwqkv_s, dqt_s, dk_s, dv_s, hide_s, *refs = refs
    me = places()
    step = pl.program_id(0)
    heads, bt = o_ref.shape[:2]
    n, middle = do_s.shape[1] // bt, do_s.shape[1] // bq
    scatters = {}
    rest = lambda ref: ref.at[:, pl.ds(since, ref.shape[1] - since)]
    for name, src, out in (("g", rest(dwg_ref), gg_ref), ("u", rest(dwu_ref), gu_ref), ("d", dwd_ref, gd_ref)):
        mine, theirs, across, from_x, from_y, send, recv, local, *refs = refs
        scatters[name] = Scatter(me, src, mine, theirs, across, from_x, from_y, out, send, recv, local)
    scatters["o"] = Scatter(me, dwob_s, None, *refs[:4], go_ref, *refs[4:])

    @pl.when(step == 0)
    def _():
        greet(me)
        squares_ref[:] = jnp.zeros_like(squares_ref)
        dwo_s[:] = jnp.zeros_like(dwo_s)
        dwqkv_s[:] = jnp.zeros_like(dwqkv_s)
        dk_s[:] = jnp.zeros_like(dk_s)
        dv_s[:] = jnp.zeros_like(dv_s)
        hide_s[:] = hidden(bk, bq, bq)

    @pl.when(step == 1)
    def _():
        pl.semaphore_wait(pltpu.get_barrier_semaphore(), 3)

    act_on(BACK_PLAN, step, scatters, squares_ref)

    @pl.when(step < n)
    def _():
        rows = pl.ds(pl.multiple_of(step * bt, bt), bt)
        dmid = dmid_ref[:]
        do = dot_t(dmid, wo_ref[:]).astype(BF16)
        for i in range(heads):
            mine = do[:, i * HEAD : (i + 1) * HEAD]
            do_s[i, rows, :] = mine
            delta_s[i : i + 1, rows] = jnp.sum((mine.astype(F32) * o_ref[i].astype(F32)).T, axis=0, keepdims=True)
        dwo_s[:] += dot(side_by_side(o_ref).T, dmid)

        @pl.when(step == n - 1)
        def _():
            dwob_s[:] = dwo_s[:].astype(BF16)

    @pl.when((step >= n) & (step < n + middle))
    def _():
        iq = step - n
        rows = pl.ds(pl.multiple_of(iq * bq, bq), bq)
        scale = HEAD**-0.5
        e = scale * LOG2E
        dqt_s[:] = jnp.zeros_like(dqt_s)

        def block(first, count, hide=None):
            keys = pl.ds(pl.multiple_of(first, bq), count)
            qs, dos = [q_ref[i] for i in range(heads)], [do_s[i, rows, :] for i in range(heads)]
            scores = [dot_t(k_ref[keys, :], x) for x in qs]
            dps = [dot_t(v_ref[keys, :], x) for x in dos]
            for i in range(heads):
                s = scores[i] * e - lse_ref[i : i + 1, :] * LOG2E
                p = jnp.exp2(s if hide is None else s + hide)
                ds = (p * (dps[i] - delta_s[i : i + 1, rows])).astype(BF16)
                dv_s[keys, :] += dot(p.astype(BF16), dos[i])
                dk_s[keys, :] += dot(ds, qs[i])
                dqt_s[i] += dot(k_ref[keys, :].T, ds)

        whole_blocks = lax.div(iq, 2)
        loop(whole_blocks, lambda j, _: block(j * bk, bk))
        pl.when(lax.rem(iq, 2) == 0)(lambda: block(whole_blocks * bk, bq, hide_s[bq:, :]))
        pl.when(lax.rem(iq, 2) == 1)(lambda: block(whole_blocks * bk, bk, hide_s[:]))
        for i in range(heads):
            dq_s[i, rows, :] = (dqt_s[i] * scale).T.astype(BF16)

    @pl.when(step >= n + middle)
    def _():
        rows = pl.ds(pl.multiple_of((step - n - middle) * bt, bt), bt)
        cos, sin = cos_ref[:], sin_ref[:]
        parts = []
        for t in [*(dq_s[i, rows, :] for i in range(heads)), (dk_s[rows, :] * HEAD**-0.5).astype(BF16)]:
            t = t.astype(F32)
            parts.append((t * cos - pltpu.roll(t, HALF, 1) * sin).astype(BF16))
        dz = jnp.concatenate([*parts, dv_s[rows, :].astype(BF16)], axis=1)
        wide = h_ref[:].astype(F32)
        a = (wide * norm_scale(wide)).T.astype(BF16)
        dwqkv_s[:] += dot(a, dz)
        if not first:
            da = rounded(dot_t(dz, wqkv_ref[:]))
            dh_ref[:] = (dmid_ref[:].astype(F32) + norm_back(wide, da)).astype(BF16)

        @pl.when(step == 2 * n + middle - 1)
        def _():
            dwqkv_ref[:] = dwqkv_s[:].astype(BF16)


def attention_back(layer, dmid, o, q, k, v, lse, h, wo, cos, sin, dwg, dwu, dwd, wqkv=None, since=0, bq=256, bk=512, bt=512):
    tokens, d = dmid.shape
    heads = o.shape[1]
    wide = d + 2 * HEAD
    n, inner = tokens // bt, tokens // bq
    one = pl.Buffered(1)
    early = lambda s: jnp.minimum(s, n - 1)
    middle = lambda s: jnp.clip(s - n, 0, inner - 1)
    late = lambda s: jnp.maximum(s - n - inner, 0)
    twice = early if wqkv is None else lambda s: jnp.where(s < n, s, late(s))
    rows = lambda w, which: pl.BlockSpec((bt, w), lambda s: (which(s), 0))
    by_head = lambda which, block: pl.BlockSpec((None, heads, block, HEAD), lambda s: (layer, 0, which(s), 0))
    all_of = lambda a: pl.BlockSpec((None, *a.shape[1:]), lambda s: (layer, 0, 0), pipeline_mode=one)
    anywhere = pl.BlockSpec(memory_space=pl.ANY)
    cuts = [(a.shape[0] // 8, a.shape[1] - first) for a, first in ((dwg, since), (dwu, since), (dwd, 0))]
    cut_o = (d // 8, d)
    out = lambda s: jax.ShapeDtypeStruct(s, BF16)
    more, more_in, more_out = ([], [], []) if wqkv is None else ([wqkv], [all_of(wqkv)], [(rows(d, late), out((tokens, d)))])
    flops = 4 * tokens * d * (d + wide) + 5 * heads * tokens * tokens * HEAD
    return pl.pallas_call(
        functools.partial(_attention_back, bq=bq, bk=bk, first=wqkv is None, since=since),
        grid=(2 * n + inner,),
        in_specs=[rows(d, twice), by_head(early, bt), by_head(middle, bq), all_of(k), all_of(v),
                  pl.BlockSpec((None, heads, bq), lambda s: (layer, 0, middle(s))), rows(d, late), all_of(wo),
                  rows(HEAD, late), rows(HEAD, late), anywhere, anywhere, anywhere, *more_in],
        out_specs=[whole(d, wide), *[anywhere] * 4, whole(8, 128), *(spec for spec, _ in more_out)],
        out_shape=[out((d, wide)), *(out(c) for c in cuts), out(cut_o), jax.ShapeDtypeStruct((8, 128), F32),
                   *(shape for _, shape in more_out)],
        scratch_shapes=[pltpu.VMEM((heads, tokens, HEAD), BF16), pltpu.VMEM((heads, tokens, HEAD), BF16), pltpu.VMEM((heads, tokens), F32),
                        pltpu.VMEM((d, d), F32), pltpu.VMEM((d, d), BF16), pltpu.VMEM((d, wide), F32),
                        pltpu.VMEM((heads, HEAD, bq), F32), pltpu.VMEM((tokens, HEAD), F32), pltpu.VMEM((tokens, HEAD), F32),
                        pltpu.VMEM((bk, bq), F32), *(s for c in cuts for s in scatter_scratch(*c)),
                        *scatter_scratch(*cut_o, in_vmem=True)],
        compiler_params=params(collective_id=2 + layer, has_side_effects=True),
        cost_estimate=cost(flops, exps=heads * tokens * tokens // 2),
        name="attention_back",
    )(dmid, o, q, k, v, lse, h, wo, cos, sin, dwg, dwu, dwd, *more)


def _finish(dwqkv_ref, *rest, known, count):
    squares_refs, (g_ref, factor_ref, own, theirs, across, from_x, from_y, send, recv, local, all_s, total_s, send_all, recv_all) = \
        rest[:known], rest[known:]
    me = places()
    greeted = greet(me, range(1, 8))
    total_s[:] = jnp.zeros_like(total_s)
    for ref in squares_refs:
        total_s[:] += ref[:]
    scatter = Scatter(me, dwqkv_ref, own, theirs, across, from_x, from_y, g_ref, send, recv, local)
    greeted()
    scatter.exchange()
    scatter.first()
    scatter.second()
    scatter.last(total_s)
    copies = [pltpu.make_async_remote_copy(src_ref=total_s, dst_ref=all_s.at[bits], send_sem=send_all.at[bits], recv_sem=recv_all.at[bits],
                                           device_id=(0, me[bits]), device_id_type=pl.DeviceIdType.MESH) for bits in range(1, 8)]
    for c in copies:
        c.start()
    for c in copies:
        c.wait_recv()
    tiles = [total_s[:], *(all_s[bits] for bits in range(1, 8))]
    tiles = [jnp.sum(t) for t in tiles]
    while len(tiles) > 1:
        tiles = [a + b for a, b in zip(tiles[::2], tiles[1::2])]
    factor_ref[:] = jnp.full((8, 128), jnp.minimum(1.0, 0.5 * lax.rsqrt(jnp.full((8, 128), tiles[0] / count) + 1e-30)), F32)
    for c in copies:
        c.wait_send()
    scatter.done()


def finish(dwqkv, squares, count):
    r, n = dwqkv.shape[0] // 8, dwqkv.shape[1]
    dma = pltpu.SemaphoreType.DMA
    anywhere = pl.BlockSpec(memory_space=pl.ANY)
    return pl.pallas_call(
        functools.partial(_finish, known=len(squares), count=count),
        in_specs=[anywhere] + [pl.BlockSpec(memory_space=pltpu.VMEM)] * len(squares),
        out_specs=[anywhere, pl.BlockSpec(memory_space=pltpu.VMEM)],
        out_shape=[jax.ShapeDtypeStruct((r, n), BF16), jax.ShapeDtypeStruct((8, 128), F32)],
        scratch_shapes=[*scatter_scratch(r, n), pltpu.VMEM((8, 8, 128), F32), pltpu.VMEM((8, 128), F32), dma((8,)), dma((8,))],
        compiler_params=pltpu.CompilerParams(collective_id=4, has_side_effects=True, vmem_limit_bytes=8 * 2**20),
        cost_estimate=cost(2e10, 1e6),
        name="finish",
    )(dwqkv, *squares)


def adamw(w, m, v, g):
    m = 0.9 * m + 0.1 * g
    v = 0.95 * v + 0.05 * g * g
    step = m * lax.rsqrt(v + 1e-8) + 0.1 * w
    return (w - 0.02 * step).astype(BF16), m, v


def solution(mesh):
    def step(x, dy, *arrays):
        weights, m, v = (arrays[i : i + 7] for i in (0, 7, 14))
        tokens, d = x.shape[1:]
        cos, sin = tables(tokens)
        *full, q, k, v_, o, lse, mid, gate, up, h1 = forward(x[0], weights, cos, sin)
        fqkv, fo, fg, fu, fd = full
        dmid, dwg, dwu, dwd = mlp_back(1, dy[0], mid, gate, up, fg, fu, fd)
        dlater, g1, u1, d1, o1, s1, dh = attention_back(1, dmid, o, q, k, v_, lse, h1, fo, cos, sin, dwg, dwu, dwd, wqkv=fqkv)
        cut = gate.shape[2] // 2
        dmid, dwg, dwu, dwd, ga, ua, qkv1, s2 = mlp_back(0, dh, mid, gate, up, fg, fu, fd, dlater, cut)
        dwqkv, gb, ub, d0, o0, s0 = attention_back(0, dmid, o, q, k, v_, lse, x[0], fo, cos, sin, dwg, dwu, dwd, since=cut)
        g0, u0 = jnp.concatenate([ga, gb], axis=1), jnp.concatenate([ua, ub], axis=1)
        qkv0, factor = finish(dwqkv, [s2, s1, s0], 8 * sum(w.size for w in weights))
        factor = factor[0, 0]
        split = lambda a: [a[:, :d], a[:, d : d + HEAD], a[:, d + HEAD :]]
        mine = [[*split(qkv0), o0, g0, u0, d0], [*split(qkv1), o1, g1, u1, d1]]
        gradients = [jnp.stack([one[i] for one in mine]).astype(F32) for i in range(7)]
        new = [adamw(w.astype(F32), m, v, g * factor) for w, m, v, g in zip(weights, m, v, gradients, strict=True)]
        return tuple(one[which] for which in range(3) for one in new)

    states, cut = P(("rep", "dp"), None, None), P(None, "dp", None)
    return jax.shard_map(
        step,
        mesh=mesh,
        in_specs=(states, states) + (cut,) * 21,
        out_specs=(P("rep", "dp", None),) * 21,
        check_vma=False,
    )
```

```python
import functools

import jax
import jax.numpy as jnp
import numpy as np
from jax import lax
from jax.experimental import pallas as pl
from jax.experimental.pallas import tpu as pltpu
from jax.sharding import PartitionSpec as P

NEG = -1e30
HIDDEN = 2 * NEG
LOG2E = 1.4426950408889634
VMEM = 127 * 2**19
STRIP = 512
HEAD = 128
HALF = HEAD // 2
THETA = 10000
F32, BF16 = jnp.float32, jnp.bfloat16


def dot(a, b, ca=1, cb=0):
    return lax.dot_general(a, b, (((ca,), (cb,)), ((), ())), preferred_element_type=F32)


def dot_t(a, b):
    return dot(a, b, 1, 1)


def loop(stop, body, start=0):
    lax.fori_loop(start, stop, body, None)


def rounded(a):
    return a.astype(BF16).astype(F32)


def norm_scale(wide):
    return lax.rsqrt(jnp.mean(wide * wide, -1, keepdims=True) + 1e-6)


def norm_back(wide, by):
    scale = norm_scale(wide)
    return scale * (by - wide * (scale * scale * jnp.mean(by * wide, -1, keepdims=True)))


def params(**more):
    return pltpu.CompilerParams(vmem_limit_bytes=VMEM, **more)


def whole(*shape):
    return pl.BlockSpec(shape, lambda *_: (0,) * len(shape))


def cost(flops, nbytes=0, exps=0):
    return pl.CostEstimate(flops=int(flops), bytes_accessed=int(nbytes), transcendentals=int(exps))


def tables(tokens):
    angle = np.arange(tokens, dtype=np.float64)[:, None] * THETA ** (-np.arange(HALF, dtype=np.float64) / HALF)
    cos, sin = np.cos(angle), np.sin(angle)
    return jnp.asarray(np.concatenate([cos, cos], 1), F32), jnp.asarray(np.concatenate([-sin, sin], 1), F32)


def hidden(keys, queries, later=0):
    gap = lax.broadcasted_iota(jnp.int32, (keys, queries), 1) - lax.broadcasted_iota(jnp.int32, (keys, queries), 0)
    return jnp.where(gap + later >= 0, 0.0, HIDDEN)


def side_by_side(ref):
    return jnp.concatenate([ref[n] for n in range(ref.shape[0])], axis=1)


X, Y, CORE, HERE = 4, 2, 1, 0
NEAR = (HERE, X, Y, X + Y)


def places():
    at = [lax.axis_index("dp")]
    for bit in (CORE, Y, X):
        at += [n + bit - 2 * bit * lax.rem(lax.div(n, bit), 2) for n in at]
    return at


def greet(me, all_of=(X, Y, CORE)):
    barrier = pltpu.get_barrier_semaphore()
    for bits in all_of:
        pl.semaphore_signal(barrier, inc=1, device_id=(0, me[bits]), device_id_type=pl.DeviceIdType.MESH)
    return lambda: pl.semaphore_wait(barrier, len(all_of))


def remote(me, bit, src, dst, send, recv):
    return pltpu.make_async_remote_copy(src_ref=src, dst_ref=dst, send_sem=send, recv_sem=recv, device_id=(0, me[bit]),
                                        device_id_type=pl.DeviceIdType.MESH)


def halves(r):
    a = (r // 2 + 15) // 16 * 16
    return (0, a), (a, r - a)


def upper(r):
    return halves(r)[0]


def lower(r):
    return halves(r)[1]


ALL = None
ROUTES = {"x": (X, HERE, ALL), "y": (Y, HERE, ALL), "core": (CORE, HERE, ALL), "xy": (Y, X, upper), "x core": (CORE, X, ALL),
          "yx": (X, Y, lower), "y core": (CORE, Y, ALL), "xy core": (CORE, X + Y, upper), "yx core": (CORE, X + Y, lower)}


class Gather:
    def __init__(self, me, block, full, send, recv, cols, at):
        first, count = cols
        self.me, self.r = me, block.shape[0]
        self.full, self.send, self.recv = full, send, recv
        self.own, self.cols = block.at[:, pl.ds(first, count)], pl.ds(at + first, count)

    def rows(self, bits, part=None):
        first, count = part or (0, self.r)
        at = pl.multiple_of(self.me[bits] * self.r + first, 16)
        return self.full.at[pl.ds(at, count), self.cols]

    def copy(self, which, got=False):
        bit, bits, part = ROUTES[which]
        there = self.rows(bits + bit if got else bits, part and part(self.r))
        n = tuple(ROUTES).index(which)
        return remote(self.me, bit, self.own if bits == HERE and not got else there, there, self.send.at[n], self.recv.at[n])

    def got(self, which):
        self.copy(which, got=True).wait_recv()

    def begin(self):
        for n in ("x", "y", "core"):
            self.copy(n).start()

    def hand_on(self):
        self.got("x")
        self.copy("xy").start()
        self.copy("x core").start()
        self.got("y")
        self.copy("yx").start()
        self.copy("y core").start()

    def finish(self):
        self.got("xy")
        self.copy("xy core").start()
        self.got("yx")
        self.copy("yx core").start()

    def arrived(self):
        for n in ("core", "x core", "y core", "xy core", "yx core"):
            self.got(n)

    def sent(self):
        for n in ROUTES:
            self.copy(n).wait_send()


class Scatter:
    def __init__(self, me, src, mine, theirs, across, from_x, from_y, out, send, recv, local):
        self.me, self.src, self.out = me, src, out
        self.r, self.n = theirs.shape[1:]
        self.own, self.theirs, self.across, self.from_x, self.from_y = mine, theirs, across, from_x, from_y
        self.send, self.recv, self.local = send, recv, local
        self.a, self.b = halves(self.r)
        self.all = (0, self.r)

    def block(self, bits, part=None):
        first, count = part or self.all
        return self.src.at[pl.ds(pl.multiple_of(self.me[bits] * self.r + first, 16), count)]

    def mine(self, j, part):
        return self.block(NEAR[j], part) if self.own is None else self.own.at[j, pl.ds(*part)]

    def load(self, j):
        return pltpu.make_async_copy(self.block(NEAR[j]), self.own.at[j], self.local.at[j])

    def copy(self, n):
        if n < 4:
            bit, src, dst = CORE, self.block(CORE + NEAR[n]), self.theirs.at[n]
        else:
            bit, j, part, to = ((X, 3, self.a, self.across), (Y, 3, self.b, self.across), (X, 1, self.a, self.from_x),
                                (Y, 2, self.b, self.from_y), (Y, 2, self.a, self.from_y), (X, 1, self.b, self.from_x))[n - 4]
            src, dst = self.mine(j, part), to.at[pl.ds(*part)]
        return remote(self.me, bit, src, dst, self.send.at[n], self.recv.at[n])

    def add(self, j, part, *more):
        step = 16
        ref = self.mine(j, part)

        def one(i, _):
            rows = pl.ds(pl.multiple_of(i * step, step), step)
            full = pl.ds(pl.multiple_of(part[0] + i * step, step), step)
            total = ref[rows, :].astype(F32) + self.theirs[j, full, :].astype(F32)
            for other in more:
                total += other[full, :].astype(F32)
            ref[rows, :] = total.astype(BF16)

        loop(part[1] // step, one)

    def exchange(self):
        for j in range(4):
            self.copy(j).start()
            if self.own is not None:
                self.load(j).start()

    def first(self):
        for j in range(4):
            if self.own is not None:
                self.load(j).wait()
            self.copy(j).wait_recv()
        self.add(3, self.all)
        self.copy(4).start()
        self.copy(5).start()
        self.add(1, self.a)
        self.add(2, self.b)

    def second(self):
        self.copy(6).start()
        self.copy(7).start()
        self.copy(4).wait_recv()
        self.add(2, self.a, self.across)
        self.copy(8).start()
        self.copy(5).wait_recv()
        self.add(1, self.b, self.across)
        self.copy(9).start()

    def result(self):
        return pltpu.make_async_copy(self.mine(0, self.all), self.out, self.local.at[4])

    def last(self, squares):
        for n in range(6, 10):
            self.copy(n).wait_recv()
        self.add(0, self.all, self.from_x, self.from_y)
        ref = self.mine(0, self.all)
        self.result().start()
        squares[:] += sum_of_squares(ref)

    def done(self):
        for n in range(10):
            self.copy(n).wait_send()
        self.result().wait()


def sum_of_squares(ref):
    rows, cols = ref.shape

    def one(i, total):
        g = ref[pl.ds(pl.multiple_of(i * 16, 16), 16), :].astype(F32)
        g = g * g
        for c in range(0, cols, 128):
            total += g[:8, c : c + 128] + g[8:, c : c + 128]
        return total

    return lax.fori_loop(0, rows // 16, one, jnp.zeros((8, 128), F32))


def scatter_scratch(r, n, in_vmem=False):
    dma = pltpu.SemaphoreType.DMA
    block = pltpu.VMEM((r, n), BF16)
    return [*([] if in_vmem else [pltpu.VMEM((4, r, n), BF16)]), pltpu.VMEM((4, r, n), BF16), block, block, block,
            dma((10,)), dma((10,)), dma((5,))]


BQ = BK = BT = BF = 512
CUT, CUT_Q = 2 * BF, 4 * HEAD
TENSORS = ("qa", "qb", "k", "v", "o", "ga", "ua", "gb", "ub", "d")
QKV, GU_A, GU_B = ["qa", "k", "v", "qb"], ["ga", "ua"], ["gb", "ub"]


def _forward(x_ref, sq, sk, sv, so, sg, su, sd, cos_ref, sin_ref, fqkv, fo, fg, fu, fd, q_o, k_o, v_o, o_o, lse_o, mid_o, gate_o, up_o, h_o,
             h_s, b_s, q_s, k_s, v_s, o_s, lse_s, act_s, wqkv_s, wo_s, wg_s, wu_s, wd_s, stage_s, top_s, mix_s, hide_s,
             send, recv, load, keep, out, wsem):
    layer, layers = pl.program_id(0), pl.num_programs(0)
    me = places()
    tokens, d = h_s.shape
    heads = q_s.shape[0]
    ff = act_s.shape[1]
    blocks = tokens // BT

    def gather(n, name):
        i = TENSORS.index(name)
        shard, full, cols, at = {
            "qa": (sq, fqkv, (0, CUT_Q), 0), "qb": (sq, fqkv, (CUT_Q, d - CUT_Q), 0), "k": (sk, fqkv, (0, HEAD), d),
            "v": (sv, fqkv, (0, HEAD), d + HEAD), "o": (so, fo, (0, d), 0), "d": (sd, fd, (0, d), 0),
            "ga": (sg, fg, (0, CUT), 0), "gb": (sg, fg, (CUT, ff - CUT), 0),
            "ua": (su, fu, (0, CUT), 0), "ub": (su, fu, (CUT, ff - CUT), 0)}[name]
        full = wqkv_s if name in QKV and n == 0 else full.at[n]
        return Gather(me, shard.at[n], full, send.at[n, i], recv.at[n, i], cols, at)

    def own_blocks():
        at = 0
        for s, f, column in ((sq, fqkv, 0), (sk, fqkv, d), (sv, fqkv, d + HEAD), (so, fo, 0), (sg, fg, 0), (su, fu, 0), (sd, fd, 0)):
            r, n = s.shape[1:]
            for i in range(s.shape[0]):
                where = pl.ds(pl.multiple_of(me[HERE] * r, 16), r), pl.ds(column, n)
                if f is fqkv and i == 0:
                    yield s.at[i], wqkv_s.at[where], None
                else:
                    yield s.at[i], act_s.at[pl.ds(at, r), pl.ds(0, n)], f.at[i, *where]
                    at += r

    copies_in = lambda: [pltpu.make_async_copy(a, b, load.at[i]) for i, (a, b, _) in enumerate(own_blocks())]
    copies_out = lambda: [pltpu.make_async_copy(b, c, load.at[i]) for i, (_, b, c) in enumerate(own_blocks()) if c is not None]
    here = lambda i, n: pl.ds(pl.multiple_of(i * n, n), n)

    def kept(*names):
        pairs = {"x": (x_ref, h_s), "q": (q_s, q_o.at[layer]), "k": (k_s, k_o.at[layer]), "v": (v_s, v_o.at[layer]), "o": (o_s, o_o.at[layer]),
                 "lse": (lse_s, lse_o.at[layer]), "mid": (h_s, mid_o.at[layer]), "h": (h_s, h_o), "qkv": (wqkv_s, fqkv.at[layer])}
        return [pltpu.make_async_copy(*pairs[n], keep.at[list(pairs).index(n)]) for n in names]

    def start(*copies):
        for c in copies:
            c.start()

    def wait(*copies):
        for c in copies:
            c.wait()

    def weight(n, name):
        return pltpu.make_async_copy(*{"qb": (fqkv.at[n], wqkv_s, wsem.at[0]), "o": (fo.at[n], wo_s, wsem.at[1]),
                                       "d": (fd.at[n], wd_s, wsem.at[2])}[name])

    def column(c, n=layer):
        cols, slot = here(c, BF), lax.rem(c, 2)
        return (pltpu.make_async_copy(fg.at[n, :, cols], wg_s.at[slot], wsem.at[3 + slot]),
                pltpu.make_async_copy(fu.at[n, :, cols], wu_s.at[slot], wsem.at[5 + slot]))

    def fetch(n, name):
        gather(n, name).arrived()
        if name in QKV:
            gather(0, name).sent()
        if name == "ua":
            start(*column(0, n))
        elif name in ("qb", "o", "d"):
            start(weight(n, name))

    def tick(phase, i):
        for n, plan in enumerate(PLAN):
            for p, k, *actions in plan:
                if p == phase:
                    @pl.when((layer == n) & (i == k))
                    def _():
                        for do, later, names in actions:
                            for name in names:
                                if do == "fetch":
                                    fetch(n + later, name)
                                else:
                                    getattr(gather(n + later, name), do)()

    @pl.when(layer == 0)
    def _():
        greeted = greet(me)
        start(*kept("x"), *copies_in())
        hide_s[:] = hidden(BK, BQ)
        greeted()
        for name in QKV:
            gather(0, name).begin()
        wait(*copies_in())
        start(*copies_out())
        wait(*kept("x"))
        for name in QKV:
            gather(0, name).hand_on()
        for name in ("o", *GU_A):
            gather(0, name).begin()
        wait(*copies_out())
        for do in (Gather.finish, Gather.arrived):
            for name in QKV:
                do(gather(0, name))

    @pl.when(layer > 0)
    def _():
        start(*kept("h"))
        wait(weight(1, "qb"))

    def qkv_step(i):
        rows = here(i, BT)
        wide = h_s[rows, :].astype(F32)
        a = (wide * norm_scale(wide)).astype(BF16)
        z = dot(a, wqkv_s[:])
        cos, sin = cos_ref[rows, :], sin_ref[rows, :]
        for n in range(heads + 1):
            t = rounded(z[:, n * HEAD : (n + 1) * HEAD])
            t = (t * cos + pltpu.roll(t, HALF, 1) * sin).astype(BF16)
            if n < heads:
                q_s[n, rows, :] = t
            else:
                k_s[rows, :] = t
        v_s[rows, :] = z[:, (heads + 1) * HEAD :].astype(BF16)

    pairwise(blocks, qkv_step, lambda i: tick("qkv", i))
    start(*kept("q", "k", "v"))

    @pl.when(layer == 0)
    def _():
        start(*kept("qkv"))

    scale = HEAD**-0.5
    e = scale * LOG2E

    def attend_step(i, _):
        top_s[:] = jnp.full(top_s.shape, NEG, F32)
        mix_s[:] = jnp.zeros(mix_s.shape, F32)

        def block(first, count, at=0, hidden=None):
            keys, cols = pl.ds(pl.multiple_of(first, BK // 2), count), pl.ds(at, BQ - at)
            rows = pl.ds(pl.multiple_of(i * BQ + at, BQ // 2), BQ - at)
            values = jnp.concatenate([v_s[keys, :].T, jnp.ones((8, count), BF16)], axis=0)
            scores = [dot_t(k_s[keys, :], q_s[n, rows, :]) for n in range(heads)]
            weights = []
            for n, s in enumerate(scores):
                s = s if hidden is None else s + hidden
                old = top_s[n : n + 1, cols]
                top = jnp.maximum(old, s.max(axis=0, keepdims=True))
                top_s[n : n + 1, cols] = top
                weights.append((jnp.exp2((s - top) * e).astype(BF16), jnp.exp2((old - top) * e)))
            for n, (p, rest) in enumerate(weights):
                mix_s[n, :, cols] = mix_s[n, :, cols] * rest + dot(values, p)

        def before(j, _):
            tick("attend", lax.div(i * (i + 1), 2) + j)
            block(j * BK, BK)

        loop(i, before)
        tick("attend", lax.div(i * (i + 3), 2))
        half = BK // 2
        block(i * BK, half, hidden=hide_s[:half, :])
        block(i * BK + half, half, half, hide_s[half:, half:])
        rows = here(i, BQ)
        for n in range(heads):
            total = mix_s[n, HEAD : HEAD + 1, :]
            o_s[n, rows, :] = (mix_s[n, :HEAD, :] * (1 / total)).T.astype(BF16)
            lse_s[n : n + 1, rows] = top_s[n : n + 1, :] * scale + jnp.log(total)

    loop(tokens // BQ, attend_step)
    start(*kept("o", "lse"))

    @pl.when(layer == 0)
    def _():
        wait(*kept("qkv"))

    @pl.when(layer > 0)
    def _():
        wait(*kept("h"))

    wait(weight(layer, "o"))

    def out_step(i):
        rows = here(i, BT)
        o = jnp.concatenate([o_s[n, rows, :] for n in range(heads)], axis=1)
        mid = (h_s[rows, :].astype(F32) + rounded(dot(o, wo_s[:]))).astype(BF16)
        h_s[rows, :] = mid
        wide = mid.astype(F32)
        b_s[rows, :] = (wide * norm_scale(wide)).astype(BF16)

    pairwise(blocks, out_step, lambda i: tick("out", i))
    start(*kept("mid"))

    def staged(i, c):
        rows, cols = here(i, BT), here(c, BF)
        return [pltpu.make_async_copy(stage_s.at[i, w], ref.at[layer, rows, cols], out.at[i, w]) for w, ref in enumerate((gate_o, up_o))]

    def gate_column(c, _):
        wait(*column(c))

        def gate_step(i):
            rows = here(i, BT)
            b = b_s[rows, :]
            gate, up = dot(b, wg_s[lax.rem(c, 2)]), dot(b, wu_s[lax.rem(c, 2)])
            stage_s[i, 0] = gate
            stage_s[i, 1] = up
            act_s[rows, here(c, BF)] = (gate * jax.nn.sigmoid(gate) * up).astype(BF16)
            start(*staged(i, c))

        for i in range(0, blocks, 2):
            tick("gate", 2 * c + i // 2)
            if i > 0:
                pl.when(c + 1 < ff // BF)(lambda: start(*column(c + 1)))

            @pl.when((layer > 0) | (c > 0))
            def _():
                wait(*staged(i, c), *staged(i + 1, c))

            gate_step(i)
            gate_step(i + 1)

    loop(ff // BF, gate_column)
    wait(*kept("q", "k", "v", "o", "lse", "mid"))

    @pl.when(layer < layers - 1)
    def _():
        wait(weight(0, "d"))

        def down_step(i):
            rows = here(i, BT)
            h_s[rows, :] = (h_s[rows, :].astype(F32) + rounded(dot(act_s[rows, :], wd_s[:]))).astype(BF16)

        pairwise(blocks, down_step, lambda i: tick("down", i))
        tick("end", 0)

    @pl.when(layer == layers - 1)
    def _():
        gather(1, "d").arrived()
        for i in range(blocks):
            wait(*staged(i, 0))
        for n in range(2):
            for name in TENSORS:
                if name not in QKV or n > 0:
                    gather(n, name).sent()


def pairwise(count, body, first):
    def two(i, _):
        first(i)
        body(2 * i)
        body(2 * i + 1)

    loop(count // 2, two)


THIS, NEXT = range(2)
PLAN = ([
    ("qkv", 1, ("hand_on", THIS, ["o"]), ("begin", THIS, GU_B)),
    ("attend", 3, ("hand_on", THIS, GU_A), ("finish", THIS, ["o"])),
    ("attend", 8, ("fetch", THIS, ["o"])),
    ("attend", 9, ("hand_on", THIS, GU_B), ("begin", THIS, ["d"])),
    ("out", 1, ("finish", THIS, GU_A), ("fetch", THIS, GU_A)),
    ("gate", 2, ("finish", THIS, GU_B)),
    ("gate", 3, ("fetch", THIS, GU_B)),
    ("gate", 4, ("begin", NEXT, QKV)),
    ("gate", 6, ("hand_on", THIS, ["d"])),
    ("gate", 8, ("hand_on", NEXT, QKV), ("begin", NEXT, ["o"])),
    ("gate", 9, ("finish", THIS, ["d"]), ("fetch", THIS, ["d"])),
    ("down", 0, ("finish", NEXT, QKV), ("begin", NEXT, GU_A)),
    ("down", 1, ("fetch", NEXT, QKV)),
], [
    ("qkv", 0, ("hand_on", THIS, ["o"])),
    ("qkv", 1, ("begin", THIS, ["gb"])),
    ("attend", 1, ("hand_on", THIS, GU_A), ("begin", THIS, ["ub"])),
    ("attend", 4, ("finish", THIS, ["o"])),
    ("attend", 7, ("fetch", THIS, ["o"])),
    ("attend", 8, ("finish", THIS, GU_A)),
    ("attend", 9, ("hand_on", THIS, GU_B), ("begin", THIS, ["d"])),
    ("out", 1, ("fetch", THIS, GU_A)),
    ("gate", 2, ("finish", THIS, GU_B)),
    ("gate", 3, ("fetch", THIS, GU_B)),
    ("gate", 6, ("hand_on", THIS, ["d"])),
    ("gate", 9, ("finish", THIS, ["d"])),
])


def forward(x, shards, cos, sin):
    tokens, d = x.shape
    layers = shards[0].shape[0]
    heads, ff = d // HEAD, shards[4].shape[2]
    full = [jax.ShapeDtypeStruct((layers, *s), BF16) for s in ((d, d + 2 * HEAD), (d, d), (d, ff), (d, ff), (ff, d))]
    shape = lambda *s: jax.ShapeDtypeStruct((layers, *s), BF16)
    wide = jax.ShapeDtypeStruct((layers, tokens, ff), F32)
    once = lambda a: pl.BlockSpec(a.shape, lambda i: (0,) * len(a.shape), pipeline_mode=pl.Buffered(1))
    anywhere = pl.BlockSpec(memory_space=pl.ANY)
    dma = pltpu.SemaphoreType.DMA
    outs = [*full, shape(heads, tokens, HEAD), shape(tokens, HEAD), shape(tokens, HEAD), shape(heads, tokens, HEAD),
            jax.ShapeDtypeStruct((layers, heads, tokens), F32), shape(tokens, d), wide, wide, jax.ShapeDtypeStruct((tokens, d), BF16)]
    states, by_head, one_head = pltpu.VMEM((tokens, d), BF16), pltpu.VMEM((heads, tokens, HEAD), BF16), pltpu.VMEM((tokens, HEAD), BF16)
    matrix, columns = lambda i: pltpu.VMEM(full[i].shape[1:], BF16), pltpu.VMEM((2, d, BF), BF16)
    routes = dma((layers, len(TENSORS), len(ROUTES)))
    return pl.pallas_call(
        _forward,
        grid=(layers,),
        in_specs=[anywhere] * 8 + [once(cos), once(sin)],
        out_specs=[anywhere] * len(outs),
        out_shape=outs,
        scratch_shapes=[states, states, by_head, one_head, one_head, by_head, pltpu.VMEM((heads, tokens), F32), pltpu.VMEM((tokens, ff), BF16),
                        matrix(0), matrix(1), columns, columns, matrix(4), pltpu.VMEM((tokens // BT, 2, BT, BF), F32),
                        pltpu.VMEM((heads, BQ), F32), pltpu.VMEM((heads, HEAD + 8, BQ), F32), pltpu.VMEM((BK, BQ), F32),
                        routes, routes, dma((7 * layers,)), dma((9,)), dma((tokens // BT, 2)), dma((7,))],
        compiler_params=params(collective_id=0, has_side_effects=True),
        cost_estimate=cost(4 * tokens * (7 * HEAD * 1200 + 3 * d * ff)),
        name="forward",
    )(x, *shards, cos, sin)


def act_on(plan, step, scatters, squares):
    for at, actions in plan.items():
        @pl.when(step == at)
        def _():
            for what, names in actions:
                for name in names:
                    getattr(scatters[name], what)(*([squares] if what == "last" else []))


MLP_PLAN = {
    1: [("exchange", ["qkv"])],
    2: [("first", ["qkv"])],
    3: [("second", ["qkv"])],
    4: [("last", ["qkv"])],
    5: [("exchange", ["g", "u"])],
    6: [("first", ["g", "u"])],
    7: [("second", ["g", "u"])],
}


def _mlp_back(*refs, bt, cut, layer):
    dy_ref, mid_ref, gate_ref, up_ref, wg_ref, wu_ref, wd_ref, *refs = refs
    if cut:
        dlater_ref, dmid_ref, dwg_ref, dwu_ref, dwd_ref, gg_ref, gu_ref, gq_ref, squares_ref, *refs = refs
    else:
        dmid_ref, dwg_ref, dwu_ref, dwd_ref, *refs = refs
    dy_s, mid_s, bt_s, dyt_s, db_s, act_s, dgu_s, out_s, in_sem, out_sem, *refs = refs
    f, steps = pl.program_id(0), pl.num_programs(0)
    tokens = dy_s.shape[0]
    bf = act_s.shape[1]
    pieces = [pl.ds(at, bt) for at in range(0, tokens, bt)]

    def loads(p):
        return [pltpu.make_async_copy(ref.at[pieces[p]], s.at[pieces[p]], in_sem.at[p, w])
                for w, (ref, s) in enumerate(((dy_ref, dy_s), (mid_ref.at[layer], mid_s)))]

    def stored(p):
        return pltpu.make_async_copy(dy_s.at[pieces[p]], dmid_ref.at[pieces[p]], in_sem.at[p, 0])

    def results(f):
        cols, slot = pl.ds(pl.multiple_of(f * bf, bf), bf), lax.rem(f, 2)
        return [pltpu.make_async_copy(out_s.at[slot, w], ref.at[:, cols], out_sem.at[slot, w]) for w, ref in enumerate((dwg_ref, dwu_ref))]

    def finished(f):
        for c in results(f):
            c.wait()

    @pl.when(f == 0)
    def _():
        for p in range(len(pieces)):
            for c in loads(p):
                c.start()

    pl.when(f >= 2)(lambda: finished(f - 2))
    if cut:
        me = places()
        scatters = {}
        firsts = lambda ref: ref.at[:, pl.ds(0, cut)]
        for name, src, out in (("qkv", dlater_ref, gq_ref), ("g", firsts(dwg_ref), gg_ref), ("u", firsts(dwu_ref), gu_ref)):
            mine, theirs, across, from_x, from_y, send, recv, local, *refs = refs
            scatters[name] = Scatter(me, src, mine, theirs, across, from_x, from_y, out, send, recv, local)

        @pl.when(f == 0)
        def _():
            greet(me)
            squares_ref[:] = jnp.zeros_like(squares_ref)

        @pl.when(f == 1)
        def _():
            pl.semaphore_wait(pltpu.get_barrier_semaphore(), 3)

        act_on(MLP_PLAN, f, scatters, squares_ref)

    @pl.when(f == 0)
    def _():
        db_s[:] = jnp.zeros_like(db_s)
        for p, here in enumerate(pieces):
            for c in loads(p):
                c.wait()
            wide = mid_s[here, :].astype(F32)
            bt_s[:, here] = (wide * norm_scale(wide)).astype(BF16).T
            dyt_s[:, here] = dy_s[here, :].T

    both = jnp.concatenate([wg_ref[:], wu_ref[:]], axis=1)
    for here in pieces:
        gate, up = gate_ref[here, :], up_ref[here, :]
        dact = rounded(dot_t(dy_s[here, :], wd_ref[:]))
        sig = jax.nn.sigmoid(gate)
        silu = gate * sig
        act_s[here, :] = (silu * up).astype(BF16)
        dgu_s[here, bf:] = (dact * silu).astype(BF16)
        dgu_s[here, :bf] = (dact * up * (sig * (1 + gate * (1 - sig)))).astype(BF16)
    dwd_ref[:] = dot(dyt_s[:], act_s[:]).astype(BF16).T
    dgu = dot(bt_s[:], dgu_s[:])
    out_s[lax.rem(f, 2), 0] = dgu[:, :bf].astype(BF16)
    out_s[lax.rem(f, 2), 1] = dgu[:, bf:].astype(BF16)
    db_s[:] += dot_t(dgu_s[:], both)
    for c in results(f):
        c.start()

    @pl.when(f == steps - 1)
    def _():
        for p, here in enumerate(pieces):
            wide = mid_s[here, :].astype(F32)
            dy_s[here, :] = (dy_s[here, :].astype(F32) + norm_back(wide, rounded(db_s[here, :]))).astype(BF16)
            stored(p).start()
        finished(f - 1)
        finished(f)
        if cut:
            for name in "gu":
                scatters[name].last(squares_ref)
            for scatter in scatters.values():
                scatter.done()
        for p in range(len(pieces)):
            stored(p).wait()


def mlp_back(layer, dy, mid, gate, up, wg, wu, wd, dlater=None, cut=0, bt=512, bf=256):
    tokens, d = dy.shape
    ff = wg.shape[2]
    anywhere = pl.BlockSpec(memory_space=pl.ANY)
    pair = pl.BlockSpec((None, tokens, bf), lambda f: (layer, 0, f))
    column, row = pl.BlockSpec((None, d, bf), lambda f: (layer, 0, f)), pl.BlockSpec((None, bf, d), lambda f: (layer, f, 0))
    out = lambda *s: jax.ShapeDtypeStruct(s, BF16)
    cuts = [(d // 8, n) for n in (dlater.shape[1], cut, cut)] if cut else []
    squares = [jax.ShapeDtypeStruct((8, 128), F32)] if cut else []
    dma = pltpu.SemaphoreType.DMA
    states, flipped = pltpu.VMEM((tokens, d), BF16), pltpu.VMEM((d, tokens), BF16)
    return pl.pallas_call(
        functools.partial(_mlp_back, bt=bt, cut=cut, layer=layer),
        grid=(ff // bf,),
        in_specs=[anywhere, anywhere, pair, pair, column, column, row, *[anywhere for _ in squares]],
        out_specs=[anywhere, anywhere, anywhere, pl.BlockSpec((bf, d), lambda f: (f, 0)), *[anywhere for _ in cuts],
                   *[whole(*s.shape) for s in squares]],
        out_shape=[out(tokens, d), out(d, ff), out(d, ff), out(ff, d), *[out(*c) for c in cuts[1:] + cuts[:1]], *squares],
        scratch_shapes=[states, states, flipped, flipped, pltpu.VMEM((tokens, d), F32), pltpu.VMEM((tokens, bf), BF16), pltpu.VMEM((tokens, 2 * bf), BF16),
                        pltpu.VMEM((2, 2, d, bf), BF16), dma((tokens // bt, 2)), dma((2, 2)), *(s for c in cuts for s in scatter_scratch(*c))],
        compiler_params=params(collective_id=1, has_side_effects=True) if cut else params(),
        cost_estimate=cost(12 * tokens * d * ff, exps=tokens * ff),
        name="mlp_back",
    )(dy, mid, gate, up, wg, wu, wd, *([dlater] if cut else []))


BACK_PLAN = {
    1: [("exchange", ["g", "u", "d"])],
    2: [("first", ["g"])],
    3: [("first", ["u"])],
    4: [("first", ["d"]), ("exchange", ["o"])],
    6: [("second", ["g"]), ("first", ["o"])],
    8: [("second", ["u"])],
    9: [("second", ["d"])],
    11: [("second", ["o"])],
    12: [("last", ["g"])],
    13: [("last", ["u"])],
    15: [("last", ["d", "o"]), ("done", ["g", "u", "d", "o"])],
}


def _attention_back(*refs, bq, bk, first, since, count):
    dmid_ref, o_ref, q_ref, k_ref, v_ref, lse_ref, h_ref, wo_ref, cos_ref, sin_ref, dwg_ref, dwu_ref, dwd_ref, *refs = refs
    if first:
        *known, gg_ref, gu_ref, gd_ref, go_ref, gq_ref, factor_ref = refs[: first + 6]
        dwqkv_ref, squares_ref, all_s, send_all, recv_all, *refs = refs[first + 6 :]
    else:
        wqkv_ref, dwqkv_ref, gg_ref, gu_ref, gd_ref, go_ref, squares_ref, dh_ref, *refs = refs
    do_s, dq_s, delta_s, dwo_s, dwob_s, dwqkv_s, dqt_s, dk_s, dv_s, hide_s, *refs = refs
    me = places()
    step = pl.program_id(0)
    heads, bt = o_ref.shape[:2]
    n, middle = do_s.shape[1] // bt, do_s.shape[1] // bq
    scatters = {}
    rest = lambda ref: ref.at[:, pl.ds(since, ref.shape[1] - since)]
    for name, src, out in (("g", rest(dwg_ref), gg_ref), ("u", rest(dwu_ref), gu_ref), ("d", dwd_ref, gd_ref)):
        mine, theirs, across, from_x, from_y, send, recv, local, *refs = refs
        scatters[name] = Scatter(me, src, mine, theirs, across, from_x, from_y, out, send, recv, local)
    for name, src, out in (("o", dwob_s, go_ref), *([("qkv", dwqkv_ref, gq_ref)] if first else [])):
        theirs, across, from_x, from_y, send, recv, local, *refs = refs
        scatters[name] = Scatter(me, src, None, theirs, across, from_x, from_y, out, send, recv, local)
    others = range(1, 8) if first else (X, Y, CORE)

    @pl.when(step == 0)
    def _():
        greet(me, others)
        squares_ref[:] = jnp.zeros_like(squares_ref)
        dwo_s[:] = jnp.zeros_like(dwo_s)
        dwqkv_s[:] = jnp.zeros_like(dwqkv_s)
        dk_s[:] = jnp.zeros_like(dk_s)
        dv_s[:] = jnp.zeros_like(dv_s)
        hide_s[:] = hidden(bk, bq, bq)

    @pl.when(step == 1)
    def _():
        pl.semaphore_wait(pltpu.get_barrier_semaphore(), len(others))

    act_on(BACK_PLAN, step, scatters, squares_ref)

    @pl.when(step < n)
    def _():
        rows = pl.ds(pl.multiple_of(step * bt, bt), bt)
        dmid = dmid_ref[:]
        do = dot_t(dmid, wo_ref[:]).astype(BF16)
        for i in range(heads):
            mine = do[:, i * HEAD : (i + 1) * HEAD]
            do_s[i, rows, :] = mine
            delta_s[i : i + 1, rows] = jnp.sum((mine.astype(F32) * o_ref[i].astype(F32)).T, axis=0, keepdims=True)
        dwo_s[:] += dot(side_by_side(o_ref).T, dmid)

        @pl.when(step == n - 1)
        def _():
            dwob_s[:] = dwo_s[:].astype(BF16)

    @pl.when((step >= n) & (step < n + middle))
    def _():
        iq = step - n
        rows = pl.ds(pl.multiple_of(iq * bq, bq), bq)
        scale = HEAD**-0.5
        e = scale * LOG2E
        dqt_s[:] = jnp.zeros_like(dqt_s)

        def block(first, count, hide=None):
            keys = pl.ds(pl.multiple_of(first, bq), count)
            qs, dos = [q_ref[i] for i in range(heads)], [do_s[i, rows, :] for i in range(heads)]
            scores = [dot_t(k_ref[keys, :], x) for x in qs]
            dps = [dot_t(v_ref[keys, :], x) for x in dos]
            for i in range(heads):
                s = scores[i] * e - lse_ref[i : i + 1, :] * LOG2E
                p = jnp.exp2(s if hide is None else s + hide)
                ds = (p * (dps[i] - delta_s[i : i + 1, rows])).astype(BF16)
                dv_s[keys, :] += dot(p.astype(BF16), dos[i])
                dk_s[keys, :] += dot(ds, qs[i])
                dqt_s[i] += dot(k_ref[keys, :].T, ds)

        whole_blocks = lax.div(iq, 2)
        loop(whole_blocks, lambda j, _: block(j * bk, bk))
        pl.when(lax.rem(iq, 2) == 0)(lambda: block(whole_blocks * bk, bq, hide_s[bq:, :]))
        pl.when(lax.rem(iq, 2) == 1)(lambda: block(whole_blocks * bk, bk, hide_s[:]))
        for i in range(heads):
            dq_s[i, rows, :] = (dqt_s[i] * scale).T.astype(BF16)

    @pl.when(step >= n + middle)
    def _():
        rows = pl.ds(pl.multiple_of((step - n - middle) * bt, bt), bt)
        cos, sin = cos_ref[:], sin_ref[:]
        parts = []
        for t in [*(dq_s[i, rows, :] for i in range(heads)), (dk_s[rows, :] * HEAD**-0.5).astype(BF16)]:
            t = t.astype(F32)
            parts.append((t * cos - pltpu.roll(t, HALF, 1) * sin).astype(BF16))
        dz = jnp.concatenate([*parts, dv_s[rows, :].astype(BF16)], axis=1)
        wide = h_ref[:].astype(F32)
        a = (wide * norm_scale(wide)).T.astype(BF16)
        dwqkv_s[:] += dot(a, dz)
        if not first:
            da = rounded(dot_t(dz, wqkv_ref[:]))
            dh_ref[:] = (dmid_ref[:].astype(F32) + norm_back(wide, da)).astype(BF16)

        @pl.when(step == 2 * n + middle - 1)
        def _():
            dwqkv_ref[:] = dwqkv_s[:].astype(BF16)
            if first:
                scatter = scatters["qkv"]
                scatter.exchange()
                for ref in known:
                    squares_ref[:] += ref[:]
                scatter.first()
                scatter.second()
                scatter.last(squares_ref)
                factor_ref[:] = clipping(me, squares_ref, all_s, send_all, recv_all, count)
                scatter.done()


def attention_back(layer, dmid, o, q, k, v, lse, h, wo, cos, sin, dwg, dwu, dwd, wqkv=None, since=0, known=(), count=0, bq=256, bk=512,
                   bt=512):
    tokens, d = dmid.shape
    heads = o.shape[1]
    wide = d + 2 * HEAD
    n, inner = tokens // bt, tokens // bq
    one = pl.Buffered(1)
    early = lambda s: jnp.minimum(s, n - 1)
    middle = lambda s: jnp.clip(s - n, 0, inner - 1)
    late = lambda s: jnp.maximum(s - n - inner, 0)
    twice = early if wqkv is None else lambda s: jnp.where(s < n, s, late(s))
    rows = lambda w, which: pl.BlockSpec((bt, w), lambda s: (which(s), 0))
    by_head = lambda which, block: pl.BlockSpec((None, heads, block, HEAD), lambda s: (layer, 0, which(s), 0))
    all_of = lambda a: pl.BlockSpec((None, *a.shape[1:]), lambda s: (layer, 0, 0), pipeline_mode=one)
    anywhere = pl.BlockSpec(memory_space=pl.ANY)
    cuts = [(a.shape[0] // 8, a.shape[1] - first) for a, first in ((dwg, since), (dwu, since), (dwd, 0))]
    cut_o = (d // 8, d)
    out = lambda s: jax.ShapeDtypeStruct(s, BF16)
    tile, dma = jax.ShapeDtypeStruct((8, 128), F32), pltpu.SemaphoreType.DMA
    blocks, block_shapes = [anywhere] * 4, [*(out(c) for c in cuts), out(cut_o)]
    if known:
        more, more_in = known, [whole(8, 128) for _ in known]
        outs, shapes = [*blocks, anywhere, whole(8, 128)], [*block_shapes, out((d // 8, wide)), tile]
        own = [pltpu.VMEM((d, wide), BF16), pltpu.VMEM((8, 128), F32), pltpu.VMEM((8, 8, 128), F32), dma((8,)), dma((8,))]
    else:
        more, more_in = [wqkv], [all_of(wqkv)]
        outs, shapes = [whole(d, wide), *blocks, whole(8, 128), rows(d, late)], [out((d, wide)), *block_shapes, tile, out((tokens, d))]
        own = []
    flops = 4 * tokens * d * (d + wide) + 5 * heads * tokens * tokens * HEAD
    return pl.pallas_call(
        functools.partial(_attention_back, bq=bq, bk=bk, first=len(known), since=since, count=count),
        grid=(2 * n + inner,),
        in_specs=[rows(d, twice), by_head(early, bt), by_head(middle, bq), all_of(k), all_of(v),
                  pl.BlockSpec((None, heads, bq), lambda s: (layer, 0, middle(s))), rows(d, late), all_of(wo),
                  rows(HEAD, late), rows(HEAD, late), anywhere, anywhere, anywhere, *more_in],
        out_specs=outs,
        out_shape=shapes,
        scratch_shapes=[*own, pltpu.VMEM((heads, tokens, HEAD), BF16), pltpu.VMEM((heads, tokens, HEAD), BF16), pltpu.VMEM((heads, tokens), F32),
                        pltpu.VMEM((d, d), F32), pltpu.VMEM((d, d), BF16), pltpu.VMEM((d, wide), F32),
                        pltpu.VMEM((heads, HEAD, bq), F32), pltpu.VMEM((tokens, HEAD), F32), pltpu.VMEM((tokens, HEAD), F32),
                        pltpu.VMEM((bk, bq), F32), *(s for c in cuts for s in scatter_scratch(*c)),
                        *scatter_scratch(*cut_o, in_vmem=True), *(scatter_scratch(d // 8, wide, in_vmem=True) if known else [])],
        compiler_params=params(collective_id=2 + layer, has_side_effects=True),
        cost_estimate=cost(flops, exps=heads * tokens * tokens // 2),
        name="attention_back",
    )(dmid, o, q, k, v, lse, h, wo, cos, sin, dwg, dwu, dwd, *more)


def clipping(me, squares, all_s, send, recv, count):
    copies = [pltpu.make_async_remote_copy(src_ref=squares, dst_ref=all_s.at[bits], send_sem=send.at[bits], recv_sem=recv.at[bits],
                                           device_id=(0, me[bits]), device_id_type=pl.DeviceIdType.MESH) for bits in range(1, 8)]
    for c in copies:
        c.start()
    for c in copies:
        c.wait_recv()
    sums = [jnp.sum(squares[:]), *(jnp.sum(all_s[bits]) for bits in range(1, 8))]
    while len(sums) > 1:
        sums = [a + b for a, b in zip(sums[::2], sums[1::2])]
    for c in copies:
        c.wait_send()
    return jnp.minimum(1.0, 0.5 * lax.rsqrt(jnp.full((8, 128), sums[0] / count) + 1e-30))


def _update(factor_ref, *refs, sources):
    count, layers = len(sources), len(sources[0])
    take = lambda many: [refs.pop(0) for _ in range(many)]
    refs = list(refs)
    weights, m, v = take(count), take(count), take(count)
    grads = take(len(refs) - 7 * count - 2)
    outs = [take(count) for _ in range(3)]
    w_s, m_s, v_s, g_s = (take(count) for _ in range(4))
    in_sem, out_sem = refs
    factor = factor_ref[0, 0]

    def inputs(i, n):
        pairs = [(weights[i].at[n], w_s[i].at[n]), (m[i].at[n], m_s[i].at[n]), (v[i].at[n], v_s[i].at[n])]
        pairs += [(grads[a].at[:, pl.ds(first, cols)], g_s[i].at[n, :, pl.ds(at, cols)]) for a, first, at, cols in sources[i][n]]
        return [pltpu.make_async_copy(a, b, in_sem.at[i, n, j]) for j, (a, b) in enumerate(pairs)]

    def results(i, n):
        return [pltpu.make_async_copy(s[i].at[n], outs[j][i].at[n], out_sem.at[i, n, j]) for j, s in enumerate((w_s, m_s, v_s))]

    order = [(i, n) for i in reversed(range(count)) for n in range(layers)]
    for at in order:
        for c in inputs(*at):
            c.start()
    for i, n in order:
        for c in inputs(i, n):
            c.wait()

        def some(j, _):
            rows = pl.ds(pl.multiple_of(j * 16, 16), 16)
            g = g_s[i][n, rows, :].astype(F32) * factor
            m = 0.9 * m_s[i][n, rows, :] + 0.1 * g
            v = 0.95 * v_s[i][n, rows, :] + 0.05 * g * g
            w = w_s[i][n, rows, :].astype(F32)
            m_s[i][n, rows, :] = m
            v_s[i][n, rows, :] = v
            w_s[i][n, rows, :] = (w - 0.02 * (m * lax.rsqrt(v + 1e-8) + 0.1 * w)).astype(BF16)

        loop(w_s[i].shape[1] // 16, some)
        for c in results(i, n):
            c.start()
    for at in order:
        for c in results(*at):
            c.wait()


def update(factor, weights, m, v, grads, sources):
    anywhere = pl.BlockSpec(memory_space=pl.ANY)
    arrays = [*weights, *m, *v]
    dma = pltpu.SemaphoreType.DMA
    grid = (len(weights), weights[0].shape[0])
    return pl.pallas_call(
        functools.partial(_update, sources=sources),
        in_specs=[pl.BlockSpec(memory_space=pltpu.SMEM)] + [anywhere] * (len(arrays) + len(grads)),
        out_specs=[anywhere] * len(arrays),
        out_shape=[jax.ShapeDtypeStruct(a.shape, a.dtype) for a in arrays],
        scratch_shapes=[pltpu.VMEM(a.shape, a.dtype) for a in [*arrays, *weights]] + [dma((*grid, 5)), dma((*grid, 3))],
        compiler_params=params(),
        name="update",
    )(factor, *arrays, *grads)


def solution(mesh):
    def step(x, dy, *arrays):
        weights, m, v = (arrays[i : i + 7] for i in (0, 7, 14))
        tokens, d = x.shape[1:]
        ff = weights[4].shape[2]
        cos, sin = tables(tokens)
        *full, q, k, v_, o, lse, mid, gate, up, h1 = forward(x[0], weights, cos, sin)
        fqkv, fo, fg, fu, fd = full
        dmid, dwg, dwu, dwd = mlp_back(1, dy[0], mid, gate, up, fg, fu, fd)
        dlater, g1, u1, d1, o1, s1, dh = attention_back(1, dmid, o, q, k, v_, lse, h1, fo, cos, sin, dwg, dwu, dwd, wqkv=fqkv)
        dmid, dwg, dwu, dwd, ga, ua, qkv1, s2 = mlp_back(0, dh, mid, gate, up, fg, fu, fd, dlater, CUT)
        gb, ub, d0, o0, qkv0, factor = attention_back(0, dmid, o, q, k, v_, lse, x[0], fo, cos, sin, dwg, dwu, dwd, since=CUT, known=[s1, s2],
                                                      count=8 * sum(w.size for w in weights))
        grads = {"qkv": [qkv0, qkv1], "o": [o0, o1], "g": [ga, gb, g1], "u": [ua, ub, u1], "d": [d0, d1]}
        flat = [g for some in grads.values() for g in some]

        def source(name, layer, first=0, cols=d):
            start = [g is grads[name][0] for g in flat].index(True)
            if name in "gu":
                return [(start, 0, 0, CUT), (start + 1, 0, CUT, ff - CUT)] if layer == 0 else [(start + 2, 0, 0, ff)]
            return [(start + layer, first, 0, cols)]

        layers = range(weights[0].shape[0])
        sources = [[source(*what[:1], n, *what[1:]) for n in layers] for what in
                   (("qkv",), ("qkv", d, HEAD), ("qkv", d + HEAD, HEAD), ("o",), ("g",), ("u",), ("d",))]
        return tuple(update(factor, weights, m, v, flat, sources))

    states, cut = P(("rep", "dp"), None, None), P(None, "dp", None)
    return jax.shard_map(
        step,
        mesh=mesh,
        in_specs=(states, states) + (cut,) * 21,
        out_specs=(P("rep", "dp", None),) * 21,
        check_vma=False,
    )
```

```python
import functools

import jax
import jax.numpy as jnp
import numpy as np
from jax import lax
from jax.experimental import pallas as pl
from jax.experimental.pallas import tpu as pltpu
from jax.sharding import PartitionSpec as P

NEG = -1e30
HIDDEN = 2 * NEG
LOG2E = 1.4426950408889634
VMEM = 127 * 2**19
STRIP = 512
HEAD = 128
HALF = HEAD // 2
TILE = (8, 128)
THETA = 10000
F32, BF16 = jnp.float32, jnp.bfloat16


def dot(a, b, ca=1, cb=0):
    return lax.dot_general(a, b, (((ca,), (cb,)), ((), ())), preferred_element_type=F32)


def dot_t(a, b):
    return dot(a, b, 1, 1)


def loop(stop, body, start=0):
    lax.fori_loop(start, stop, body, None)


def rounded(a):
    return a.astype(BF16).astype(F32)


def norm_scale(wide):
    return lax.rsqrt(jnp.mean(wide * wide, -1, keepdims=True) + 1e-6)


def norm_back(wide, by):
    scale = norm_scale(wide)
    return scale * (by - wide * (scale * scale * jnp.mean(by * wide, -1, keepdims=True)))


def params(**more):
    return pltpu.CompilerParams(vmem_limit_bytes=VMEM, **more)


def whole(*shape):
    return pl.BlockSpec(shape, lambda *_: (0,) * len(shape))


def cost(flops, nbytes=0, exps=0):
    return pl.CostEstimate(flops=int(flops), bytes_accessed=int(nbytes), transcendentals=int(exps))


def tables(tokens):
    angle = np.arange(tokens, dtype=np.float64)[:, None] * THETA ** (-np.arange(HALF, dtype=np.float64) / HALF)
    cos, sin = np.cos(angle), np.sin(angle)
    return jnp.asarray(np.concatenate([cos, cos], 1), F32), jnp.asarray(np.concatenate([-sin, sin], 1), F32)


def hidden(keys, queries, later=0):
    gap = lax.broadcasted_iota(jnp.int32, (keys, queries), 1) - lax.broadcasted_iota(jnp.int32, (keys, queries), 0)
    return jnp.where(gap + later >= 0, 0.0, HIDDEN)


def side_by_side(ref):
    return jnp.concatenate([ref[n] for n in range(ref.shape[0])], axis=1)


X, Y, CORE, HERE = 4, 2, 1, 0
OTHERS = range(1, 8)
NEAR = (HERE, X, Y, X + Y)


def places():
    at = [lax.axis_index("dp")]
    for bit in (CORE, Y, X):
        at += [n + bit - 2 * bit * lax.rem(lax.div(n, bit), 2) for n in at]
    return at


def greet(me, all_of=(X, Y, CORE)):
    barrier = pltpu.get_barrier_semaphore()
    for bits in all_of:
        pl.semaphore_signal(barrier, inc=1, device_id=(0, me[bits]), device_id_type=pl.DeviceIdType.MESH)
    return lambda: pl.semaphore_wait(barrier, len(all_of))


def remote(me, bit, src, dst, send, recv):
    return pltpu.make_async_remote_copy(src_ref=src, dst_ref=dst, send_sem=send, recv_sem=recv, device_id=(0, me[bit]),
                                        device_id_type=pl.DeviceIdType.MESH)


def halves(r):
    a = (r // 2 + 15) // 16 * 16
    return (0, a), (a, r - a)


def upper(r):
    return halves(r)[0]


def lower(r):
    return halves(r)[1]


ALL = None
ROUTES = {"x": (X, HERE, ALL), "y": (Y, HERE, ALL), "core": (CORE, HERE, ALL), "xy": (Y, X, upper), "x core": (CORE, X, ALL),
          "yx": (X, Y, lower), "y core": (CORE, Y, ALL), "xy core": (CORE, X + Y, upper), "yx core": (CORE, X + Y, lower)}


class Gather:
    def __init__(self, me, block, full, send, recv, cols, at):
        first, count = cols
        self.me, self.r = me, block.shape[0]
        self.full, self.send, self.recv = full, send, recv
        self.own, self.cols = block.at[:, pl.ds(first, count)], pl.ds(at + first, count)

    def rows(self, bits, part=None):
        first, count = part or (0, self.r)
        at = pl.multiple_of(self.me[bits] * self.r + first, 16)
        return self.full.at[pl.ds(at, count), self.cols]

    def copy(self, which, got=False):
        bit, bits, part = ROUTES[which]
        there = self.rows(bits + bit if got else bits, part and part(self.r))
        n = tuple(ROUTES).index(which)
        return remote(self.me, bit, self.own if bits == HERE and not got else there, there, self.send.at[n], self.recv.at[n])

    def got(self, which):
        self.copy(which, got=True).wait_recv()

    def begin(self):
        for n in ("x", "y", "core"):
            self.copy(n).start()

    def hand_on(self):
        self.got("x")
        self.copy("xy").start()
        self.copy("x core").start()
        self.got("y")
        self.copy("yx").start()
        self.copy("y core").start()

    def finish(self):
        self.got("xy")
        self.copy("xy core").start()
        self.got("yx")
        self.copy("yx core").start()

    def arrived(self):
        for n in ("core", "x core", "y core", "xy core", "yx core"):
            self.got(n)

    def sent(self):
        for n in ROUTES:
            self.copy(n).wait_send()


class Scatter:
    def __init__(self, me, src, mine, theirs, across, from_x, from_y, out, send, recv, local):
        self.me, self.src, self.out = me, src, out
        self.r, self.n = theirs.shape[1:]
        self.own, self.theirs, self.across, self.from_x, self.from_y = mine, theirs, across, from_x, from_y
        self.send, self.recv, self.local = send, recv, local
        self.a, self.b = halves(self.r)
        self.all = (0, self.r)

    def block(self, bits, part=None):
        first, count = part or self.all
        return self.src.at[pl.ds(pl.multiple_of(self.me[bits] * self.r + first, 16), count)]

    def mine(self, j, part):
        return self.block(NEAR[j], part) if self.own is None else self.own.at[j, pl.ds(*part)]

    def load(self, j):
        return pltpu.make_async_copy(self.block(NEAR[j]), self.own.at[j], self.local.at[j])

    def copy(self, n):
        if n < 4:
            bit, src, dst = CORE, self.block(CORE + NEAR[n]), self.theirs.at[n]
        else:
            bit, j, part, to = ((X, 3, self.a, self.across), (Y, 3, self.b, self.across), (X, 1, self.a, self.from_x),
                                (Y, 2, self.b, self.from_y), (Y, 2, self.a, self.from_y), (X, 1, self.b, self.from_x))[n - 4]
            src, dst = self.mine(j, part), to.at[pl.ds(*part)]
        return remote(self.me, bit, src, dst, self.send.at[n], self.recv.at[n])

    def add(self, j, part, *more):
        step = 16
        ref = self.mine(j, part)

        def one(i, _):
            rows = pl.ds(pl.multiple_of(i * step, step), step)
            full = pl.ds(pl.multiple_of(part[0] + i * step, step), step)
            total = ref[rows, :].astype(F32) + self.theirs[j, full, :].astype(F32)
            for other in more:
                total += other[full, :].astype(F32)
            ref[rows, :] = total.astype(BF16)

        loop(part[1] // step, one)

    def exchange(self):
        for j in range(4):
            self.copy(j).start()
            if self.own is not None:
                self.load(j).start()

    def first(self):
        for j in range(4):
            if self.own is not None:
                self.load(j).wait()
            self.copy(j).wait_recv()
        self.add(3, self.all)
        self.copy(4).start()
        self.copy(5).start()
        self.add(1, self.a)
        self.add(2, self.b)

    def second(self):
        self.copy(6).start()
        self.copy(7).start()
        self.copy(4).wait_recv()
        self.add(2, self.a, self.across)
        self.copy(8).start()
        self.copy(5).wait_recv()
        self.add(1, self.b, self.across)
        self.copy(9).start()

    def result(self):
        return pltpu.make_async_copy(self.mine(0, self.all), self.out, self.local.at[4])

    def last(self, squares):
        for n in range(6, 10):
            self.copy(n).wait_recv()
        self.add(0, self.all, self.from_x, self.from_y)
        ref = self.mine(0, self.all)
        self.result().start()
        squares[:] += sum_of_squares(ref)

    def done(self):
        for n in range(10):
            self.copy(n).wait_send()
        self.result().wait()


def sum_of_squares(ref):
    rows, cols = ref.shape

    def one(i, total):
        g = ref[pl.ds(pl.multiple_of(i * 16, 16), 16), :].astype(F32)
        g = g * g
        for c in range(0, cols, 128):
            total += g[:8, c : c + 128] + g[8:, c : c + 128]
        return total

    return lax.fori_loop(0, rows // 16, one, jnp.zeros(TILE, F32))


def scatter_scratch(r, n, in_vmem=False):
    dma = pltpu.SemaphoreType.DMA
    block = pltpu.VMEM((r, n), BF16)
    return [*([] if in_vmem else [pltpu.VMEM((4, r, n), BF16)]), pltpu.VMEM((4, r, n), BF16), block, block, block,
            dma((10,)), dma((10,)), dma((5,))]


BQ = BK = BT = BF = 512
CUT, CUT_Q = 2 * BF, 4 * HEAD
TENSORS = ("qa", "qb", "k", "v", "o", "ga", "ua", "gb", "ub", "d")
QKV, GU_A, GU_B = ["qa", "k", "v", "qb"], ["ga", "ua"], ["gb", "ub"]


def _forward(x_ref, sq, sk, sv, so, sg, su, sd, cos_ref, sin_ref, fqkv, fo, fg, fu, fd, q_o, k_o, v_o, o_o, lse_o, mid_o, gate_o, up_o, h_o,
             h_s, b_s, q_s, k_s, v_s, o_s, lse_s, act_s, wqkv_s, wo_s, wg_s, wu_s, wd_s, stage_s, top_s, mix_s, hide_s,
             send, recv, load, keep, out, wsem):
    layer, layers = pl.program_id(0), pl.num_programs(0)
    me = places()
    tokens, d = h_s.shape
    heads = q_s.shape[0]
    ff = act_s.shape[1]
    blocks = tokens // BT

    def gather(n, name):
        i = TENSORS.index(name)
        shard, full, cols, at = {
            "qa": (sq, fqkv, (0, CUT_Q), 0), "qb": (sq, fqkv, (CUT_Q, d - CUT_Q), 0), "k": (sk, fqkv, (0, HEAD), d),
            "v": (sv, fqkv, (0, HEAD), d + HEAD), "o": (so, fo, (0, d), 0), "d": (sd, fd, (0, d), 0),
            "ga": (sg, fg, (0, CUT), 0), "gb": (sg, fg, (CUT, ff - CUT), 0),
            "ua": (su, fu, (0, CUT), 0), "ub": (su, fu, (CUT, ff - CUT), 0)}[name]
        full = wqkv_s if name in QKV and n == 0 else full.at[n]
        return Gather(me, shard.at[n], full, send.at[n, i], recv.at[n, i], cols, at)

    def own_blocks():
        at = 0
        for s, f, column in ((sq, fqkv, 0), (sk, fqkv, d), (sv, fqkv, d + HEAD), (so, fo, 0), (sg, fg, 0), (su, fu, 0), (sd, fd, 0)):
            r, n = s.shape[1:]
            for i in range(s.shape[0]):
                where = pl.ds(pl.multiple_of(me[HERE] * r, 16), r), pl.ds(column, n)
                if f is fqkv and i == 0:
                    yield s.at[i], wqkv_s.at[where], None
                else:
                    yield s.at[i], act_s.at[pl.ds(at, r), pl.ds(0, n)], f.at[i, *where]
                    at += r

    copies_in = lambda: [pltpu.make_async_copy(a, b, load.at[i]) for i, (a, b, _) in enumerate(own_blocks())]
    copies_out = lambda: [pltpu.make_async_copy(b, c, load.at[i]) for i, (_, b, c) in enumerate(own_blocks()) if c is not None]
    here = lambda i, n: pl.ds(pl.multiple_of(i * n, n), n)

    def kept(*names):
        pairs = {"x": (x_ref, h_s), "q": (q_s, q_o.at[layer]), "k": (k_s, k_o.at[layer]), "v": (v_s, v_o.at[layer]), "o": (o_s, o_o.at[layer]),
                 "lse": (lse_s, lse_o.at[layer]), "mid": (h_s, mid_o.at[layer]), "h": (h_s, h_o), "qkv": (wqkv_s, fqkv.at[layer])}
        return [pltpu.make_async_copy(*pairs[n], keep.at[list(pairs).index(n)]) for n in names]

    def start(*copies):
        for c in copies:
            c.start()

    def wait(*copies):
        for c in copies:
            c.wait()

    def weight(n, name):
        return pltpu.make_async_copy(*{"qb": (fqkv.at[n], wqkv_s, wsem.at[0]), "o": (fo.at[n], wo_s, wsem.at[1]),
                                       "d": (fd.at[n], wd_s, wsem.at[2])}[name])

    def column(c, n=layer):
        cols, slot = here(c, BF), lax.rem(c, 2)
        return (pltpu.make_async_copy(fg.at[n, :, cols], wg_s.at[slot], wsem.at[3 + slot]),
                pltpu.make_async_copy(fu.at[n, :, cols], wu_s.at[slot], wsem.at[5 + slot]))

    def fetch(n, name):
        gather(n, name).arrived()
        if name in QKV:
            gather(0, name).sent()
        if name == "ua":
            start(*column(0, n))
        elif name in ("qb", "o", "d"):
            start(weight(n, name))

    def tick(phase, i):
        for n, plan in enumerate(PLAN):
            for p, k, *actions in plan:
                if p == phase:
                    @pl.when((layer == n) & (i == k))
                    def _():
                        for do, later, names in actions:
                            for name in names:
                                if do == "fetch":
                                    fetch(n + later, name)
                                else:
                                    getattr(gather(n + later, name), do)()

    @pl.when(layer == 0)
    def _():
        greeted = greet(me)
        start(*kept("x"), *copies_in())
        hide_s[:] = hidden(BK, BQ)
        greeted()
        for name in QKV:
            gather(0, name).begin()
        wait(*copies_in())
        start(*copies_out())
        wait(*kept("x"))
        for name in QKV:
            gather(0, name).hand_on()
        for name in ("o", *GU_A):
            gather(0, name).begin()
        wait(*copies_out())
        for do in (Gather.finish, Gather.arrived):
            for name in QKV:
                do(gather(0, name))

    @pl.when(layer > 0)
    def _():
        start(*kept("h"))
        wait(weight(1, "qb"))

    def qkv_step(i):
        rows = here(i, BT)
        wide = h_s[rows, :].astype(F32)
        a = (wide * norm_scale(wide)).astype(BF16)
        z = dot(a, wqkv_s[:])
        cos, sin = cos_ref[rows, :], sin_ref[rows, :]
        for n in range(heads + 1):
            t = rounded(z[:, n * HEAD : (n + 1) * HEAD])
            t = (t * cos + pltpu.roll(t, HALF, 1) * sin).astype(BF16)
            if n < heads:
                q_s[n, rows, :] = t
            else:
                k_s[rows, :] = t
        v_s[rows, :] = z[:, (heads + 1) * HEAD :].astype(BF16)

    pairwise(blocks, qkv_step, lambda i: tick("qkv", i))
    start(*kept("q", "k", "v"))

    @pl.when(layer == 0)
    def _():
        start(*kept("qkv"))

    scale = HEAD**-0.5
    e = scale * LOG2E

    def attend_step(i, _):
        top_s[:] = jnp.full(top_s.shape, NEG, F32)
        mix_s[:] = jnp.zeros(mix_s.shape, F32)

        def block(first, count, at=0, hidden=None):
            keys, cols = pl.ds(pl.multiple_of(first, BK // 2), count), pl.ds(at, BQ - at)
            rows = pl.ds(pl.multiple_of(i * BQ + at, BQ // 2), BQ - at)
            values = jnp.concatenate([v_s[keys, :].T, jnp.ones((8, count), BF16)], axis=0)
            scores = [dot_t(k_s[keys, :], q_s[n, rows, :]) for n in range(heads)]
            weights = []
            for n, s in enumerate(scores):
                s = s if hidden is None else s + hidden
                old = top_s[n : n + 1, cols]
                top = jnp.maximum(old, s.max(axis=0, keepdims=True))
                top_s[n : n + 1, cols] = top
                weights.append((jnp.exp2((s - top) * e).astype(BF16), jnp.exp2((old - top) * e)))
            for n, (p, rest) in enumerate(weights):
                mix_s[n, :, cols] = mix_s[n, :, cols] * rest + dot(values, p)

        def before(j, _):
            tick("attend", lax.div(i * (i + 1), 2) + j)
            block(j * BK, BK)

        loop(i, before)
        tick("attend", lax.div(i * (i + 3), 2))
        half = BK // 2
        block(i * BK, half, hidden=hide_s[:half, :])
        block(i * BK + half, half, half, hide_s[half:, half:])
        rows = here(i, BQ)
        for n in range(heads):
            total = mix_s[n, HEAD : HEAD + 1, :]
            o_s[n, rows, :] = (mix_s[n, :HEAD, :] * (1 / total)).T.astype(BF16)
            lse_s[n : n + 1, rows] = top_s[n : n + 1, :] * scale + jnp.log(total)

    loop(tokens // BQ, attend_step)
    start(*kept("o", "lse"))

    @pl.when(layer == 0)
    def _():
        wait(*kept("qkv"))

    @pl.when(layer > 0)
    def _():
        wait(*kept("h"))

    wait(weight(layer, "o"))

    def out_step(i):
        rows = here(i, BT)
        o = jnp.concatenate([o_s[n, rows, :] for n in range(heads)], axis=1)
        mid = (h_s[rows, :].astype(F32) + rounded(dot(o, wo_s[:]))).astype(BF16)
        h_s[rows, :] = mid
        wide = mid.astype(F32)
        b_s[rows, :] = (wide * norm_scale(wide)).astype(BF16)

    pairwise(blocks, out_step, lambda i: tick("out", i))
    start(*kept("mid"))

    def staged(i, c):
        rows, cols = here(i, BT), here(c, BF)
        return [pltpu.make_async_copy(stage_s.at[i, w], ref.at[layer, rows, cols], out.at[i, w]) for w, ref in enumerate((gate_o, up_o))]

    def gate_column(c, _):
        wait(*column(c))

        def gate_step(i):
            rows = here(i, BT)
            b = b_s[rows, :]
            gate, up = dot(b, wg_s[lax.rem(c, 2)]), dot(b, wu_s[lax.rem(c, 2)])
            stage_s[i, 0] = gate
            stage_s[i, 1] = up
            act_s[rows, here(c, BF)] = (gate * jax.nn.sigmoid(gate) * up).astype(BF16)
            start(*staged(i, c))

        for i in range(0, blocks, 2):
            tick("gate", 2 * c + i // 2)
            if i > 0:
                pl.when(c + 1 < ff // BF)(lambda: start(*column(c + 1)))

            @pl.when((layer > 0) | (c > 0))
            def _():
                wait(*staged(i, c), *staged(i + 1, c))

            gate_step(i)
            gate_step(i + 1)

    loop(ff // BF, gate_column)
    wait(*kept("q", "k", "v", "o", "lse", "mid"))

    @pl.when(layer < layers - 1)
    def _():
        wait(weight(0, "d"))

        def down_step(i):
            rows = here(i, BT)
            h_s[rows, :] = (h_s[rows, :].astype(F32) + rounded(dot(act_s[rows, :], wd_s[:]))).astype(BF16)

        pairwise(blocks, down_step, lambda i: tick("down", i))
        tick("end", 0)

    @pl.when(layer == layers - 1)
    def _():
        gather(1, "d").arrived()
        for i in range(blocks):
            wait(*staged(i, 0))
        for n in range(2):
            for name in TENSORS:
                if name not in QKV or n > 0:
                    gather(n, name).sent()


def pairwise(count, body, first):
    def two(i, _):
        first(i)
        body(2 * i)
        body(2 * i + 1)

    loop(count // 2, two)


THIS, NEXT = range(2)
PLAN = ([
    ("qkv", 1, ("hand_on", THIS, ["o"]), ("begin", THIS, GU_B)),
    ("attend", 3, ("hand_on", THIS, GU_A), ("finish", THIS, ["o"])),
    ("attend", 8, ("fetch", THIS, ["o"])),
    ("attend", 9, ("hand_on", THIS, GU_B), ("begin", THIS, ["d"])),
    ("out", 1, ("finish", THIS, GU_A), ("fetch", THIS, GU_A)),
    ("gate", 2, ("finish", THIS, GU_B)),
    ("gate", 3, ("fetch", THIS, GU_B)),
    ("gate", 4, ("begin", NEXT, QKV)),
    ("gate", 6, ("hand_on", THIS, ["d"])),
    ("gate", 8, ("hand_on", NEXT, QKV), ("begin", NEXT, ["o"])),
    ("gate", 9, ("finish", THIS, ["d"]), ("fetch", THIS, ["d"])),
    ("down", 0, ("finish", NEXT, QKV), ("begin", NEXT, GU_A)),
    ("down", 1, ("fetch", NEXT, QKV)),
], [
    ("qkv", 0, ("hand_on", THIS, ["o"])),
    ("qkv", 1, ("begin", THIS, ["gb"])),
    ("attend", 1, ("hand_on", THIS, GU_A), ("begin", THIS, ["ub"])),
    ("attend", 4, ("finish", THIS, ["o"])),
    ("attend", 7, ("fetch", THIS, ["o"])),
    ("attend", 8, ("finish", THIS, GU_A)),
    ("attend", 9, ("hand_on", THIS, GU_B), ("begin", THIS, ["d"])),
    ("out", 1, ("fetch", THIS, GU_A)),
    ("gate", 2, ("finish", THIS, GU_B)),
    ("gate", 3, ("fetch", THIS, GU_B)),
    ("gate", 6, ("hand_on", THIS, ["d"])),
    ("gate", 9, ("finish", THIS, ["d"])),
])


def forward(x, shards, cos, sin):
    tokens, d = x.shape
    layers = shards[0].shape[0]
    heads, ff = d // HEAD, shards[4].shape[2]
    full = [jax.ShapeDtypeStruct((layers, *s), BF16) for s in ((d, d + 2 * HEAD), (d, d), (d, ff), (d, ff), (ff, d))]
    shape = lambda *s: jax.ShapeDtypeStruct((layers, *s), BF16)
    wide = jax.ShapeDtypeStruct((layers, tokens, ff), F32)
    once = lambda a: pl.BlockSpec(a.shape, lambda i: (0,) * len(a.shape), pipeline_mode=pl.Buffered(1))
    anywhere = pl.BlockSpec(memory_space=pl.ANY)
    dma = pltpu.SemaphoreType.DMA
    outs = [*full, shape(heads, tokens, HEAD), shape(tokens, HEAD), shape(tokens, HEAD), shape(heads, tokens, HEAD),
            jax.ShapeDtypeStruct((layers, heads, tokens), F32), shape(tokens, d), wide, wide, jax.ShapeDtypeStruct((tokens, d), BF16)]
    states, by_head, one_head = pltpu.VMEM((tokens, d), BF16), pltpu.VMEM((heads, tokens, HEAD), BF16), pltpu.VMEM((tokens, HEAD), BF16)
    matrix, columns = lambda i: pltpu.VMEM(full[i].shape[1:], BF16), pltpu.VMEM((2, d, BF), BF16)
    routes = dma((layers, len(TENSORS), len(ROUTES)))
    return pl.pallas_call(
        _forward,
        grid=(layers,),
        in_specs=[anywhere] * 8 + [once(cos), once(sin)],
        out_specs=[anywhere] * len(outs),
        out_shape=outs,
        scratch_shapes=[states, states, by_head, one_head, one_head, by_head, pltpu.VMEM((heads, tokens), F32), pltpu.VMEM((tokens, ff), BF16),
                        matrix(0), matrix(1), columns, columns, matrix(4), pltpu.VMEM((tokens // BT, 2, BT, BF), F32),
                        pltpu.VMEM((heads, BQ), F32), pltpu.VMEM((heads, HEAD + 8, BQ), F32), pltpu.VMEM((BK, BQ), F32),
                        routes, routes, dma((7 * layers,)), dma((9,)), dma((tokens // BT, 2)), dma((7,))],
        compiler_params=params(collective_id=0, has_side_effects=True),
        cost_estimate=cost(4 * tokens * (7 * HEAD * 1200 + 3 * d * ff)),
        name="forward",
    )(x, *shards, cos, sin)


def act_on(plan, step, scatters, squares):
    for at, actions in plan.items():
        @pl.when(step == at)
        def _():
            for what, names in actions:
                for name in names:
                    getattr(scatters[name], what)(*([squares] if what == "last" else []))


MLP_PLAN = {
    1: [("exchange", ["qkv"])],
    2: [("first", ["qkv"])],
    3: [("second", ["qkv"])],
    5: [("exchange", ["g", "u"])],
    6: [("first", ["g", "u"]), ("last", ["qkv"])],
    7: [("second", ["g", "u"])],
}


def _mlp_back(*refs, bt, cut, layer):
    dy_ref, mid_ref, gate_ref, up_ref, wg_ref, wu_ref, wd_ref, *refs = refs
    ready = lambda copies: [c.wait() for c in copies]
    if cut:
        dlater_ref, dmid_ref, dwg_ref, dwu_ref, dwd_ref, gg_ref, gu_ref, gq_ref, squares_ref, *refs = refs
    else:
        dmid_ref, dwg_ref, dwu_ref, dwd_ref, *refs = refs
    dy_s, mid_s, gu_s, bt_s, dyt_s, db_s, act_s, dgu_s, out_s, in_sem, gu_sem, out_sem, *refs = refs
    f, steps = pl.program_id(0), pl.num_programs(0)
    tokens = dy_s.shape[0]
    bf = act_s.shape[1]
    pieces = [pl.ds(at, bt) for at in range(0, tokens, bt)]

    def loads(p):
        return [pltpu.make_async_copy(ref.at[pieces[p]], s.at[pieces[p]], in_sem.at[p, w])
                for w, (ref, s) in enumerate(((dy_ref, dy_s), (mid_ref.at[layer], mid_s)))]

    def hidden_blocks(f):
        cols, slot = pl.ds(pl.multiple_of(f * bf, bf), bf), lax.rem(f, 2)
        return [pltpu.make_async_copy(ref.at[layer, :, cols], gu_s.at[slot, w], gu_sem.at[slot, w]) for w, ref in enumerate((gate_ref, up_ref))]

    def stored(p):
        return pltpu.make_async_copy(dy_s.at[pieces[p]], dmid_ref.at[pieces[p]], in_sem.at[p, 0])

    def results(f):
        cols, slot = pl.ds(pl.multiple_of(f * bf, bf), bf), lax.rem(f, 2)
        return [pltpu.make_async_copy(out_s.at[slot, w], ref.at[:, cols], out_sem.at[slot, w]) for w, ref in enumerate((dwg_ref, dwu_ref))]

    finished = lambda f: ready(results(f))

    @pl.when(f == 0)
    def _():
        for copies in (*map(loads, range(len(pieces))), hidden_blocks(f)):
            for c in copies:
                c.start()

    @pl.when(f + 1 < steps)
    def _():
        for c in hidden_blocks(f + 1):
            c.start()

    @pl.when(f >= 2)
    def _():
        finished(f - 2)

    if cut:
        me = places()
        scatters = {}
        firsts = lambda ref: ref.at[:, pl.ds(0, cut)]
        for name, src, out in (("qkv", dlater_ref, gq_ref), ("g", firsts(dwg_ref), gg_ref), ("u", firsts(dwu_ref), gu_ref)):
            mine, theirs, across, from_x, from_y, send, recv, local, *refs = refs
            scatters[name] = Scatter(me, src, mine, theirs, across, from_x, from_y, out, send, recv, local)

        @pl.when(f == 0)
        def _():
            greet(me)
            squares_ref[:] = jnp.zeros_like(squares_ref)

        @pl.when(f == 1)
        def _():
            pl.semaphore_wait(pltpu.get_barrier_semaphore(), 3)

        act_on(MLP_PLAN, f, scatters, squares_ref)

    @pl.when(f == 0)
    def _():
        db_s[:] = jnp.zeros_like(db_s)
        for p, here in enumerate(pieces):
            ready(loads(p))
            wide = mid_s[here, :].astype(F32)
            bt_s[:, here] = (wide * norm_scale(wide)).astype(BF16).T
            dyt_s[:, here] = dy_s[here, :].T

    ready(hidden_blocks(f))
    both = jnp.concatenate([wg_ref[:], wu_ref[:]], axis=1)
    for here in pieces:
        gate, up = (gu_s[lax.rem(f, 2), w, here, :] for w in range(2))
        dact = rounded(dot_t(dy_s[here, :], wd_ref[:]))
        sig = jax.nn.sigmoid(gate)
        silu = gate * sig
        act_s[here, :] = (silu * up).astype(BF16)
        dgu_s[here, bf:] = (dact * silu).astype(BF16)
        dgu_s[here, :bf] = (dact * up * (sig * (1 + gate * (1 - sig)))).astype(BF16)
    dwd_ref[:] = dot(dyt_s[:], act_s[:]).astype(BF16).T
    dgu = dot(bt_s[:], dgu_s[:])
    out_s[lax.rem(f, 2), 0] = dgu[:, :bf].astype(BF16)
    out_s[lax.rem(f, 2), 1] = dgu[:, bf:].astype(BF16)
    db_s[:] += dot_t(dgu_s[:], both)
    for c in results(f):
        c.start()

    @pl.when(f == steps - 1)
    def _():
        for p, here in enumerate(pieces):
            wide = mid_s[here, :].astype(F32)
            dy_s[here, :] = (dy_s[here, :].astype(F32) + norm_back(wide, rounded(db_s[here, :]))).astype(BF16)
            stored(p).start()
        finished(f - 1)
        finished(f)
        if cut:
            for name in "gu":
                scatters[name].last(squares_ref)
            for scatter in scatters.values():
                scatter.done()
        for p in range(len(pieces)):
            stored(p).wait()


def mlp_back(layer, dy, mid, gate, up, wg, wu, wd, dlater=None, cut=0, bt=512, bf=256):
    tokens, d = dy.shape
    ff = wg.shape[2]
    anywhere = pl.BlockSpec(memory_space=pl.ANY)
    column, row = pl.BlockSpec((None, d, bf), lambda f: (layer, 0, f)), pl.BlockSpec((None, bf, d), lambda f: (layer, f, 0))
    out = lambda *s: jax.ShapeDtypeStruct(s, BF16)
    cuts = [(d // 8, n) for n in (dlater.shape[1], cut, cut)] if cut else []
    squares = [jax.ShapeDtypeStruct(TILE, F32)] if cut else []
    dma = pltpu.SemaphoreType.DMA
    states, flipped = pltpu.VMEM((tokens, d), BF16), pltpu.VMEM((d, tokens), BF16)
    return pl.pallas_call(
        functools.partial(_mlp_back, bt=bt, cut=cut, layer=layer),
        grid=(ff // bf,),
        in_specs=[anywhere] * 4 + [column, column, row, *[anywhere for _ in squares]],
        out_specs=[anywhere, anywhere, anywhere, pl.BlockSpec((bf, d), lambda f: (f, 0)), *[anywhere for _ in cuts],
                   *[whole(*s.shape) for s in squares]],
        out_shape=[out(tokens, d), out(d, ff), out(d, ff), out(ff, d), *[out(*c) for c in cuts[1:] + cuts[:1]], *squares],
        scratch_shapes=[states, states, pltpu.VMEM((2, 2, tokens, bf), F32), flipped, flipped, pltpu.VMEM((tokens, d), F32), pltpu.VMEM((tokens, bf), BF16), pltpu.VMEM((tokens, 2 * bf), BF16),
                        pltpu.VMEM((2, 2, d, bf), BF16), dma((tokens // bt, 2)), dma((2, 2)), dma((2, 2)), *(s for c in cuts for s in scatter_scratch(*c))],
        compiler_params=params(collective_id=1, has_side_effects=True) if cut else params(),
        cost_estimate=cost(12 * tokens * d * ff, exps=tokens * ff),
        name="mlp_back",
    )(dy, mid, gate, up, wg, wu, wd, *([dlater] if cut else []))


BACK_PLAN = {
    1: [("exchange", ["g", "u", "d"])],
    2: [("first", ["g"])],
    3: [("first", ["u"])],
    4: [("first", ["d"]), ("exchange", ["o"])],
    6: [("second", ["g"]), ("first", ["o"])],
    8: [("second", ["u"])],
    9: [("second", ["d"])],
    11: [("second", ["o"])],
    12: [("last", ["g"])],
    13: [("last", ["u"])],
    15: [("last", ["d", "o"]), ("done", ["g", "u", "d", "o"])],
}


def _attention_back(*refs, bq, bk, first, since, count, layer):
    dmid_ref, o_ref, q_ref, k_ref, v_ref, lse_ref, h_ref, wo_ref, cos_ref, sin_ref, dwg_ref, dwu_ref, dwd_ref, *refs = refs
    if first:
        *known, gg_ref, gu_ref, gd_ref, go_ref, gq_ref, factor_ref = refs[: first + 6]
        dwqkv_ref, squares_ref, all_s, send_all, recv_all, *refs = refs[first + 6 :]
    else:
        wqkv_ref, dwqkv_ref, gg_ref, gu_ref, gd_ref, go_ref, squares_ref, dh_ref, *refs = refs
    k_s, v_s, late_sem, *refs = refs
    do_s, dq_s, delta_s, dwo_s, dwob_s, dwqkv_s, dqt_s, dk_s, dv_s, hide_s, *refs = refs
    me = places()
    step = pl.program_id(0)
    heads, bt = o_ref.shape[:2]
    n, middle = do_s.shape[1] // bt, do_s.shape[1] // bq
    scatters = {}
    rest = lambda ref: ref.at[:, pl.ds(since, ref.shape[1] - since)]
    for name, src, out in (("g", rest(dwg_ref), gg_ref), ("u", rest(dwu_ref), gu_ref), ("d", dwd_ref, gd_ref)):
        mine, theirs, across, from_x, from_y, send, recv, local, *refs = refs
        scatters[name] = Scatter(me, src, mine, theirs, across, from_x, from_y, out, send, recv, local)
    for name, src, out in (("o", dwob_s, go_ref), *([("qkv", dwqkv_ref, gq_ref)] if first else [])):
        theirs, across, from_x, from_y, send, recv, local, *refs = refs
        scatters[name] = Scatter(me, src, None, theirs, across, from_x, from_y, out, send, recv, local)
    others = OTHERS if first else (X, Y, CORE)

    keys = [pltpu.make_async_copy(ref.at[layer], s, late_sem.at[i]) for i, (ref, s) in enumerate(((k_ref, k_s), (v_ref, v_s)))]

    @pl.when(step == 0)
    def _():
        for c in keys:
            c.start()
        greet(me, others)
        squares_ref[:] = jnp.zeros_like(squares_ref)
        dwo_s[:] = jnp.zeros_like(dwo_s)
        dwqkv_s[:] = jnp.zeros_like(dwqkv_s)
        dk_s[:] = jnp.zeros_like(dk_s)
        dv_s[:] = jnp.zeros_like(dv_s)
        hide_s[:] = hidden(bk, bq, bq)

    @pl.when(step == 1)
    def _():
        pl.semaphore_wait(pltpu.get_barrier_semaphore(), len(others))

    act_on(BACK_PLAN, step, scatters, squares_ref)

    @pl.when(step < n)
    def _():
        rows = pl.ds(pl.multiple_of(step * bt, bt), bt)
        dmid = dmid_ref[:]
        do = dot_t(dmid, wo_ref[:]).astype(BF16)
        for i in range(heads):
            mine = do[:, i * HEAD : (i + 1) * HEAD]
            do_s[i, rows, :] = mine
            delta_s[i : i + 1, rows] = jnp.sum((mine.astype(F32) * o_ref[i].astype(F32)).T, axis=0, keepdims=True)
        dwo_s[:] += dot(side_by_side(o_ref).T, dmid)

        @pl.when(step == n - 1)
        def _():
            dwob_s[:] = dwo_s[:].astype(BF16)

    @pl.when((step >= n) & (step < n + middle))
    def _():
        iq = step - n

        @pl.when(iq == 0)
        def _():
            for c in reversed(keys):
                c.wait()

        rows = pl.ds(pl.multiple_of(iq * bq, bq), bq)
        scale = HEAD**-0.5
        e = scale * LOG2E
        dqt_s[:] = jnp.zeros_like(dqt_s)

        def block(first, count, hide=None):
            keys = pl.ds(pl.multiple_of(first, bq), count)
            qs, dos = [q_ref[i] for i in range(heads)], [do_s[i, rows, :] for i in range(heads)]
            scores = [dot_t(k_s[keys, :], x) for x in qs]
            dps = [dot_t(v_s[keys, :], x) for x in dos]
            for i in range(heads):
                s = scores[i] * e - lse_ref[i : i + 1, :] * LOG2E
                p = jnp.exp2(s if hide is None else s + hide)
                ds = (p * (dps[i] - delta_s[i : i + 1, rows])).astype(BF16)
                dv_s[keys, :] += dot(p.astype(BF16), dos[i])
                dk_s[keys, :] += dot(ds, qs[i])
                dqt_s[i] += dot(k_s[keys, :].T, ds)

        whole_blocks = lax.div(iq, 2)
        loop(whole_blocks, lambda j, _: block(j * bk, bk))
        pl.when(lax.rem(iq, 2) == 0)(lambda: block(whole_blocks * bk, bq, hide_s[bq:, :]))
        pl.when(lax.rem(iq, 2) == 1)(lambda: block(whole_blocks * bk, bk, hide_s[:]))
        for i in range(heads):
            dq_s[i, rows, :] = (dqt_s[i] * scale).T.astype(BF16)

    @pl.when(step >= n + middle)
    def _():
        rows = pl.ds(pl.multiple_of((step - n - middle) * bt, bt), bt)
        cos, sin = cos_ref[:], sin_ref[:]
        parts = []
        for t in [*(dq_s[i, rows, :] for i in range(heads)), (dk_s[rows, :] * HEAD**-0.5).astype(BF16)]:
            t = t.astype(F32)
            parts.append((t * cos - pltpu.roll(t, HALF, 1) * sin).astype(BF16))
        dz = jnp.concatenate([*parts, dv_s[rows, :].astype(BF16)], axis=1)
        wide = h_ref[:].astype(F32)
        a = (wide * norm_scale(wide)).T.astype(BF16)
        dwqkv_s[:] += dot(a, dz)
        if not first:
            da = rounded(dot_t(dz, wqkv_ref[:]))
            dh_ref[:] = (dmid_ref[:].astype(F32) + norm_back(wide, da)).astype(BF16)

        @pl.when(step == 2 * n + middle - 1)
        def _():
            dwqkv_ref[:] = dwqkv_s[:].astype(BF16)
            if first:
                scatter = scatters["qkv"]
                scatter.exchange()
                for ref in known:
                    squares_ref[:] += ref[:]
                scatter.first()
                scatter.second()
                scatter.last(squares_ref)
                factor_ref[:] = clipping(me, squares_ref, all_s, send_all, recv_all, count)
                scatter.done()


def attention_back(layer, dmid, o, q, k, v, lse, h, wo, cos, sin, dwg, dwu, dwd, wqkv=None, since=0, known=(), count=0, bq=256, bk=512,
                   bt=512):
    tokens, d = dmid.shape
    heads = o.shape[1]
    wide = d + 2 * HEAD
    n, inner = tokens // bt, tokens // bq
    one = pl.Buffered(1)
    early = lambda s: jnp.minimum(s, n - 1)
    middle = lambda s: jnp.clip(s - n, 0, inner - 1)
    late = lambda s: jnp.maximum(s - n - inner, 0)
    twice = early if wqkv is None else lambda s: jnp.where(s < n, s, late(s))
    rows = lambda w, which: pl.BlockSpec((bt, w), lambda s: (which(s), 0))
    by_head = lambda which, block: pl.BlockSpec((None, heads, block, HEAD), lambda s: (layer, 0, which(s), 0))
    all_of = lambda a: pl.BlockSpec((None, *a.shape[1:]), lambda s: (layer, 0, 0), pipeline_mode=one)
    anywhere = pl.BlockSpec(memory_space=pl.ANY)
    cuts = [(a.shape[0] // 8, a.shape[1] - first) for a, first in ((dwg, since), (dwu, since), (dwd, 0))]
    cut_o = (d // 8, d)
    out = lambda s: jax.ShapeDtypeStruct(s, BF16)
    tile, dma = jax.ShapeDtypeStruct(TILE, F32), pltpu.SemaphoreType.DMA
    blocks, block_shapes = [anywhere] * 4, [*(out(c) for c in cuts), out(cut_o)]
    if known:
        more, more_in = known, [whole(*TILE) for _ in known]
        outs, shapes = [*blocks, anywhere, whole(*TILE)], [*block_shapes, out((d // 8, wide)), tile]
        own = [pltpu.VMEM((d, wide), BF16), pltpu.VMEM(TILE, F32), pltpu.VMEM((8, *TILE), F32), dma((8,)), dma((8,))]
    else:
        more, more_in = [wqkv], [all_of(wqkv)]
        outs, shapes = [whole(d, wide), *blocks, whole(*TILE), rows(d, late)], [out((d, wide)), *block_shapes, tile, out((tokens, d))]
        own = []
    flops = 4 * tokens * d * (d + wide) + 5 * heads * tokens * tokens * HEAD
    return pl.pallas_call(
        functools.partial(_attention_back, bq=bq, bk=bk, first=len(known), since=since, count=count, layer=layer),
        grid=(2 * n + inner,),
        in_specs=[rows(d, twice), by_head(early, bt), by_head(middle, bq), anywhere, anywhere,
                  pl.BlockSpec((None, heads, bq), lambda s: (layer, 0, middle(s))), rows(d, late), all_of(wo),
                  rows(HEAD, late), rows(HEAD, late), anywhere, anywhere, anywhere, *more_in],
        out_specs=outs,
        out_shape=shapes,
        scratch_shapes=[*own, pltpu.VMEM(k.shape[1:], BF16), pltpu.VMEM(k.shape[1:], BF16), dma((2,)), pltpu.VMEM((heads, tokens, HEAD), BF16), pltpu.VMEM((heads, tokens, HEAD), BF16), pltpu.VMEM((heads, tokens), F32),
                        pltpu.VMEM((d, d), F32), pltpu.VMEM((d, d), BF16), pltpu.VMEM((d, wide), F32),
                        pltpu.VMEM((heads, HEAD, bq), F32), pltpu.VMEM((tokens, HEAD), F32), pltpu.VMEM((tokens, HEAD), F32),
                        pltpu.VMEM((bk, bq), F32), *(s for c in cuts for s in scatter_scratch(*c)),
                        *scatter_scratch(*cut_o, in_vmem=True), *(scatter_scratch(d // 8, wide, in_vmem=True) if known else [])],
        compiler_params=params(collective_id=2 + layer, has_side_effects=True),
        cost_estimate=cost(flops, exps=heads * tokens * tokens // 2),
        name="attention_back",
    )(dmid, o, q, k, v, lse, h, wo, cos, sin, dwg, dwu, dwd, *more)


def clipping(me, squares, all_s, send, recv, count):
    copies = [pltpu.make_async_remote_copy(src_ref=squares, dst_ref=all_s.at[bits], send_sem=send.at[bits], recv_sem=recv.at[bits],
                                           device_id=(0, me[bits]), device_id_type=pl.DeviceIdType.MESH) for bits in OTHERS]
    for c in copies:
        c.start()
    for c in copies:
        c.wait_recv()
    sums = [jnp.sum(squares[:]), *(jnp.sum(all_s[bits]) for bits in OTHERS)]
    while len(sums) > 1:
        sums = [a + b for a, b in zip(sums[::2], sums[1::2])]
    for c in copies:
        c.wait_send()
    return jnp.minimum(1.0, 0.5 * lax.rsqrt(jnp.full(TILE, sums[0] / count) + 1e-30))


def adamw(w, m, v, g):
    m = 0.9 * m + 0.1 * g
    v = 0.95 * v + 0.05 * g * g
    step = m * lax.rsqrt(v + 1e-8) + 0.1 * w
    return (w - 0.02 * step).astype(BF16), m, v


def solution(mesh):
    def step(x, dy, *arrays):
        weights, m, v = (arrays[i : i + 7] for i in (0, 7, 14))
        tokens, d = x.shape[1:]
        cos, sin = tables(tokens)
        *full, q, k, v_, o, lse, mid, gate, up, h1 = forward(x[0], weights, cos, sin)
        fqkv, fo, fg, fu, fd = full
        dmid, dwg, dwu, dwd = mlp_back(1, dy[0], mid, gate, up, fg, fu, fd)
        dlater, g1, u1, d1, o1, s1, dh = attention_back(1, dmid, o, q, k, v_, lse, h1, fo, cos, sin, dwg, dwu, dwd, wqkv=fqkv)
        dmid, dwg, dwu, dwd, ga, ua, qkv1, s2 = mlp_back(0, dh, mid, gate, up, fg, fu, fd, dlater, CUT)
        gb, ub, d0, o0, qkv0, factor = attention_back(0, dmid, o, q, k, v_, lse, x[0], fo, cos, sin, dwg, dwu, dwd, since=CUT, known=[s1, s2],
                                                      count=8 * sum(w.size for w in weights))
        g0, u0 = jnp.concatenate([ga, gb], axis=1), jnp.concatenate([ua, ub], axis=1)
        factor = factor[0, 0]
        split = lambda a: [a[:, :d], a[:, d : d + HEAD], a[:, d + HEAD :]]
        mine = [[*split(qkv0), o0, g0, u0, d0], [*split(qkv1), o1, g1, u1, d1]]
        gradients = [jnp.stack([one[i] for one in mine]).astype(F32) for i in range(7)]
        new = [adamw(w.astype(F32), m, v, g * factor) for w, m, v, g in zip(weights, m, v, gradients, strict=True)]
        return tuple(one[which] for which in range(3) for one in new)

    states, cut = P(("rep", "dp"), None, None), P(None, "dp", None)
    return jax.shard_map(
        step,
        mesh=mesh,
        in_specs=(states, states) + (cut,) * 21,
        out_specs=(P("rep", "dp", None),) * 21,
        check_vma=False,
    )
```

```python
import functools

import jax
import jax.numpy as jnp
import numpy as np
from jax import lax
from jax.experimental import pallas as pl
from jax.experimental.pallas import tpu as pltpu
from jax.sharding import PartitionSpec as P

NEG = -1e30
HIDDEN = 2 * NEG
LOG2E = 1.4426950408889634
VMEM = 127 * 2**19
STRIP = 512
HEAD = 128
HALF = HEAD // 2
TILE = (8, 128)
THETA = 10000
F32, BF16 = jnp.float32, jnp.bfloat16


def dot(a, b, ca=1, cb=0):
    return lax.dot_general(a, b, (((ca,), (cb,)), ((), ())), preferred_element_type=F32)


def dot_t(a, b):
    return dot(a, b, 1, 1)


def loop(stop, body, start=0):
    lax.fori_loop(start, stop, body, None)


def rounded(a):
    return a.astype(BF16).astype(F32)


def norm_scale(wide):
    return lax.rsqrt(jnp.mean(wide * wide, -1, keepdims=True) + 1e-6)


def norm_back(wide, by):
    scale = norm_scale(wide)
    return scale * (by - wide * (scale * scale * jnp.mean(by * wide, -1, keepdims=True)))


def params(**more):
    return pltpu.CompilerParams(vmem_limit_bytes=VMEM, **more)


def whole(*shape):
    return pl.BlockSpec(shape, lambda *_: (0,) * len(shape))


def cost(flops, nbytes=0, exps=0):
    return pl.CostEstimate(flops=int(flops), bytes_accessed=int(nbytes), transcendentals=int(exps))


def tables(tokens):
    angle = np.arange(tokens, dtype=np.float64)[:, None] * THETA ** (-np.arange(HALF, dtype=np.float64) / HALF)
    cos, sin = np.cos(angle), np.sin(angle)
    return jnp.asarray(np.concatenate([cos, cos], 1), F32), jnp.asarray(np.concatenate([-sin, sin], 1), F32)


def hidden(keys, queries, later=0):
    gap = lax.broadcasted_iota(jnp.int32, (keys, queries), 1) - lax.broadcasted_iota(jnp.int32, (keys, queries), 0)
    return jnp.where(gap + later >= 0, 0.0, HIDDEN)


def side_by_side(ref):
    return jnp.concatenate([ref[n] for n in range(ref.shape[0])], axis=1)


X, Y, CORE, HERE = 4, 2, 1, 0
OTHERS = range(1, 8)
NEAR = (HERE, X, Y, X + Y)


def places():
    at = [lax.axis_index("dp")]
    for bit in (CORE, Y, X):
        at += [n + bit - 2 * bit * lax.rem(lax.div(n, bit), 2) for n in at]
    return at


def greet(me, all_of=(X, Y, CORE)):
    barrier = pltpu.get_barrier_semaphore()
    for bits in all_of:
        pl.semaphore_signal(barrier, inc=1, device_id=(0, me[bits]), device_id_type=pl.DeviceIdType.MESH)
    return lambda: pl.semaphore_wait(barrier, len(all_of))


def remote(me, bit, src, dst, send, recv):
    return pltpu.make_async_remote_copy(src_ref=src, dst_ref=dst, send_sem=send, recv_sem=recv, device_id=(0, me[bit]),
                                        device_id_type=pl.DeviceIdType.MESH)


def halves(r):
    a = (r // 2 + 15) // 16 * 16
    return (0, a), (a, r - a)


def upper(r):
    return halves(r)[0]


def lower(r):
    return halves(r)[1]


ALL = None
ROUTES = {"x": (X, HERE, ALL), "y": (Y, HERE, ALL), "core": (CORE, HERE, ALL), "xy": (Y, X, upper), "x core": (CORE, X, ALL),
          "yx": (X, Y, lower), "y core": (CORE, Y, ALL), "xy core": (CORE, X + Y, upper), "yx core": (CORE, X + Y, lower)}


class Gather:
    def __init__(self, me, block, full, send, recv, cols, at):
        first, count = cols
        self.me, self.r = me, block.shape[0]
        self.full, self.send, self.recv = full, send, recv
        self.own, self.cols = block.at[:, pl.ds(first, count)], pl.ds(at + first, count)

    def rows(self, bits, part=None):
        first, count = part or (0, self.r)
        at = pl.multiple_of(self.me[bits] * self.r + first, 16)
        return self.full.at[pl.ds(at, count), self.cols]

    def copy(self, which, got=False):
        bit, bits, part = ROUTES[which]
        there = self.rows(bits + bit if got else bits, part and part(self.r))
        n = tuple(ROUTES).index(which)
        return remote(self.me, bit, self.own if bits == HERE and not got else there, there, self.send.at[n], self.recv.at[n])

    def got(self, which):
        self.copy(which, got=True).wait_recv()

    def begin(self):
        for n in ("x", "y", "core"):
            self.copy(n).start()

    def hand_on(self):
        self.got("x")
        self.copy("xy").start()
        self.copy("x core").start()
        self.got("y")
        self.copy("yx").start()
        self.copy("y core").start()

    def finish(self):
        self.got("xy")
        self.copy("xy core").start()
        self.got("yx")
        self.copy("yx core").start()

    def arrived(self):
        for n in ("core", "x core", "y core", "xy core", "yx core"):
            self.got(n)

    def sent(self):
        for n in ROUTES:
            self.copy(n).wait_send()


class Scatter:
    def __init__(self, me, src, mine, theirs, across, from_x, from_y, out, send, recv, local):
        self.me, self.src, self.out = me, src, out
        self.r, self.n = theirs.shape[1:]
        self.own, self.theirs, self.across, self.from_x, self.from_y = mine, theirs, across, from_x, from_y
        self.send, self.recv, self.local = send, recv, local
        self.a, self.b = halves(self.r)
        self.all = (0, self.r)

    def block(self, bits, part=None):
        first, count = part or self.all
        return self.src.at[pl.ds(pl.multiple_of(self.me[bits] * self.r + first, 16), count)]

    def mine(self, j, part):
        return self.block(NEAR[j], part) if self.own is None else self.own.at[j, pl.ds(*part)]

    def load(self, j):
        return pltpu.make_async_copy(self.block(NEAR[j]), self.own.at[j], self.local.at[j])

    def copy(self, n):
        if n < 4:
            bit, src, dst = CORE, self.block(CORE + NEAR[n]), self.theirs.at[n]
        else:
            bit, j, part, to = ((X, 3, self.a, self.across), (Y, 3, self.b, self.across), (X, 1, self.a, self.from_x),
                                (Y, 2, self.b, self.from_y), (Y, 2, self.a, self.from_y), (X, 1, self.b, self.from_x))[n - 4]
            src, dst = self.mine(j, part), to.at[pl.ds(*part)]
        return remote(self.me, bit, src, dst, self.send.at[n], self.recv.at[n])

    def add(self, j, part, *more):
        step = 16
        ref = self.mine(j, part)

        def one(i, _):
            rows = pl.ds(pl.multiple_of(i * step, step), step)
            full = pl.ds(pl.multiple_of(part[0] + i * step, step), step)
            total = ref[rows, :].astype(F32) + self.theirs[j, full, :].astype(F32)
            for other in more:
                total += other[full, :].astype(F32)
            ref[rows, :] = total.astype(BF16)

        loop(part[1] // step, one)

    def exchange(self):
        for j in range(4):
            self.copy(j).start()
            if self.own is not None:
                self.load(j).start()

    def first(self):
        for j in range(4):
            if self.own is not None:
                self.load(j).wait()
            self.copy(j).wait_recv()
        self.add(3, self.all)
        self.copy(4).start()
        self.copy(5).start()
        self.add(1, self.a)
        self.add(2, self.b)

    def second(self):
        self.copy(6).start()
        self.copy(7).start()
        self.copy(4).wait_recv()
        self.add(2, self.a, self.across)
        self.copy(8).start()
        self.copy(5).wait_recv()
        self.add(1, self.b, self.across)
        self.copy(9).start()

    def results(self):
        at, copies = 0, []
        for i, out in enumerate(self.out if isinstance(self.out, list) else [self.out]):
            block = self.mine(0, self.all).at[:, pl.ds(at, out.shape[1])]
            copies.append(pltpu.make_async_copy(block, out, self.local.at[4 + i]))
            at += out.shape[1]
        return copies

    def last(self, squares):
        for n in range(6, 10):
            self.copy(n).wait_recv()
        self.add(0, self.all, self.from_x, self.from_y)
        ref = self.mine(0, self.all)
        for c in self.results():
            c.start()
        squares[:] += sum_of_squares(ref)

    def done(self):
        for n in range(10):
            self.copy(n).wait_send()
        for c in self.results():
            c.wait()


def sum_of_squares(ref):
    rows, cols = ref.shape

    def one(i, total):
        g = ref[pl.ds(pl.multiple_of(i * 16, 16), 16), :].astype(F32)
        g = g * g
        for c in range(0, cols, 128):
            total += g[:8, c : c + 128] + g[8:, c : c + 128]
        return total

    return lax.fori_loop(0, rows // 16, one, jnp.zeros(TILE, F32))


def scatter_scratch(r, n, in_vmem=False):
    dma = pltpu.SemaphoreType.DMA
    block = pltpu.VMEM((r, n), BF16)
    return [*([] if in_vmem else [pltpu.VMEM((4, r, n), BF16)]), pltpu.VMEM((4, r, n), BF16), block, block, block,
            dma((10,)), dma((10,)), dma((7,))]


BQ = BK = BT = BF = 512
CUT, CUT_Q = 2 * BF, 4 * HEAD
TENSORS = ("qa", "qb", "k", "v", "o", "ga", "ua", "gb", "ub", "d")
QKV, GU_A, GU_B = ["qa", "k", "v", "qb"], ["ga", "ua"], ["gb", "ub"]


def _forward(x_ref, sq, sk, sv, so, sg, su, sd, cos_ref, sin_ref, fqkv, fo, fg, fu, fd, q_o, k_o, v_o, o_o, lse_o, mid_o, gate_o, up_o, h_o,
             h_s, b_s, q_s, k_s, v_s, o_s, lse_s, act_s, wqkv_s, wo_s, wg_s, wu_s, wd_s, stage_s, top_s, mix_s, hide_s,
             send, recv, load, keep, out, wsem):
    layer, layers = pl.program_id(0), pl.num_programs(0)
    me = places()
    tokens, d = h_s.shape
    heads = q_s.shape[0]
    ff = act_s.shape[1]
    blocks = tokens // BT

    def gather(n, name):
        i = TENSORS.index(name)
        shard, full, cols, at = {
            "qa": (sq, fqkv, (0, CUT_Q), 0), "qb": (sq, fqkv, (CUT_Q, d - CUT_Q), 0), "k": (sk, fqkv, (0, HEAD), d),
            "v": (sv, fqkv, (0, HEAD), d + HEAD), "o": (so, fo, (0, d), 0), "d": (sd, fd, (0, d), 0),
            "ga": (sg, fg, (0, CUT), 0), "gb": (sg, fg, (CUT, ff - CUT), 0),
            "ua": (su, fu, (0, CUT), 0), "ub": (su, fu, (CUT, ff - CUT), 0)}[name]
        full = wqkv_s if name in QKV and n == 0 else full.at[n]
        return Gather(me, shard.at[n], full, send.at[n, i], recv.at[n, i], cols, at)

    def own_blocks():
        at = 0
        for s, f, column in ((sq, fqkv, 0), (sk, fqkv, d), (sv, fqkv, d + HEAD), (so, fo, 0), (sg, fg, 0), (su, fu, 0), (sd, fd, 0)):
            r, n = s.shape[1:]
            for i in range(s.shape[0]):
                where = pl.ds(pl.multiple_of(me[HERE] * r, 16), r), pl.ds(column, n)
                if f is fqkv and i == 0:
                    yield s.at[i], wqkv_s.at[where], None
                else:
                    yield s.at[i], act_s.at[pl.ds(at, r), pl.ds(0, n)], f.at[i, *where]
                    at += r

    copies_in = lambda: [pltpu.make_async_copy(a, b, load.at[i]) for i, (a, b, _) in enumerate(own_blocks())]
    copies_out = lambda: [pltpu.make_async_copy(b, c, load.at[i]) for i, (_, b, c) in enumerate(own_blocks()) if c is not None]
    here = lambda i, n: pl.ds(pl.multiple_of(i * n, n), n)

    def kept(*names):
        pairs = {"x": (x_ref, h_s), "q": (q_s, q_o.at[layer]), "k": (k_s, k_o.at[layer]), "v": (v_s, v_o.at[layer]), "o": (o_s, o_o.at[layer]),
                 "lse": (lse_s, lse_o.at[layer]), "mid": (h_s, mid_o.at[layer]), "h": (h_s, h_o), "qkv": (wqkv_s, fqkv.at[layer])}
        return [pltpu.make_async_copy(*pairs[n], keep.at[list(pairs).index(n)]) for n in names]

    def start(*copies):
        for c in copies:
            c.start()

    def wait(*copies):
        for c in copies:
            c.wait()

    def weight(n, name):
        return pltpu.make_async_copy(*{"qb": (fqkv.at[n], wqkv_s, wsem.at[0]), "o": (fo.at[n], wo_s, wsem.at[1]),
                                       "d": (fd.at[n], wd_s, wsem.at[2])}[name])

    def column(c, n=layer):
        cols, slot = here(c, BF), lax.rem(c, 2)
        return (pltpu.make_async_copy(fg.at[n, :, cols], wg_s.at[slot], wsem.at[3 + slot]),
                pltpu.make_async_copy(fu.at[n, :, cols], wu_s.at[slot], wsem.at[5 + slot]))

    def fetch(n, name):
        gather(n, name).arrived()
        if name in QKV:
            gather(0, name).sent()
        if name == "ua":
            start(*column(0, n))
        elif name in ("qb", "o", "d"):
            start(weight(n, name))

    def tick(phase, i):
        for n, plan in enumerate(PLAN):
            for p, k, *actions in plan:
                if p == phase:
                    @pl.when((layer == n) & (i == k))
                    def _():
                        for do, later, names in actions:
                            for name in names:
                                if do == "fetch":
                                    fetch(n + later, name)
                                else:
                                    getattr(gather(n + later, name), do)()

    @pl.when(layer == 0)
    def _():
        greeted = greet(me)
        start(*kept("x"), *copies_in())
        hide_s[:] = hidden(BK, BQ)
        greeted()
        for name in QKV:
            gather(0, name).begin()
        wait(*copies_in())
        start(*copies_out())
        wait(*kept("x"))
        for name in QKV:
            gather(0, name).hand_on()
        for name in ("o", *GU_A):
            gather(0, name).begin()
        wait(*copies_out())
        for do in (Gather.finish, Gather.arrived):
            for name in QKV:
                do(gather(0, name))

    @pl.when(layer > 0)
    def _():
        start(*kept("h"))
        wait(weight(1, "qb"))

    def qkv_step(i):
        rows = here(i, BT)
        wide = h_s[rows, :].astype(F32)
        a = (wide * norm_scale(wide)).astype(BF16)
        z = dot(a, wqkv_s[:])
        cos, sin = cos_ref[rows, :], sin_ref[rows, :]
        for n in range(heads + 1):
            t = rounded(z[:, n * HEAD : (n + 1) * HEAD])
            t = (t * cos + pltpu.roll(t, HALF, 1) * sin).astype(BF16)
            if n < heads:
                q_s[n, rows, :] = t
            else:
                k_s[rows, :] = t
        v_s[rows, :] = z[:, (heads + 1) * HEAD :].astype(BF16)

    pairwise(blocks, qkv_step, lambda i: tick("qkv", i))
    start(*kept("q", "k", "v"))

    @pl.when(layer == 0)
    def _():
        start(*kept("qkv"))

    scale = HEAD**-0.5
    e = scale * LOG2E

    def attend_step(i, _):
        top_s[:] = jnp.full(top_s.shape, NEG, F32)
        mix_s[:] = jnp.zeros(mix_s.shape, F32)

        def block(first, count, at=0, hidden=None):
            keys, cols = pl.ds(pl.multiple_of(first, BK // 2), count), pl.ds(at, BQ - at)
            rows = pl.ds(pl.multiple_of(i * BQ + at, BQ // 2), BQ - at)
            values = jnp.concatenate([v_s[keys, :].T, jnp.ones((8, count), BF16)], axis=0)
            scores = [dot_t(k_s[keys, :], q_s[n, rows, :]) for n in range(heads)]
            weights = []
            for n, s in enumerate(scores):
                s = s if hidden is None else s + hidden
                old = top_s[n : n + 1, cols]
                top = jnp.maximum(old, s.max(axis=0, keepdims=True))
                top_s[n : n + 1, cols] = top
                weights.append((jnp.exp2((s - top) * e).astype(BF16), jnp.exp2((old - top) * e)))
            for n, (p, rest) in enumerate(weights):
                mix_s[n, :, cols] = mix_s[n, :, cols] * rest + dot(values, p)

        def before(j, _):
            tick("attend", lax.div(i * (i + 1), 2) + j)
            block(j * BK, BK)

        loop(i, before)
        tick("attend", lax.div(i * (i + 3), 2))
        half = BK // 2
        block(i * BK, half, hidden=hide_s[:half, :])
        block(i * BK + half, half, half, hide_s[half:, half:])
        rows = here(i, BQ)
        for n in range(heads):
            total = mix_s[n, HEAD : HEAD + 1, :]
            o_s[n, rows, :] = (mix_s[n, :HEAD, :] * (1 / total)).T.astype(BF16)
            lse_s[n : n + 1, rows] = top_s[n : n + 1, :] * scale + jnp.log(total)

    loop(tokens // BQ, attend_step)
    start(*kept("o", "lse"))

    @pl.when(layer == 0)
    def _():
        wait(*kept("qkv"))

    @pl.when(layer > 0)
    def _():
        wait(*kept("h"))

    wait(weight(layer, "o"))

    def out_step(i):
        rows = here(i, BT)
        o = jnp.concatenate([o_s[n, rows, :] for n in range(heads)], axis=1)
        mid = (h_s[rows, :].astype(F32) + rounded(dot(o, wo_s[:]))).astype(BF16)
        h_s[rows, :] = mid
        wide = mid.astype(F32)
        b_s[rows, :] = (wide * norm_scale(wide)).astype(BF16)

    pairwise(blocks, out_step, lambda i: tick("out", i))
    start(*kept("mid"))

    def staged(i, c):
        rows, cols = here(i, BT), here(c, BF)
        return [pltpu.make_async_copy(stage_s.at[i, w], ref.at[layer, rows, cols], out.at[i, w]) for w, ref in enumerate((gate_o, up_o))]

    def gate_column(c, _):
        wait(*column(c))

        def gate_step(i):
            rows = here(i, BT)
            b = b_s[rows, :]
            gate, up = dot(b, wg_s[lax.rem(c, 2)]), dot(b, wu_s[lax.rem(c, 2)])
            stage_s[i, 0] = gate
            stage_s[i, 1] = up
            act_s[rows, here(c, BF)] = (gate * jax.nn.sigmoid(gate) * up).astype(BF16)
            start(*staged(i, c))

        for i in range(0, blocks, 2):
            tick("gate", 2 * c + i // 2)
            if i > 0:
                pl.when(c + 1 < ff // BF)(lambda: start(*column(c + 1)))

            @pl.when((layer > 0) | (c > 0))
            def _():
                wait(*staged(i, c), *staged(i + 1, c))

            gate_step(i)
            gate_step(i + 1)

    loop(ff // BF, gate_column)
    wait(*kept("q", "k", "v", "o", "lse", "mid"))

    @pl.when(layer < layers - 1)
    def _():
        wait(weight(0, "d"))

        def down_step(i):
            rows = here(i, BT)
            h_s[rows, :] = (h_s[rows, :].astype(F32) + rounded(dot(act_s[rows, :], wd_s[:]))).astype(BF16)

        pairwise(blocks, down_step, lambda i: tick("down", i))
        tick("end", 0)

    @pl.when(layer == layers - 1)
    def _():
        gather(1, "d").arrived()
        for i in range(blocks):
            wait(*staged(i, 0))
        for n in range(2):
            for name in TENSORS:
                if name not in QKV or n > 0:
                    gather(n, name).sent()


def pairwise(count, body, first):
    def two(i, _):
        first(i)
        body(2 * i)
        body(2 * i + 1)

    loop(count // 2, two)


THIS, NEXT = range(2)
PLAN = ([
    ("qkv", 1, ("hand_on", THIS, ["o"]), ("begin", THIS, GU_B)),
    ("attend", 3, ("hand_on", THIS, GU_A), ("finish", THIS, ["o"])),
    ("attend", 8, ("fetch", THIS, ["o"])),
    ("attend", 9, ("hand_on", THIS, GU_B), ("begin", THIS, ["d"])),
    ("out", 1, ("finish", THIS, GU_A), ("fetch", THIS, GU_A)),
    ("gate", 2, ("finish", THIS, GU_B)),
    ("gate", 3, ("fetch", THIS, GU_B)),
    ("gate", 4, ("begin", NEXT, QKV)),
    ("gate", 6, ("hand_on", THIS, ["d"])),
    ("gate", 8, ("hand_on", NEXT, QKV), ("begin", NEXT, ["o"])),
    ("gate", 9, ("finish", THIS, ["d"]), ("fetch", THIS, ["d"])),
    ("down", 0, ("finish", NEXT, QKV), ("begin", NEXT, GU_A)),
    ("down", 1, ("fetch", NEXT, QKV)),
], [
    ("qkv", 0, ("hand_on", THIS, ["o"])),
    ("qkv", 1, ("begin", THIS, ["gb"])),
    ("attend", 1, ("hand_on", THIS, GU_A), ("begin", THIS, ["ub"])),
    ("attend", 4, ("finish", THIS, ["o"])),
    ("attend", 7, ("fetch", THIS, ["o"])),
    ("attend", 8, ("finish", THIS, GU_A)),
    ("attend", 9, ("hand_on", THIS, GU_B), ("begin", THIS, ["d"])),
    ("out", 1, ("fetch", THIS, GU_A)),
    ("gate", 2, ("finish", THIS, GU_B)),
    ("gate", 3, ("fetch", THIS, GU_B)),
    ("gate", 6, ("hand_on", THIS, ["d"])),
    ("gate", 9, ("finish", THIS, ["d"])),
])


def forward(x, shards, cos, sin):
    tokens, d = x.shape
    layers = shards[0].shape[0]
    heads, ff = d // HEAD, shards[4].shape[2]
    full = [jax.ShapeDtypeStruct((layers, *s), BF16) for s in ((d, d + 2 * HEAD), (d, d), (d, ff), (d, ff), (ff, d))]
    shape = lambda *s: jax.ShapeDtypeStruct((layers, *s), BF16)
    wide = jax.ShapeDtypeStruct((layers, tokens, ff), F32)
    once = lambda a: pl.BlockSpec(a.shape, lambda i: (0,) * len(a.shape), pipeline_mode=pl.Buffered(1))
    anywhere = pl.BlockSpec(memory_space=pl.ANY)
    dma = pltpu.SemaphoreType.DMA
    outs = [*full, shape(heads, tokens, HEAD), shape(tokens, HEAD), shape(tokens, HEAD), shape(heads, tokens, HEAD),
            jax.ShapeDtypeStruct((layers, heads, tokens), F32), shape(tokens, d), wide, wide, jax.ShapeDtypeStruct((tokens, d), BF16)]
    states, by_head, one_head = pltpu.VMEM((tokens, d), BF16), pltpu.VMEM((heads, tokens, HEAD), BF16), pltpu.VMEM((tokens, HEAD), BF16)
    matrix, columns = lambda i: pltpu.VMEM(full[i].shape[1:], BF16), pltpu.VMEM((2, d, BF), BF16)
    routes = dma((layers, len(TENSORS), len(ROUTES)))
    return pl.pallas_call(
        _forward,
        grid=(layers,),
        in_specs=[anywhere] * 8 + [once(cos), once(sin)],
        out_specs=[anywhere] * len(outs),
        out_shape=outs,
        scratch_shapes=[states, states, by_head, one_head, one_head, by_head, pltpu.VMEM((heads, tokens), F32), pltpu.VMEM((tokens, ff), BF16),
                        matrix(0), matrix(1), columns, columns, matrix(4), pltpu.VMEM((tokens // BT, 2, BT, BF), F32),
                        pltpu.VMEM((heads, BQ), F32), pltpu.VMEM((heads, HEAD + 8, BQ), F32), pltpu.VMEM((BK, BQ), F32),
                        routes, routes, dma((7 * layers,)), dma((9,)), dma((tokens // BT, 2)), dma((7,))],
        compiler_params=params(collective_id=0, has_side_effects=True),
        cost_estimate=cost(4 * tokens * (7 * HEAD * 1200 + 3 * d * ff)),
        name="forward",
    )(x, *shards, cos, sin)


def act_on(plan, step, scatters, squares):
    for at, actions in plan.items():
        @pl.when(step == at)
        def _():
            for what, names in actions:
                for name in names:
                    getattr(scatters[name], what)(*([squares] if what == "last" else []))


MLP_PLAN = {
    1: [("exchange", ["qkv"])],
    2: [("first", ["qkv"])],
    3: [("second", ["qkv"])],
    5: [("exchange", ["g", "u"])],
    6: [("first", ["g", "u"]), ("last", ["qkv"])],
    7: [("second", ["g", "u"])],
}


def _mlp_back(*refs, bt, cut, layer):
    dy_ref, mid_ref, gate_ref, up_ref, wg_ref, wu_ref, wd_ref, *refs = refs
    ready = lambda copies: [c.wait() for c in copies]
    if cut:
        dlater_ref, dmid_ref, dwg_ref, dwu_ref, dwd_ref, gg_ref, gu_ref, gq_ref, gk_ref, gv_ref, squares_ref, *refs = refs
    else:
        dmid_ref, dwg_ref, dwu_ref, dwd_ref, *refs = refs
    dy_s, mid_s, gu_s, bt_s, dyt_s, db_s, act_s, dgu_s, out_s, in_sem, gu_sem, out_sem, *refs = refs
    f, steps = pl.program_id(0), pl.num_programs(0)
    tokens = dy_s.shape[0]
    bf = act_s.shape[1]
    pieces = [pl.ds(at, bt) for at in range(0, tokens, bt)]

    def loads(p):
        return [pltpu.make_async_copy(ref.at[pieces[p]], s.at[pieces[p]], in_sem.at[p, w])
                for w, (ref, s) in enumerate(((dy_ref, dy_s), (mid_ref.at[layer], mid_s)))]

    def hidden_blocks(f):
        cols, slot = pl.ds(pl.multiple_of(f * bf, bf), bf), lax.rem(f, 2)
        return [pltpu.make_async_copy(ref.at[layer, :, cols], gu_s.at[slot, w], gu_sem.at[slot, w]) for w, ref in enumerate((gate_ref, up_ref))]

    def stored(p):
        return pltpu.make_async_copy(dy_s.at[pieces[p]], dmid_ref.at[pieces[p]], in_sem.at[p, 0])

    def results(f):
        cols, slot = pl.ds(pl.multiple_of(f * bf, bf), bf), lax.rem(f, 2)
        return [pltpu.make_async_copy(out_s.at[slot, w], ref.at[:, cols], out_sem.at[slot, w]) for w, ref in enumerate((dwg_ref, dwu_ref))]

    finished = lambda f: ready(results(f))

    @pl.when(f == 0)
    def _():
        for copies in (*map(loads, range(len(pieces))), hidden_blocks(f)):
            for c in copies:
                c.start()

    @pl.when(f + 1 < steps)
    def _():
        for c in hidden_blocks(f + 1):
            c.start()

    @pl.when(f >= 2)
    def _():
        finished(f - 2)

    if cut:
        me = places()
        scatters = {}
        firsts = lambda ref: ref.at[:, pl.ds(0, cut)]
        for name, src, out in (("qkv", dlater_ref, [gq_ref, gk_ref, gv_ref]), ("g", firsts(dwg_ref), gg_ref), ("u", firsts(dwu_ref), gu_ref)):
            mine, theirs, across, from_x, from_y, send, recv, local, *refs = refs
            scatters[name] = Scatter(me, src, mine, theirs, across, from_x, from_y, out, send, recv, local)

        @pl.when(f == 0)
        def _():
            greet(me)
            squares_ref[:] = jnp.zeros_like(squares_ref)

        @pl.when(f == 1)
        def _():
            pl.semaphore_wait(pltpu.get_barrier_semaphore(), 3)

        act_on(MLP_PLAN, f, scatters, squares_ref)

    @pl.when(f == 0)
    def _():
        db_s[:] = jnp.zeros_like(db_s)
        for p, here in enumerate(pieces):
            ready(loads(p))
            wide = mid_s[here, :].astype(F32)
            bt_s[:, here] = (wide * norm_scale(wide)).astype(BF16).T
            dyt_s[:, here] = dy_s[here, :].T

    ready(hidden_blocks(f))
    both = jnp.concatenate([wg_ref[:], wu_ref[:]], axis=1)
    for here in pieces:
        gate, up = (gu_s[lax.rem(f, 2), w, here, :] for w in range(2))
        dact = rounded(dot_t(dy_s[here, :], wd_ref[:]))
        sig = jax.nn.sigmoid(gate)
        silu = gate * sig
        act_s[here, :] = (silu * up).astype(BF16)
        dgu_s[here, bf:] = (dact * silu).astype(BF16)
        dgu_s[here, :bf] = (dact * up * (sig * (1 + gate * (1 - sig)))).astype(BF16)
    dwd_ref[:] = dot(dyt_s[:], act_s[:]).astype(BF16).T
    dgu = dot(bt_s[:], dgu_s[:])
    out_s[lax.rem(f, 2), 0] = dgu[:, :bf].astype(BF16)
    out_s[lax.rem(f, 2), 1] = dgu[:, bf:].astype(BF16)
    db_s[:] += dot_t(dgu_s[:], both)
    for c in results(f):
        c.start()

    @pl.when(f == steps - 1)
    def _():
        for p, here in enumerate(pieces):
            wide = mid_s[here, :].astype(F32)
            dy_s[here, :] = (dy_s[here, :].astype(F32) + norm_back(wide, rounded(db_s[here, :]))).astype(BF16)
            stored(p).start()
        finished(f - 1)
        finished(f)
        if cut:
            for name in "gu":
                scatters[name].last(squares_ref)
            for scatter in scatters.values():
                scatter.done()
        for p in range(len(pieces)):
            stored(p).wait()


def mlp_back(layer, dy, mid, gate, up, wg, wu, wd, dlater=None, cut=0, bt=512, bf=256):
    tokens, d = dy.shape
    ff = wg.shape[2]
    anywhere = pl.BlockSpec(memory_space=pl.ANY)
    column, row = pl.BlockSpec((None, d, bf), lambda f: (layer, 0, f)), pl.BlockSpec((None, bf, d), lambda f: (layer, f, 0))
    out = lambda *s: jax.ShapeDtypeStruct(s, BF16)
    cuts = [(d // 8, n) for n in (dlater.shape[1], cut, cut)] if cut else []
    squares = [jax.ShapeDtypeStruct(TILE, F32)] if cut else []
    blocks = [*cuts[1:], *((d // 8, n) for n in (d, HEAD, HEAD))] if cut else []
    dma = pltpu.SemaphoreType.DMA
    states, flipped = pltpu.VMEM((tokens, d), BF16), pltpu.VMEM((d, tokens), BF16)
    return pl.pallas_call(
        functools.partial(_mlp_back, bt=bt, cut=cut, layer=layer),
        grid=(ff // bf,),
        in_specs=[anywhere] * 4 + [column, column, row, *[anywhere for _ in squares]],
        out_specs=[anywhere, anywhere, anywhere, pl.BlockSpec((bf, d), lambda f: (f, 0)), *[anywhere for _ in blocks],
                   *[whole(*s.shape) for s in squares]],
        out_shape=[out(tokens, d), out(d, ff), out(d, ff), out(ff, d), *[out(*c) for c in blocks], *squares],
        scratch_shapes=[states, states, pltpu.VMEM((2, 2, tokens, bf), F32), flipped, flipped, pltpu.VMEM((tokens, d), F32), pltpu.VMEM((tokens, bf), BF16), pltpu.VMEM((tokens, 2 * bf), BF16),
                        pltpu.VMEM((2, 2, d, bf), BF16), dma((tokens // bt, 2)), dma((2, 2)), dma((2, 2)), *(s for c in cuts for s in scatter_scratch(*c))],
        compiler_params=params(collective_id=1, has_side_effects=True) if cut else params(),
        cost_estimate=cost(12 * tokens * d * ff, exps=tokens * ff),
        name="mlp_back",
    )(dy, mid, gate, up, wg, wu, wd, *([dlater] if cut else []))


BACK_PLAN = {
    1: [("exchange", ["g", "u", "d"])],
    2: [("first", ["g"])],
    3: [("first", ["u"])],
    4: [("first", ["d"]), ("exchange", ["o"])],
    6: [("second", ["g"]), ("first", ["o"])],
    8: [("second", ["u"])],
    9: [("second", ["d"])],
    11: [("second", ["o"])],
    12: [("last", ["g"])],
    13: [("last", ["u"])],
    15: [("last", ["d", "o"]), ("done", ["g", "u", "d", "o"])],
}


def _attention_back(*refs, bq, bk, first, since, count, layer):
    dmid_ref, o_ref, q_ref, k_ref, v_ref, lse_ref, h_ref, wo_ref, cos_ref, sin_ref, dwg_ref, dwu_ref, dwd_ref, *refs = refs
    if first:
        *known, gg_ref, gu_ref, gd_ref, go_ref, gq_ref, gk_ref, gv_ref, factor_ref = refs[: first + 8]
        dwqkv_ref, squares_ref, all_s, send_all, recv_all, *refs = refs[first + 8 :]
    else:
        wqkv_ref, dwqkv_ref, gg_ref, gu_ref, gd_ref, go_ref, squares_ref, dh_ref, *refs = refs
    k_s, v_s, late_sem, *refs = refs
    do_s, dq_s, delta_s, dwo_s, dwob_s, dwqkv_s, dqt_s, dk_s, dv_s, hide_s, *refs = refs
    me = places()
    step = pl.program_id(0)
    heads, bt = o_ref.shape[:2]
    n, middle = do_s.shape[1] // bt, do_s.shape[1] // bq
    scatters = {}
    rest = lambda ref: ref.at[:, pl.ds(since, ref.shape[1] - since)]
    for name, src, out in (("g", rest(dwg_ref), gg_ref), ("u", rest(dwu_ref), gu_ref), ("d", dwd_ref, gd_ref)):
        mine, theirs, across, from_x, from_y, send, recv, local, *refs = refs
        scatters[name] = Scatter(me, src, mine, theirs, across, from_x, from_y, out, send, recv, local)
    for name, src, out in (("o", dwob_s, go_ref), *([("qkv", dwqkv_ref, [gq_ref, gk_ref, gv_ref])] if first else [])):
        theirs, across, from_x, from_y, send, recv, local, *refs = refs
        scatters[name] = Scatter(me, src, None, theirs, across, from_x, from_y, out, send, recv, local)
    others = OTHERS if first else (X, Y, CORE)

    keys = [pltpu.make_async_copy(ref.at[layer], s, late_sem.at[i]) for i, (ref, s) in enumerate(((k_ref, k_s), (v_ref, v_s)))]

    @pl.when(step == 0)
    def _():
        for c in keys:
            c.start()
        greet(me, others)
        squares_ref[:] = jnp.zeros_like(squares_ref)
        dwo_s[:] = jnp.zeros_like(dwo_s)
        dwqkv_s[:] = jnp.zeros_like(dwqkv_s)
        dk_s[:] = jnp.zeros_like(dk_s)
        dv_s[:] = jnp.zeros_like(dv_s)
        hide_s[:] = hidden(bk, bq, bq)

    @pl.when(step == 1)
    def _():
        pl.semaphore_wait(pltpu.get_barrier_semaphore(), len(others))

    act_on(BACK_PLAN, step, scatters, squares_ref)

    @pl.when(step < n)
    def _():
        rows = pl.ds(pl.multiple_of(step * bt, bt), bt)
        dmid = dmid_ref[:]
        do = dot_t(dmid, wo_ref[:]).astype(BF16)
        for i in range(heads):
            mine = do[:, i * HEAD : (i + 1) * HEAD]
            do_s[i, rows, :] = mine
            delta_s[i : i + 1, rows] = jnp.sum((mine.astype(F32) * o_ref[i].astype(F32)).T, axis=0, keepdims=True)
        dwo_s[:] += dot(side_by_side(o_ref).T, dmid)

        @pl.when(step == n - 1)
        def _():
            dwob_s[:] = dwo_s[:].astype(BF16)

    @pl.when((step >= n) & (step < n + middle))
    def _():
        iq = step - n

        @pl.when(iq == 0)
        def _():
            for c in reversed(keys):
                c.wait()

        rows = pl.ds(pl.multiple_of(iq * bq, bq), bq)
        scale = HEAD**-0.5
        e = scale * LOG2E
        dqt_s[:] = jnp.zeros_like(dqt_s)

        def block(first, count, hide=None):
            keys = pl.ds(pl.multiple_of(first, bq), count)
            qs, dos = [q_ref[i] for i in range(heads)], [do_s[i, rows, :] for i in range(heads)]
            scores = [dot_t(k_s[keys, :], x) for x in qs]
            dps = [dot_t(v_s[keys, :], x) for x in dos]
            for i in range(heads):
                s = scores[i] * e - lse_ref[i : i + 1, :] * LOG2E
                p = jnp.exp2(s if hide is None else s + hide)
                ds = (p * (dps[i] - delta_s[i : i + 1, rows])).astype(BF16)
                dv_s[keys, :] += dot(p.astype(BF16), dos[i])
                dk_s[keys, :] += dot(ds, qs[i])
                dqt_s[i] += dot(k_s[keys, :].T, ds)

        whole_blocks = lax.div(iq, 2)
        loop(whole_blocks, lambda j, _: block(j * bk, bk))
        pl.when(lax.rem(iq, 2) == 0)(lambda: block(whole_blocks * bk, bq, hide_s[bq:, :]))
        pl.when(lax.rem(iq, 2) == 1)(lambda: block(whole_blocks * bk, bk, hide_s[:]))
        for i in range(heads):
            dq_s[i, rows, :] = (dqt_s[i] * scale).T.astype(BF16)

    @pl.when(step >= n + middle)
    def _():
        rows = pl.ds(pl.multiple_of((step - n - middle) * bt, bt), bt)
        cos, sin = cos_ref[:], sin_ref[:]
        parts = []
        for t in [*(dq_s[i, rows, :] for i in range(heads)), (dk_s[rows, :] * HEAD**-0.5).astype(BF16)]:
            t = t.astype(F32)
            parts.append((t * cos - pltpu.roll(t, HALF, 1) * sin).astype(BF16))
        dz = jnp.concatenate([*parts, dv_s[rows, :].astype(BF16)], axis=1)
        wide = h_ref[:].astype(F32)
        a = (wide * norm_scale(wide)).T.astype(BF16)
        if not first:
            da = rounded(dot_t(dz, wqkv_ref[:]))
        dwqkv_s[:] += dot(a, dz)
        if not first:
            dh_ref[:] = (dmid_ref[:].astype(F32) + norm_back(wide, da)).astype(BF16)

        @pl.when(step == 2 * n + middle - 1)
        def _():
            dwqkv_ref[:] = dwqkv_s[:].astype(BF16)
            if first:
                scatter = scatters["qkv"]
                scatter.exchange()
                for ref in known:
                    squares_ref[:] += ref[:]
                scatter.first()
                scatter.second()
                scatter.last(squares_ref)
                factor_ref[0, 0] = clipping(me, squares_ref, all_s, send_all, recv_all, count)
                scatter.done()


def attention_back(layer, dmid, o, q, k, v, lse, h, wo, cos, sin, dwg, dwu, dwd, wqkv=None, since=0, known=(), count=0, bq=256, bk=512,
                   bt=512):
    tokens, d = dmid.shape
    heads = o.shape[1]
    wide = d + 2 * HEAD
    n, inner = tokens // bt, tokens // bq
    one = pl.Buffered(1)
    early = lambda s: jnp.minimum(s, n - 1)
    middle = lambda s: jnp.clip(s - n, 0, inner - 1)
    late = lambda s: jnp.maximum(s - n - inner, 0)
    twice = early if wqkv is None else lambda s: jnp.where(s < n, s, late(s))
    rows = lambda w, which: pl.BlockSpec((bt, w), lambda s: (which(s), 0))
    by_head = lambda which, block: pl.BlockSpec((None, heads, block, HEAD), lambda s: (layer, 0, which(s), 0))
    all_of = lambda a: pl.BlockSpec((None, *a.shape[1:]), lambda s: (layer, 0, 0), pipeline_mode=one)
    anywhere = pl.BlockSpec(memory_space=pl.ANY)
    cuts = [(a.shape[0] // 8, a.shape[1] - first) for a, first in ((dwg, since), (dwu, since), (dwd, 0))]
    cut_o = (d // 8, d)
    out = lambda s: jax.ShapeDtypeStruct(s, BF16)
    tile, dma = jax.ShapeDtypeStruct(TILE, F32), pltpu.SemaphoreType.DMA
    blocks, block_shapes = [anywhere] * 4, [*(out(c) for c in cuts), out(cut_o)]
    if known:
        more, more_in = known, [whole(*TILE) for _ in known]
        outs = [*blocks, *[anywhere] * 3, pl.BlockSpec(memory_space=pltpu.SMEM)]
        shapes = [*block_shapes, *(out((d // 8, n)) for n in (d, HEAD, HEAD)), jax.ShapeDtypeStruct((1, 1), F32)]
        own = [pltpu.VMEM((d, wide), BF16), pltpu.VMEM(TILE, F32), pltpu.VMEM((8, *TILE), F32), dma((8,)), dma((8,))]
    else:
        more, more_in = [wqkv], [all_of(wqkv)]
        outs, shapes = [whole(d, wide), *blocks, whole(*TILE), rows(d, late)], [out((d, wide)), *block_shapes, tile, out((tokens, d))]
        own = []
    flops = 4 * tokens * d * (d + wide) + 5 * heads * tokens * tokens * HEAD
    return pl.pallas_call(
        functools.partial(_attention_back, bq=bq, bk=bk, first=len(known), since=since, count=count, layer=layer),
        grid=(2 * n + inner,),
        in_specs=[rows(d, twice), by_head(early, bt), by_head(middle, bq), anywhere, anywhere,
                  pl.BlockSpec((None, heads, bq), lambda s: (layer, 0, middle(s))), rows(d, late), all_of(wo),
                  rows(HEAD, late), rows(HEAD, late), anywhere, anywhere, anywhere, *more_in],
        out_specs=outs,
        out_shape=shapes,
        scratch_shapes=[*own, pltpu.VMEM(k.shape[1:], BF16), pltpu.VMEM(k.shape[1:], BF16), dma((2,)), pltpu.VMEM((heads, tokens, HEAD), BF16), pltpu.VMEM((heads, tokens, HEAD), BF16), pltpu.VMEM((heads, tokens), F32),
                        pltpu.VMEM((d, d), F32), pltpu.VMEM((d, d), BF16), pltpu.VMEM((d, wide), F32),
                        pltpu.VMEM((heads, HEAD, bq), F32), pltpu.VMEM((tokens, HEAD), F32), pltpu.VMEM((tokens, HEAD), F32),
                        pltpu.VMEM((bk, bq), F32), *(s for c in cuts for s in scatter_scratch(*c)),
                        *scatter_scratch(*cut_o, in_vmem=True), *(scatter_scratch(d // 8, wide, in_vmem=True) if known else [])],
        compiler_params=params(collective_id=2 + layer, has_side_effects=True),
        cost_estimate=cost(flops, exps=heads * tokens * tokens // 2),
        name="attention_back",
    )(dmid, o, q, k, v, lse, h, wo, cos, sin, dwg, dwu, dwd, *more)


def clipping(me, squares, all_s, send, recv, count):
    copies = [pltpu.make_async_remote_copy(src_ref=squares, dst_ref=all_s.at[bits], send_sem=send.at[bits], recv_sem=recv.at[bits],
                                           device_id=(0, me[bits]), device_id_type=pl.DeviceIdType.MESH) for bits in OTHERS]
    for c in copies:
        c.start()
    for c in copies:
        c.wait_recv()
    sums = [jnp.sum(squares[:]), *(jnp.sum(all_s[bits]) for bits in OTHERS)]
    while len(sums) > 1:
        sums = [a + b for a, b in zip(sums[::2], sums[1::2])]
    for c in copies:
        c.wait_send()
    return jnp.max(jnp.minimum(1.0, 0.5 * lax.rsqrt(jnp.full(TILE, sums[0] / count) + 1e-30)))


def adamw(w, m, v, g):
    m = 0.9 * m + 0.1 * g
    v = 0.95 * v + 0.05 * g * g
    step = m * lax.rsqrt(v + 1e-8) + 0.1 * w
    return (w - 0.02 * step).astype(BF16), m, v


def solution(mesh):
    def step(x, dy, *arrays):
        weights, m, v = (arrays[i : i + 7] for i in (0, 7, 14))
        tokens = x.shape[1]
        cos, sin = tables(tokens)
        *full, q, k, v_, o, lse, mid, gate, up, h1 = forward(x[0], weights, cos, sin)
        fqkv, fo, fg, fu, fd = full
        dmid, dwg, dwu, dwd = mlp_back(1, dy[0], mid, gate, up, fg, fu, fd)
        dlater, g1, u1, d1, o1, s1, dh = attention_back(1, dmid, o, q, k, v_, lse, h1, fo, cos, sin, dwg, dwu, dwd, wqkv=fqkv)
        dmid, dwg, dwu, dwd, ga, ua, *qkv1, s2 = mlp_back(0, dh, mid, gate, up, fg, fu, fd, dlater, CUT)
        gb, ub, d0, o0, *qkv0, factor = attention_back(0, dmid, o, q, k, v_, lse, x[0], fo, cos, sin, dwg, dwu, dwd, since=CUT, known=[s1, s2],
                                                      count=8 * sum(w.size for w in weights))
        g0, u0 = jnp.concatenate([ga, gb], axis=1), jnp.concatenate([ua, ub], axis=1)
        factor = factor[0, 0]
        mine = [[*qkv0, o0, g0, u0, d0], [*qkv1, o1, g1, u1, d1]]
        gradients = [jnp.stack([one[i] for one in mine]).astype(F32) for i in range(7)]
        new = [adamw(w.astype(F32), m, v, g * factor) for w, m, v, g in zip(weights, m, v, gradients, strict=True)]
        return tuple(one[which] for which in range(3) for one in new)

    states, cut = P(("rep", "dp"), None, None), P(None, "dp", None)
    return jax.shard_map(
        step,
        mesh=mesh,
        in_specs=(states, states) + (cut,) * 21,
        out_specs=(P("rep", "dp", None),) * 21,
        check_vma=False,
    )
```

```python
import functools

import jax
import jax.numpy as jnp
import numpy as np
from jax import lax
from jax.experimental import pallas as pl
from jax.experimental.pallas import tpu as pltpu
from jax.sharding import PartitionSpec as P

NEG = -1e30
HIDDEN = 2 * NEG
LOG2E = 1.4426950408889634
VMEM = 127 * 2**19
STRIP = 512
HEAD = 128
HALF = HEAD // 2
TILE = (8, 128)
THETA = 10000
F32, BF16 = jnp.float32, jnp.bfloat16


def dot(a, b, ca=1, cb=0):
    return lax.dot_general(a, b, (((ca,), (cb,)), ((), ())), preferred_element_type=F32)


def dot_t(a, b):
    return dot(a, b, 1, 1)


def loop(stop, body, start=0):
    lax.fori_loop(start, stop, body, None)


def rounded(a):
    return a.astype(BF16).astype(F32)


def norm_scale(wide):
    return lax.rsqrt(jnp.mean(wide * wide, -1, keepdims=True) + 1e-6)


def norm_back(wide, by):
    scale = norm_scale(wide)
    return scale * (by - wide * (scale * scale * jnp.mean(by * wide, -1, keepdims=True)))


def params(**more):
    return pltpu.CompilerParams(vmem_limit_bytes=VMEM, **more)


def whole(*shape):
    return pl.BlockSpec(shape, lambda *_: (0,) * len(shape))


def cost(flops, nbytes=0, exps=0):
    return pl.CostEstimate(flops=int(flops), bytes_accessed=int(nbytes), transcendentals=int(exps))


def tables(tokens):
    angle = np.arange(tokens, dtype=np.float64)[:, None] * THETA ** (-np.arange(HALF, dtype=np.float64) / HALF)
    cos, sin = np.cos(angle), np.sin(angle)
    return jnp.asarray(np.concatenate([cos, cos], 1), F32), jnp.asarray(np.concatenate([-sin, sin], 1), F32)


def hidden(keys, queries, later=0):
    gap = lax.broadcasted_iota(jnp.int32, (keys, queries), 1) - lax.broadcasted_iota(jnp.int32, (keys, queries), 0)
    return jnp.where(gap + later >= 0, 0.0, HIDDEN)


def side_by_side(ref):
    return jnp.concatenate([ref[n] for n in range(ref.shape[0])], axis=1)


X, Y, CORE, HERE = 4, 2, 1, 0
OTHERS = range(1, 8)
NEAR = (HERE, X, Y, X + Y)


def places():
    at = [lax.axis_index("dp")]
    for bit in (CORE, Y, X):
        at += [n + bit - 2 * bit * lax.rem(lax.div(n, bit), 2) for n in at]
    return at


def greet(me, all_of=(X, Y, CORE)):
    barrier = pltpu.get_barrier_semaphore()
    for bits in all_of:
        pl.semaphore_signal(barrier, inc=1, device_id=(0, me[bits]), device_id_type=pl.DeviceIdType.MESH)
    return lambda: pl.semaphore_wait(barrier, len(all_of))


def remote(me, bit, src, dst, send, recv):
    return pltpu.make_async_remote_copy(src_ref=src, dst_ref=dst, send_sem=send, recv_sem=recv, device_id=(0, me[bit]),
                                        device_id_type=pl.DeviceIdType.MESH)


def halves(r):
    a = (r // 2 + 15) // 16 * 16
    return (0, a), (a, r - a)


def upper(r):
    return halves(r)[0]


def lower(r):
    return halves(r)[1]


ALL = None
ROUTES = {"x": (X, HERE, ALL), "y": (Y, HERE, ALL), "core": (CORE, HERE, ALL), "xy": (Y, X, upper), "x core": (CORE, X, ALL),
          "yx": (X, Y, lower), "y core": (CORE, Y, ALL), "xy core": (CORE, X + Y, upper), "yx core": (CORE, X + Y, lower)}


class Gather:
    def __init__(self, me, block, full, send, recv, cols, at):
        first, count = cols
        self.me, self.r = me, block.shape[0]
        self.full, self.send, self.recv = full, send, recv
        self.own, self.cols = block.at[:, pl.ds(first, count)], pl.ds(at + first, count)

    def rows(self, bits, part=None):
        first, count = part or (0, self.r)
        at = pl.multiple_of(self.me[bits] * self.r + first, 16)
        return self.full.at[pl.ds(at, count), self.cols]

    def copy(self, which, got=False):
        bit, bits, part = ROUTES[which]
        there = self.rows(bits + bit if got else bits, part and part(self.r))
        n = tuple(ROUTES).index(which)
        return remote(self.me, bit, self.own if bits == HERE and not got else there, there, self.send.at[n], self.recv.at[n])

    def got(self, which):
        self.copy(which, got=True).wait_recv()

    def begin(self):
        for n in ("x", "y", "core"):
            self.copy(n).start()

    def hand_on(self):
        self.got("x")
        self.copy("xy").start()
        self.copy("x core").start()
        self.got("y")
        self.copy("yx").start()
        self.copy("y core").start()

    def finish(self):
        self.got("xy")
        self.copy("xy core").start()
        self.got("yx")
        self.copy("yx core").start()

    def arrived(self):
        for n in ("core", "x core", "y core", "xy core", "yx core"):
            self.got(n)

    def sent(self):
        for n in ROUTES:
            self.copy(n).wait_send()


class Scatter:
    def __init__(self, me, src, mine, theirs, across, from_x, from_y, out, send, recv, local):
        self.me, self.src, self.out = me, src, out
        self.r, self.n = theirs.shape[1:]
        self.own, self.theirs, self.across, self.from_x, self.from_y = mine, theirs, across, from_x, from_y
        self.send, self.recv, self.local = send, recv, local
        self.a, self.b = halves(self.r)
        self.all = (0, self.r)

    def block(self, bits, part=None):
        first, count = part or self.all
        return self.src.at[pl.ds(pl.multiple_of(self.me[bits] * self.r + first, 16), count)]

    def mine(self, j, part):
        return self.block(NEAR[j], part) if self.own is None else self.own.at[j, pl.ds(*part)]

    def load(self, j):
        return pltpu.make_async_copy(self.block(NEAR[j]), self.own.at[j], self.local.at[j])

    def copy(self, n):
        if n < 4:
            bit, src, dst = CORE, self.block(CORE + NEAR[n]), self.theirs.at[n]
        else:
            bit, j, part, to = ((X, 3, self.a, self.across), (Y, 3, self.b, self.across), (X, 1, self.a, self.from_x),
                                (Y, 2, self.b, self.from_y), (Y, 2, self.a, self.from_y), (X, 1, self.b, self.from_x))[n - 4]
            src, dst = self.mine(j, part), to.at[pl.ds(*part)]
        return remote(self.me, bit, src, dst, self.send.at[n], self.recv.at[n])

    def add(self, j, part, *more):
        step = 16
        ref = self.mine(j, part)

        def one(i, _):
            rows = pl.ds(pl.multiple_of(i * step, step), step)
            full = pl.ds(pl.multiple_of(part[0] + i * step, step), step)
            total = ref[rows, :].astype(F32) + self.theirs[j, full, :].astype(F32)
            for other in more:
                total += other[full, :].astype(F32)
            ref[rows, :] = total.astype(BF16)

        loop(part[1] // step, one)

    def exchange(self):
        for j in range(4):
            self.copy(j).start()
            if self.own is not None:
                self.load(j).start()

    def first(self):
        for j in range(4):
            if self.own is not None:
                self.load(j).wait()
            self.copy(j).wait_recv()
        self.add(3, self.all)
        self.copy(4).start()
        self.copy(5).start()
        self.add(1, self.a)
        self.add(2, self.b)

    def second(self):
        self.copy(6).start()
        self.copy(7).start()
        self.copy(4).wait_recv()
        self.add(2, self.a, self.across)
        self.copy(8).start()
        self.copy(5).wait_recv()
        self.add(1, self.b, self.across)
        self.copy(9).start()

    def results(self):
        at, copies = 0, []
        for i, out in enumerate(self.out if isinstance(self.out, list) else [self.out]):
            block = self.mine(0, self.all).at[:, pl.ds(at, out.shape[1])]
            copies.append(pltpu.make_async_copy(block, out, self.local.at[4 + i]))
            at += out.shape[1]
        return copies

    def last(self, squares):
        for n in range(6, 10):
            self.copy(n).wait_recv()
        self.add(0, self.all, self.from_x, self.from_y)
        ref = self.mine(0, self.all)
        for c in self.results():
            c.start()
        squares[:] += sum_of_squares(ref)

    def done(self):
        for n in range(10):
            self.copy(n).wait_send()
        for c in self.results():
            c.wait()


def sum_of_squares(ref):
    rows, cols = ref.shape

    def one(i, total):
        g = ref[pl.ds(pl.multiple_of(i * 16, 16), 16), :].astype(F32)
        g = g * g
        for c in range(0, cols, 128):
            total += g[:8, c : c + 128] + g[8:, c : c + 128]
        return total

    return lax.fori_loop(0, rows // 16, one, jnp.zeros(TILE, F32))


def scatter_scratch(r, n, in_vmem=False):
    dma = pltpu.SemaphoreType.DMA
    block = pltpu.VMEM((r, n), BF16)
    return [*([] if in_vmem else [pltpu.VMEM((4, r, n), BF16)]), pltpu.VMEM((4, r, n), BF16), block, block, block,
            dma((10,)), dma((10,)), dma((7,))]


BQ = BK = BT = BF = 512
CUT, CUT_Q = 2 * BF, 4 * HEAD
TENSORS = ("qa", "qb", "k", "v", "o", "ga", "ua", "gb", "ub", "d")
QKV, GU_A, GU_B = ["qa", "k", "v", "qb"], ["ga", "ua"], ["gb", "ub"]


def _forward(x_ref, sq, sk, sv, so, sg, su, sd, cos_ref, sin_ref, fqkv, fo, fg, fu, fd, q_o, k_o, v_o, o_o, lse_o, mid_o, gate_o, up_o, h_o,
             h_s, b_s, q_s, k_s, v_s, o_s, lse_s, act_s, wqkv_s, wo_s, wg_s, wu_s, wd_s, stage_s, top_s, mix_s, hide_s,
             send, recv, load, keep, out, wsem):
    layer, layers = pl.program_id(0), pl.num_programs(0)
    me = places()
    tokens, d = h_s.shape
    heads = q_s.shape[0]
    ff = act_s.shape[1]
    blocks = tokens // BT

    def gather(n, name):
        i = TENSORS.index(name)
        shard, full, cols, at = {
            "qa": (sq, fqkv, (0, CUT_Q), 0), "qb": (sq, fqkv, (CUT_Q, d - CUT_Q), 0), "k": (sk, fqkv, (0, HEAD), d),
            "v": (sv, fqkv, (0, HEAD), d + HEAD), "o": (so, fo, (0, d), 0), "d": (sd, fd, (0, d), 0),
            "ga": (sg, fg, (0, CUT), 0), "gb": (sg, fg, (CUT, ff - CUT), 0),
            "ua": (su, fu, (0, CUT), 0), "ub": (su, fu, (CUT, ff - CUT), 0)}[name]
        full = wqkv_s if name in QKV and n == 0 else full.at[n]
        return Gather(me, shard.at[n], full, send.at[n, i], recv.at[n, i], cols, at)

    def own_blocks():
        at = 0
        for s, f, column in ((sq, fqkv, 0), (sk, fqkv, d), (sv, fqkv, d + HEAD), (so, fo, 0), (sg, fg, 0), (su, fu, 0), (sd, fd, 0)):
            r, n = s.shape[1:]
            for i in range(s.shape[0]):
                where = pl.ds(pl.multiple_of(me[HERE] * r, 16), r), pl.ds(column, n)
                if f is fqkv and i == 0:
                    yield s.at[i], wqkv_s.at[where], None
                else:
                    yield s.at[i], act_s.at[pl.ds(at, r), pl.ds(0, n)], f.at[i, *where]
                    at += r

    copies_in = lambda: [pltpu.make_async_copy(a, b, load.at[i]) for i, (a, b, _) in enumerate(own_blocks())]
    copies_out = lambda: [pltpu.make_async_copy(b, c, load.at[i]) for i, (_, b, c) in enumerate(own_blocks()) if c is not None]
    here = lambda i, n: pl.ds(pl.multiple_of(i * n, n), n)

    def kept(*names):
        pairs = {"x": (x_ref, h_s), "q": (q_s, q_o.at[layer]), "k": (k_s, k_o.at[layer]), "v": (v_s, v_o.at[layer]), "o": (o_s, o_o.at[layer]),
                 "lse": (lse_s, lse_o.at[layer]), "mid": (h_s, mid_o.at[layer]), "h": (h_s, h_o), "qkv": (wqkv_s, fqkv.at[layer])}
        return [pltpu.make_async_copy(*pairs[n], keep.at[list(pairs).index(n)]) for n in names]

    def start(*copies):
        for c in copies:
            c.start()

    def wait(*copies):
        for c in copies:
            c.wait()

    def weight(n, name):
        return pltpu.make_async_copy(*{"qb": (fqkv.at[n], wqkv_s, wsem.at[0]), "o": (fo.at[n], wo_s, wsem.at[1]),
                                       "d": (fd.at[n], wd_s, wsem.at[2])}[name])

    def column(c, n=layer):
        cols, slot = here(c, BF), lax.rem(c, 2)
        return (pltpu.make_async_copy(fg.at[n, :, cols], wg_s.at[slot], wsem.at[3 + slot]),
                pltpu.make_async_copy(fu.at[n, :, cols], wu_s.at[slot], wsem.at[5 + slot]))

    def fetch(n, name):
        gather(n, name).arrived()
        if name in QKV:
            gather(0, name).sent()
        if name == "ua":
            start(*column(0, n))
        elif name in ("qb", "o", "d"):
            start(weight(n, name))

    def tick(phase, i):
        for n, plan in enumerate(PLAN):
            for p, k, *actions in plan:
                if p == phase:
                    @pl.when((layer == n) & (i == k))
                    def _():
                        for do, later, names in actions:
                            for name in names:
                                if do == "fetch":
                                    fetch(n + later, name)
                                else:
                                    getattr(gather(n + later, name), do)()

    @pl.when(layer == 0)
    def _():
        greeted = greet(me)
        start(*kept("x"), *copies_in())
        hide_s[:] = hidden(BK, BQ)
        greeted()
        for name in QKV:
            gather(0, name).begin()
        wait(*copies_in())
        start(*copies_out())
        wait(*kept("x"))
        for name in QKV:
            gather(0, name).hand_on()
        for name in ("o", *GU_A):
            gather(0, name).begin()
        wait(*copies_out())
        for do in (Gather.finish, Gather.arrived):
            for name in QKV:
                do(gather(0, name))

    @pl.when(layer > 0)
    def _():
        start(*kept("h"))
        wait(weight(1, "qb"))

    def qkv_step(i):
        rows = here(i, BT)
        wide = h_s[rows, :].astype(F32)
        a = (wide * norm_scale(wide)).astype(BF16)
        z = dot(a, wqkv_s[:])
        cos, sin = cos_ref[rows, :], sin_ref[rows, :]
        for n in range(heads + 1):
            t = rounded(z[:, n * HEAD : (n + 1) * HEAD])
            t = (t * cos + pltpu.roll(t, HALF, 1) * sin).astype(BF16)
            if n < heads:
                q_s[n, rows, :] = t
            else:
                k_s[rows, :] = t
        v_s[rows, :] = z[:, (heads + 1) * HEAD :].astype(BF16)

    pairwise(blocks, qkv_step, lambda i: tick("qkv", i))
    start(*kept("q", "k", "v"))

    @pl.when(layer == 0)
    def _():
        start(*kept("qkv"))

    scale = HEAD**-0.5
    e = scale * LOG2E

    def attend_step(i, _):
        top_s[:] = jnp.full(top_s.shape, NEG, F32)
        mix_s[:] = jnp.zeros(mix_s.shape, F32)

        def block(first, count, at=0, hidden=None):
            keys, cols = pl.ds(pl.multiple_of(first, BK // 2), count), pl.ds(at, BQ - at)
            rows = pl.ds(pl.multiple_of(i * BQ + at, BQ // 2), BQ - at)
            values = jnp.concatenate([v_s[keys, :].T, jnp.ones((8, count), BF16)], axis=0)
            scores = [dot_t(k_s[keys, :], q_s[n, rows, :]) for n in range(heads)]
            weights = []
            for n, s in enumerate(scores):
                s = s if hidden is None else s + hidden
                old = top_s[n : n + 1, cols]
                top = jnp.maximum(old, s.max(axis=0, keepdims=True))
                top_s[n : n + 1, cols] = top
                weights.append((jnp.exp2((s - top) * e).astype(BF16), jnp.exp2((old - top) * e)))
            for n, (p, rest) in enumerate(weights):
                mix_s[n, :, cols] = mix_s[n, :, cols] * rest + dot(values, p)

        def before(j, _):
            tick("attend", lax.div(i * (i + 1), 2) + j)
            block(j * BK, BK)

        loop(i, before)
        tick("attend", lax.div(i * (i + 3), 2))
        half = BK // 2
        block(i * BK, half, hidden=hide_s[:half, :])
        block(i * BK + half, half, half, hide_s[half:, half:])
        rows = here(i, BQ)
        for n in range(heads):
            total = mix_s[n, HEAD : HEAD + 1, :]
            o_s[n, rows, :] = (mix_s[n, :HEAD, :] * (1 / total)).T.astype(BF16)
            lse_s[n : n + 1, rows] = top_s[n : n + 1, :] * scale + jnp.log(total)

    loop(tokens // BQ, attend_step)
    start(*kept("o", "lse"))

    @pl.when(layer == 0)
    def _():
        wait(*kept("qkv"))

    @pl.when(layer > 0)
    def _():
        wait(*kept("h"))

    wait(weight(layer, "o"))

    def out_step(i):
        rows = here(i, BT)
        o = jnp.concatenate([o_s[n, rows, :] for n in range(heads)], axis=1)
        mid = (h_s[rows, :].astype(F32) + rounded(dot(o, wo_s[:]))).astype(BF16)
        h_s[rows, :] = mid
        wide = mid.astype(F32)
        b_s[rows, :] = (wide * norm_scale(wide)).astype(BF16)

    pairwise(blocks, out_step, lambda i: tick("out", i))
    start(*kept("mid"))

    def staged(i, c):
        rows, cols = here(i, BT), here(c, BF)
        return [pltpu.make_async_copy(stage_s.at[i, w], ref.at[layer, rows, cols], out.at[i, w]) for w, ref in enumerate((gate_o, up_o))]

    def gate_column(c, _):
        wait(*column(c))

        def gate_step(i):
            rows = here(i, BT)
            b = b_s[rows, :]
            gate, up = dot(b, wg_s[lax.rem(c, 2)]), dot(b, wu_s[lax.rem(c, 2)])
            stage_s[i, 0] = gate
            stage_s[i, 1] = up
            act_s[rows, here(c, BF)] = (gate * jax.nn.sigmoid(gate) * up).astype(BF16)
            start(*staged(i, c))

        for i in range(0, blocks, 2):
            tick("gate", 2 * c + i // 2)
            if i > 0:
                pl.when(c + 1 < ff // BF)(lambda: start(*column(c + 1)))

            @pl.when((layer > 0) | (c > 0))
            def _():
                wait(*staged(i, c), *staged(i + 1, c))

            gate_step(i)
            gate_step(i + 1)

    loop(ff // BF, gate_column)
    wait(*kept("q", "k", "v", "o", "lse", "mid"))

    @pl.when(layer < layers - 1)
    def _():
        wait(weight(0, "d"))

        def down_step(i):
            rows = here(i, BT)
            h_s[rows, :] = (h_s[rows, :].astype(F32) + rounded(dot(act_s[rows, :], wd_s[:]))).astype(BF16)

        pairwise(blocks, down_step, lambda i: tick("down", i))
        tick("end", 0)

    @pl.when(layer == layers - 1)
    def _():
        gather(1, "d").arrived()
        for i in range(blocks):
            wait(*staged(i, 0))
        for n in range(2):
            for name in TENSORS:
                if name not in QKV or n > 0:
                    gather(n, name).sent()


def pairwise(count, body, first):
    def two(i, _):
        first(i)
        body(2 * i)
        body(2 * i + 1)

    loop(count // 2, two)


THIS, NEXT = range(2)
PLAN = ([
    ("qkv", 1, ("hand_on", THIS, ["o"]), ("begin", THIS, GU_B)),
    ("attend", 3, ("hand_on", THIS, GU_A), ("finish", THIS, ["o"])),
    ("attend", 8, ("fetch", THIS, ["o"])),
    ("attend", 9, ("hand_on", THIS, GU_B), ("begin", THIS, ["d"])),
    ("out", 1, ("finish", THIS, GU_A), ("fetch", THIS, GU_A)),
    ("gate", 2, ("finish", THIS, GU_B)),
    ("gate", 3, ("fetch", THIS, GU_B)),
    ("gate", 4, ("begin", NEXT, QKV)),
    ("gate", 6, ("hand_on", THIS, ["d"])),
    ("gate", 8, ("hand_on", NEXT, QKV), ("begin", NEXT, ["o"])),
    ("gate", 9, ("finish", THIS, ["d"]), ("fetch", THIS, ["d"])),
    ("down", 0, ("finish", NEXT, QKV), ("begin", NEXT, GU_A)),
    ("down", 1, ("fetch", NEXT, QKV)),
], [
    ("qkv", 0, ("hand_on", THIS, ["o"])),
    ("qkv", 1, ("begin", THIS, ["gb"])),
    ("attend", 1, ("hand_on", THIS, GU_A), ("begin", THIS, ["ub"])),
    ("attend", 4, ("finish", THIS, ["o"])),
    ("attend", 7, ("fetch", THIS, ["o"])),
    ("attend", 8, ("finish", THIS, GU_A)),
    ("attend", 9, ("hand_on", THIS, GU_B), ("begin", THIS, ["d"])),
    ("out", 1, ("fetch", THIS, GU_A)),
    ("gate", 2, ("finish", THIS, GU_B)),
    ("gate", 3, ("fetch", THIS, GU_B)),
    ("gate", 6, ("hand_on", THIS, ["d"])),
    ("gate", 9, ("finish", THIS, ["d"])),
])


def forward(x, shards, cos, sin):
    tokens, d = x.shape
    layers = shards[0].shape[0]
    heads, ff = d // HEAD, shards[4].shape[2]
    full = [jax.ShapeDtypeStruct((layers, *s), BF16) for s in ((d, d + 2 * HEAD), (d, d), (d, ff), (d, ff), (ff, d))]
    shape = lambda *s: jax.ShapeDtypeStruct((layers, *s), BF16)
    wide = jax.ShapeDtypeStruct((layers, tokens, ff), F32)
    once = lambda a: pl.BlockSpec(a.shape, lambda i: (0,) * len(a.shape), pipeline_mode=pl.Buffered(1))
    anywhere = pl.BlockSpec(memory_space=pl.ANY)
    dma = pltpu.SemaphoreType.DMA
    outs = [*full, shape(heads, tokens, HEAD), shape(tokens, HEAD), shape(tokens, HEAD), shape(heads, tokens, HEAD),
            jax.ShapeDtypeStruct((layers, heads, tokens), F32), shape(tokens, d), wide, wide, jax.ShapeDtypeStruct((tokens, d), BF16)]
    states, by_head, one_head = pltpu.VMEM((tokens, d), BF16), pltpu.VMEM((heads, tokens, HEAD), BF16), pltpu.VMEM((tokens, HEAD), BF16)
    matrix, columns = lambda i: pltpu.VMEM(full[i].shape[1:], BF16), pltpu.VMEM((2, d, BF), BF16)
    routes = dma((layers, len(TENSORS), len(ROUTES)))
    return pl.pallas_call(
        _forward,
        grid=(layers,),
        in_specs=[anywhere] * 8 + [once(cos), once(sin)],
        out_specs=[anywhere] * len(outs),
        out_shape=outs,
        scratch_shapes=[states, states, by_head, one_head, one_head, by_head, pltpu.VMEM((heads, tokens), F32), pltpu.VMEM((tokens, ff), BF16),
                        matrix(0), matrix(1), columns, columns, matrix(4), pltpu.VMEM((tokens // BT, 2, BT, BF), F32),
                        pltpu.VMEM((heads, BQ), F32), pltpu.VMEM((heads, HEAD + 8, BQ), F32), pltpu.VMEM((BK, BQ), F32),
                        routes, routes, dma((7 * layers,)), dma((9,)), dma((tokens // BT, 2)), dma((7,))],
        compiler_params=params(collective_id=0, has_side_effects=True),
        cost_estimate=cost(4 * tokens * (7 * HEAD * 1200 + 3 * d * ff)),
        name="forward",
    )(x, *shards, cos, sin)


def act_on(plan, step, scatters, squares):
    for at, actions in plan.items():
        @pl.when(step == at)
        def _():
            for what, names in actions:
                for name in names:
                    getattr(scatters[name], what)(*([squares] if what == "last" else []))


MLP_PLAN = {
    1: [("exchange", ["qkv"])],
    2: [("first", ["qkv"])],
    3: [("second", ["qkv"])],
    5: [("exchange", ["g", "u"])],
    6: [("first", ["g", "u"]), ("last", ["qkv"])],
    7: [("second", ["g", "u"])],
}


def _mlp_back(*refs, bt, cut, layer):
    dy_ref, mid_ref, gate_ref, up_ref, wg_ref, wu_ref, wd_ref, *refs = refs
    ready = lambda copies: [c.wait() for c in copies]
    if cut:
        dlater_ref, dmid_ref, dwg_ref, dwu_ref, dwd_ref, gg_ref, gu_ref, gq_ref, gk_ref, gv_ref, squares_ref, *refs = refs
    else:
        dmid_ref, dwg_ref, dwu_ref, dwd_ref, *refs = refs
    dy_s, mid_s, gu_s, bt_s, dyt_s, db_s, act_s, dgu_s, out_s, in_sem, gu_sem, out_sem, *refs = refs
    f, steps = pl.program_id(0), pl.num_programs(0)
    tokens = dy_s.shape[0]
    bf = act_s.shape[1]
    pieces = [pl.ds(at, bt) for at in range(0, tokens, bt)]

    def loads(p):
        return [pltpu.make_async_copy(ref.at[pieces[p]], s.at[pieces[p]], in_sem.at[p, w])
                for w, (ref, s) in enumerate(((dy_ref, dy_s), (mid_ref.at[layer], mid_s)))]

    def hidden_blocks(f):
        cols, slot = pl.ds(pl.multiple_of(f * bf, bf), bf), lax.rem(f, 2)
        return [pltpu.make_async_copy(ref.at[layer, :, cols], gu_s.at[slot, w], gu_sem.at[slot, w]) for w, ref in enumerate((gate_ref, up_ref))]

    def stored(p):
        return pltpu.make_async_copy(dy_s.at[pieces[p]], dmid_ref.at[pieces[p]], in_sem.at[p, 0])

    def results(f):
        cols, slot = pl.ds(pl.multiple_of(f * bf, bf), bf), lax.rem(f, 2)
        return [pltpu.make_async_copy(out_s.at[slot, w], ref.at[:, cols], out_sem.at[slot, w]) for w, ref in enumerate((dwg_ref, dwu_ref))]

    finished = lambda f: ready(results(f))

    @pl.when(f == 0)
    def _():
        for copies in (*map(loads, range(len(pieces))), hidden_blocks(f)):
            for c in copies:
                c.start()

    @pl.when(f + 1 < steps)
    def _():
        for c in hidden_blocks(f + 1):
            c.start()

    @pl.when(f >= 2)
    def _():
        finished(f - 2)

    if cut:
        me = places()
        scatters = {}
        firsts = lambda ref: ref.at[:, pl.ds(0, cut)]
        for name, src, out in (("qkv", dlater_ref, [gq_ref, gk_ref, gv_ref]), ("g", firsts(dwg_ref), gg_ref), ("u", firsts(dwu_ref), gu_ref)):
            mine, theirs, across, from_x, from_y, send, recv, local, *refs = refs
            scatters[name] = Scatter(me, src, mine, theirs, across, from_x, from_y, out, send, recv, local)

        @pl.when(f == 0)
        def _():
            greet(me)
            squares_ref[:] = jnp.zeros_like(squares_ref)

        @pl.when(f == 1)
        def _():
            pl.semaphore_wait(pltpu.get_barrier_semaphore(), 3)

        act_on(MLP_PLAN, f, scatters, squares_ref)

    @pl.when(f == 0)
    def _():
        db_s[:] = jnp.zeros_like(db_s)
        for p, here in enumerate(pieces):
            ready(loads(p))
            wide = mid_s[here, :].astype(F32)
            bt_s[:, here] = (wide * norm_scale(wide)).astype(BF16).T
            dyt_s[:, here] = dy_s[here, :].T

    ready(hidden_blocks(f))
    both = jnp.concatenate([wg_ref[:], wu_ref[:]], axis=1)
    for here in pieces:
        gate, up = (gu_s[lax.rem(f, 2), w, here, :] for w in range(2))
        dact = rounded(dot_t(dy_s[here, :], wd_ref[:]))
        sig = jax.nn.sigmoid(gate)
        silu = gate * sig
        act_s[here, :] = (silu * up).astype(BF16)
        dgu_s[here, bf:] = (dact * silu).astype(BF16)
        dgu_s[here, :bf] = (dact * up * (sig * (1 + gate * (1 - sig)))).astype(BF16)
    dwd_ref[:] = dot(dyt_s[:], act_s[:]).astype(BF16).T
    dgu = dot(bt_s[:], dgu_s[:])
    out_s[lax.rem(f, 2), 0] = dgu[:, :bf].astype(BF16)
    out_s[lax.rem(f, 2), 1] = dgu[:, bf:].astype(BF16)
    db_s[:] += dot_t(dgu_s[:], both)
    for c in results(f):
        c.start()

    @pl.when(f == steps - 1)
    def _():
        for p, here in enumerate(pieces):
            wide = mid_s[here, :].astype(F32)
            dy_s[here, :] = (dy_s[here, :].astype(F32) + norm_back(wide, rounded(db_s[here, :]))).astype(BF16)
            stored(p).start()
        finished(f - 1)
        finished(f)
        if cut:
            for name in "gu":
                scatters[name].last(squares_ref)
            for scatter in scatters.values():
                scatter.done()
        for p in range(len(pieces)):
            stored(p).wait()


def mlp_back(layer, dy, mid, gate, up, wg, wu, wd, dlater=None, cut=0, bt=512, bf=256):
    tokens, d = dy.shape
    ff = wg.shape[2]
    anywhere = pl.BlockSpec(memory_space=pl.ANY)
    column, row = pl.BlockSpec((None, d, bf), lambda f: (layer, 0, f)), pl.BlockSpec((None, bf, d), lambda f: (layer, f, 0))
    out = lambda *s: jax.ShapeDtypeStruct(s, BF16)
    cuts = [(d // 8, n) for n in (dlater.shape[1], cut, cut)] if cut else []
    squares = [jax.ShapeDtypeStruct(TILE, F32)] if cut else []
    blocks = [*cuts[1:], *((d // 8, n) for n in (d, HEAD, HEAD))] if cut else []
    dma = pltpu.SemaphoreType.DMA
    states, flipped = pltpu.VMEM((tokens, d), BF16), pltpu.VMEM((d, tokens), BF16)
    return pl.pallas_call(
        functools.partial(_mlp_back, bt=bt, cut=cut, layer=layer),
        grid=(ff // bf,),
        in_specs=[anywhere] * 4 + [column, column, row, *[anywhere for _ in squares]],
        out_specs=[anywhere, anywhere, anywhere, pl.BlockSpec((bf, d), lambda f: (f, 0)), *[anywhere for _ in blocks],
                   *[whole(*s.shape) for s in squares]],
        out_shape=[out(tokens, d), out(d, ff), out(d, ff), out(ff, d), *[out(*c) for c in blocks], *squares],
        scratch_shapes=[states, states, pltpu.VMEM((2, 2, tokens, bf), F32), flipped, flipped, pltpu.VMEM((tokens, d), F32), pltpu.VMEM((tokens, bf), BF16), pltpu.VMEM((tokens, 2 * bf), BF16),
                        pltpu.VMEM((2, 2, d, bf), BF16), dma((tokens // bt, 2)), dma((2, 2)), dma((2, 2)), *(s for c in cuts for s in scatter_scratch(*c))],
        compiler_params=params(collective_id=1, has_side_effects=True) if cut else params(),
        cost_estimate=cost(12 * tokens * d * ff, exps=tokens * ff),
        name="mlp_back",
    )(dy, mid, gate, up, wg, wu, wd, *([dlater] if cut else []))


CUT_QKV = 5 * HEAD
BACK_PLAN = {
    1: [("exchange", ["g", "u", "d"])],
    2: [("first", ["g"])],
    3: [("first", ["u"])],
    4: [("first", ["d"]), ("exchange", ["o"])],
    6: [("second", ["g"]), ("first", ["o"])],
    8: [("second", ["u"])],
    9: [("second", ["d"])],
    11: [("second", ["o"])],
    12: [("last", ["g"])],
    13: [("last", ["u"])],
    15: [("last", ["d", "o"]), ("done", ["g", "u", "d", "o"])],
}


def _attention_back(*refs, bq, bk, first, since, count, layer):
    dmid_ref, o_ref, q_ref, k_ref, v_ref, lse_ref, h_ref, wo_ref, cos_ref, sin_ref, dwg_ref, dwu_ref, dwd_ref, *refs = refs
    if first:
        *known, gg_ref, gu_ref, gd_ref, go_ref, gq_ref, gk_ref, gv_ref, factor_ref = refs[: first + 8]
        dwqkv_ref, squares_ref, all_s, send_all, recv_all, *refs = refs[first + 8 :]
    else:
        wqkv_ref, dwqkv_ref, gg_ref, gu_ref, gd_ref, go_ref, squares_ref, dh_ref, *refs = refs
    k_s, v_s, late_sem, *refs = refs
    do_s, dq_s, delta_s, dwo_s, dwob_s, dwqkv_s, dqt_s, dk_s, dv_s, hide_s, *refs = refs
    me = places()
    step = pl.program_id(0)
    heads, bt = o_ref.shape[:2]
    n, middle = do_s.shape[1] // bt, do_s.shape[1] // bq
    scatters = {}
    rest = lambda ref: ref.at[:, pl.ds(since, ref.shape[1] - since)]
    for name, src, out in (("g", rest(dwg_ref), gg_ref), ("u", rest(dwu_ref), gu_ref), ("d", dwd_ref, gd_ref)):
        mine, theirs, across, from_x, from_y, send, recv, local, *refs = refs
        scatters[name] = Scatter(me, src, mine, theirs, across, from_x, from_y, out, send, recv, local)
    halves_of_qkv = []
    if first:
        part = lambda ref, at, end: ref.at[:, pl.ds(at, end - at)]
        width = gq_ref.shape[1]
        halves_of_qkv = [("q", part(dwqkv_ref, 0, CUT_QKV), part(gq_ref, 0, CUT_QKV)),
                         ("kv", part(dwqkv_ref, CUT_QKV, dwqkv_ref.shape[1]), [part(gq_ref, CUT_QKV, width), gk_ref, gv_ref])]
    for name, src, out in (("o", dwob_s, go_ref), *halves_of_qkv):
        theirs, across, from_x, from_y, send, recv, local, *refs = refs
        scatters[name] = Scatter(me, src, None, theirs, across, from_x, from_y, out, send, recv, local)
    others = OTHERS if first else (X, Y, CORE)

    keys = [pltpu.make_async_copy(ref.at[layer], s, late_sem.at[i]) for i, (ref, s) in enumerate(((k_ref, k_s), (v_ref, v_s)))]

    @pl.when(step == 0)
    def _():
        for c in keys:
            c.start()
        greet(me, others)
        squares_ref[:] = jnp.zeros_like(squares_ref)
        dwo_s[:] = jnp.zeros_like(dwo_s)
        dwqkv_s[:] = jnp.zeros_like(dwqkv_s)
        dk_s[:] = jnp.zeros_like(dk_s)
        dv_s[:] = jnp.zeros_like(dv_s)
        hide_s[:] = hidden(bk, bq, bq)

    @pl.when(step == 1)
    def _():
        pl.semaphore_wait(pltpu.get_barrier_semaphore(), len(others))

    act_on(BACK_PLAN, step, scatters, squares_ref)

    @pl.when(step < n)
    def _():
        rows = pl.ds(pl.multiple_of(step * bt, bt), bt)
        dmid = dmid_ref[:]
        do = dot_t(dmid, wo_ref[:]).astype(BF16)
        for i in range(heads):
            mine = do[:, i * HEAD : (i + 1) * HEAD]
            do_s[i, rows, :] = mine
            delta_s[i : i + 1, rows] = jnp.sum((mine.astype(F32) * o_ref[i].astype(F32)).T, axis=0, keepdims=True)
        dwo_s[:] += dot(side_by_side(o_ref).T, dmid)

        @pl.when(step == n - 1)
        def _():
            dwob_s[:] = dwo_s[:].astype(BF16)

    @pl.when((step >= n) & (step < n + middle))
    def _():
        iq = step - n

        @pl.when(iq == 0)
        def _():
            for c in reversed(keys):
                c.wait()

        rows = pl.ds(pl.multiple_of(iq * bq, bq), bq)
        scale = HEAD**-0.5
        e = scale * LOG2E
        dqt_s[:] = jnp.zeros_like(dqt_s)

        def block(first, count, hide=None):
            keys = pl.ds(pl.multiple_of(first, bq), count)
            qs, dos = [q_ref[i] for i in range(heads)], [do_s[i, rows, :] for i in range(heads)]
            scores = [dot_t(k_s[keys, :], x) for x in qs]
            dps = [dot_t(v_s[keys, :], x) for x in dos]
            for i in range(heads):
                s = scores[i] * e - lse_ref[i : i + 1, :] * LOG2E
                p = jnp.exp2(s if hide is None else s + hide)
                ds = (p * (dps[i] - delta_s[i : i + 1, rows])).astype(BF16)
                dv_s[keys, :] += dot(p.astype(BF16), dos[i])
                dk_s[keys, :] += dot(ds, qs[i])
                dqt_s[i] += dot(k_s[keys, :].T, ds)

        whole_blocks = lax.div(iq, 2)
        loop(whole_blocks, lambda j, _: block(j * bk, bk))
        pl.when(lax.rem(iq, 2) == 0)(lambda: block(whole_blocks * bk, bq, hide_s[bq:, :]))
        pl.when(lax.rem(iq, 2) == 1)(lambda: block(whole_blocks * bk, bk, hide_s[:]))
        for i in range(heads):
            dq_s[i, rows, :] = (dqt_s[i] * scale).T.astype(BF16)

    @pl.when(step >= n + middle)
    def _():
        rows = pl.ds(pl.multiple_of((step - n - middle) * bt, bt), bt)
        cos, sin = cos_ref[:], sin_ref[:]
        parts = []
        for t in [*(dq_s[i, rows, :] for i in range(heads)), (dk_s[rows, :] * HEAD**-0.5).astype(BF16)]:
            t = t.astype(F32)
            parts.append((t * cos - pltpu.roll(t, HALF, 1) * sin).astype(BF16))
        dz = jnp.concatenate([*parts, dv_s[rows, :].astype(BF16)], axis=1)
        wide = h_ref[:].astype(F32)
        a = (wide * norm_scale(wide)).T.astype(BF16)
        if not first:
            da = rounded(dot_t(dz, wqkv_ref[:]))
        dwqkv_s[:] += dot(a, dz)
        if not first:
            dh_ref[:] = (dmid_ref[:].astype(F32) + norm_back(wide, da)).astype(BF16)

        @pl.when(step == 2 * n + middle - 1)
        def _():
            dwqkv_ref[:] = dwqkv_s[:].astype(BF16)
            if first:
                both = scatters["q"], scatters["kv"]
                for scatter in both:
                    scatter.exchange()
                for ref in known:
                    squares_ref[:] += ref[:]
                for do in (Scatter.first, Scatter.second):
                    for scatter in both:
                        do(scatter)
                for scatter in both:
                    scatter.last(squares_ref)
                factor_ref[0, 0] = clipping(me, squares_ref, all_s, send_all, recv_all, count)
                for scatter in both:
                    scatter.done()


def attention_back(layer, dmid, o, q, k, v, lse, h, wo, cos, sin, dwg, dwu, dwd, wqkv=None, since=0, known=(), count=0, bq=256, bk=512,
                   bt=512):
    tokens, d = dmid.shape
    heads = o.shape[1]
    wide = d + 2 * HEAD
    n, inner = tokens // bt, tokens // bq
    one = pl.Buffered(1)
    early = lambda s: jnp.minimum(s, n - 1)
    middle = lambda s: jnp.clip(s - n, 0, inner - 1)
    late = lambda s: jnp.maximum(s - n - inner, 0)
    twice = early if wqkv is None else lambda s: jnp.where(s < n, s, late(s))
    rows = lambda w, which: pl.BlockSpec((bt, w), lambda s: (which(s), 0))
    by_head = lambda which, block: pl.BlockSpec((None, heads, block, HEAD), lambda s: (layer, 0, which(s), 0))
    all_of = lambda a: pl.BlockSpec((None, *a.shape[1:]), lambda s: (layer, 0, 0), pipeline_mode=one)
    anywhere = pl.BlockSpec(memory_space=pl.ANY)
    cuts = [(a.shape[0] // 8, a.shape[1] - first) for a, first in ((dwg, since), (dwu, since), (dwd, 0))]
    cut_o = (d // 8, d)
    out = lambda s: jax.ShapeDtypeStruct(s, BF16)
    tile, dma = jax.ShapeDtypeStruct(TILE, F32), pltpu.SemaphoreType.DMA
    blocks, block_shapes = [anywhere] * 4, [*(out(c) for c in cuts), out(cut_o)]
    if known:
        more, more_in = known, [whole(*TILE) for _ in known]
        outs = [*blocks, *[anywhere] * 3, pl.BlockSpec(memory_space=pltpu.SMEM)]
        shapes = [*block_shapes, *(out((d // 8, n)) for n in (d, HEAD, HEAD)), jax.ShapeDtypeStruct((1, 1), F32)]
        own = [pltpu.VMEM((d, wide), BF16), pltpu.VMEM(TILE, F32), pltpu.VMEM((8, *TILE), F32), dma((8,)), dma((8,))]
    else:
        more, more_in = [wqkv], [all_of(wqkv)]
        outs, shapes = [whole(d, wide), *blocks, whole(*TILE), rows(d, late)], [out((d, wide)), *block_shapes, tile, out((tokens, d))]
        own = []
    flops = 4 * tokens * d * (d + wide) + 5 * heads * tokens * tokens * HEAD
    return pl.pallas_call(
        functools.partial(_attention_back, bq=bq, bk=bk, first=len(known), since=since, count=count, layer=layer),
        grid=(2 * n + inner,),
        in_specs=[rows(d, twice), by_head(early, bt), by_head(middle, bq), anywhere, anywhere,
                  pl.BlockSpec((None, heads, bq), lambda s: (layer, 0, middle(s))), rows(d, late), all_of(wo),
                  rows(HEAD, late), rows(HEAD, late), anywhere, anywhere, anywhere, *more_in],
        out_specs=outs,
        out_shape=shapes,
        scratch_shapes=[*own, pltpu.VMEM(k.shape[1:], BF16), pltpu.VMEM(k.shape[1:], BF16), dma((2,)), pltpu.VMEM((heads, tokens, HEAD), BF16), pltpu.VMEM((heads, tokens, HEAD), BF16), pltpu.VMEM((heads, tokens), F32),
                        pltpu.VMEM((d, d), F32), pltpu.VMEM((d, d), BF16), pltpu.VMEM((d, wide), F32),
                        pltpu.VMEM((heads, HEAD, bq), F32), pltpu.VMEM((tokens, HEAD), F32), pltpu.VMEM((tokens, HEAD), F32),
                        pltpu.VMEM((bk, bq), F32), *(s for c in cuts for s in scatter_scratch(*c)),
                        *scatter_scratch(*cut_o, in_vmem=True), *(s for n in (CUT_QKV, wide - CUT_QKV) if known for s in scatter_scratch(d // 8, n, in_vmem=True))],
        compiler_params=params(collective_id=2 + layer, has_side_effects=True),
        cost_estimate=cost(flops, exps=heads * tokens * tokens // 2),
        name="attention_back",
    )(dmid, o, q, k, v, lse, h, wo, cos, sin, dwg, dwu, dwd, *more)


def clipping(me, squares, all_s, send, recv, count):
    copies = [pltpu.make_async_remote_copy(src_ref=squares, dst_ref=all_s.at[bits], send_sem=send.at[bits], recv_sem=recv.at[bits],
                                           device_id=(0, me[bits]), device_id_type=pl.DeviceIdType.MESH) for bits in OTHERS]
    for c in copies:
        c.start()
    for c in copies:
        c.wait_recv()
    sums = [jnp.sum(squares[:]), *(jnp.sum(all_s[bits]) for bits in OTHERS)]
    while len(sums) > 1:
        sums = [a + b for a, b in zip(sums[::2], sums[1::2])]
    for c in copies:
        c.wait_send()
    return jnp.max(jnp.minimum(1.0, 0.5 * lax.rsqrt(jnp.full(TILE, sums[0] / count) + 1e-30)))


def adamw(w, m, v, g):
    m = 0.9 * m + 0.1 * g
    v = 0.95 * v + 0.05 * g * g
    step = m * lax.rsqrt(v + 1e-8) + 0.1 * w
    return (w - 0.02 * step).astype(BF16), m, v


def solution(mesh):
    def step(x, dy, *arrays):
        weights, m, v = (arrays[i : i + 7] for i in (0, 7, 14))
        tokens = x.shape[1]
        cos, sin = tables(tokens)
        *full, q, k, v_, o, lse, mid, gate, up, h1 = forward(x[0], weights, cos, sin)
        fqkv, fo, fg, fu, fd = full
        dmid, dwg, dwu, dwd = mlp_back(1, dy[0], mid, gate, up, fg, fu, fd)
        dlater, g1, u1, d1, o1, s1, dh = attention_back(1, dmid, o, q, k, v_, lse, h1, fo, cos, sin, dwg, dwu, dwd, wqkv=fqkv)
        dmid, dwg, dwu, dwd, ga, ua, *qkv1, s2 = mlp_back(0, dh, mid, gate, up, fg, fu, fd, dlater, CUT)
        gb, ub, d0, o0, *qkv0, factor = attention_back(0, dmid, o, q, k, v_, lse, x[0], fo, cos, sin, dwg, dwu, dwd, since=CUT, known=[s1, s2],
                                                      count=8 * sum(w.size for w in weights))
        g0, u0 = jnp.concatenate([ga, gb], axis=1), jnp.concatenate([ua, ub], axis=1)
        factor = factor[0, 0]
        mine = [[*qkv0, o0, g0, u0, d0], [*qkv1, o1, g1, u1, d1]]
        gradients = [jnp.stack([one[i] for one in mine]).astype(F32) for i in range(7)]
        new = [adamw(w.astype(F32), m, v, g * factor) for w, m, v, g in zip(weights, m, v, gradients, strict=True)]
        return tuple(one[which] for which in range(3) for one in new)

    states, cut = P(("rep", "dp"), None, None), P(None, "dp", None)
    return jax.shard_map(
        step,
        mesh=mesh,
        in_specs=(states, states) + (cut,) * 21,
        out_specs=(P("rep", "dp", None),) * 21,
        check_vma=False,
    )
```
